128 devices in a mesh: rep: 16 (over z, y), nodes: 8 (over x, core).
Axes of the slice: x: 4, y: 4, z: 4, core: 2. Of those that a mesh axis runs over, the one named last changes fastest.
Arguments:
- adjacency: bfloat16 [16, 1536, 24576], P(None, 'nodes', 'rep')
- features: bfloat16 [24576, 128], P(('rep', 'nodes'))
- w_one: float32 [128, 256], replicated
- w_two: float32 [256, 40], replicated
- labels: int32 [24576], P(('rep', 'nodes'))
- label_mask: int32 [24576], P(('rep', 'nodes'))
Outputs:
- output 1: float32 [], replicated
- output 2: float32 [128, 256], replicated
- output 3: float32 [256, 40], replicated
All inputs are finite; a program needn't handle non-finite values.
Results may differ from the reference program's by a relative error of at most 0.001.
Values are sent between devices in bfloat16 or wider.
A program may use at most 1 GiB of HBM per device.

```python
import jax
import jax.numpy as jnp
from jax import lax

REPLICAS = 16
NODE_GROUP = 8
ROWS_DEV = 192
F_IN = 128
F_HID = 256
N_CLASS = 40
N_COMM = 16

N_TOTAL = ROWS_DEV * REPLICAS * NODE_GROUP


def make_adjacency(edge_key, community):
    col_ids = jnp.arange(N_TOTAL)

    def one_block(block_id):
        row_ids = block_id * ROWS_DEV + jnp.arange(ROWS_DEV)
        coin_draw = jax.random.randint(jax.random.fold_in(edge_key, block_id), (ROWS_DEV, N_TOTAL), 0, 1000)
        comm_rows = lax.dynamic_slice(community, (block_id * ROWS_DEV,), (ROWS_DEV,))
        same_comm = comm_rows[:, None] == community[None, :]
        has_edge = (coin_draw < jnp.where(same_comm, 500, 40)) | (row_ids[:, None] == col_ids[None, :])
        degree = jnp.sum(has_edge.astype(jnp.int32), axis=1)
        return (has_edge.astype(jnp.float32) / degree[:, None].astype(jnp.float32)).astype(jnp.bfloat16)

    row_blocks = lax.map(one_block, jnp.arange(N_TOTAL // ROWS_DEV))
    return row_blocks.reshape(REPLICAS, N_TOTAL // REPLICAS, N_TOTAL)


def setup_inputs(seed: int = 0) -> dict:
    base_key = jax.random.key(seed)
    key_list = jax.random.split(base_key, 8)
    community = jax.random.randint(key_list[0], (N_TOTAL,), 0, N_COMM)
    adjacency = make_adjacency(key_list[1], community)
    comm_embed = jax.random.normal(key_list[2], (N_COMM, F_IN), jnp.float32)
    feat_noise = 0.5 * jax.random.normal(key_list[3], (N_TOTAL, F_IN), jnp.float32)
    features = (comm_embed[community] + feat_noise).astype(jnp.bfloat16)
    w_one = jax.random.normal(key_list[4], (F_IN, F_HID), jnp.float32) * F_IN ** -0.5
    w_two = 2.0 * jax.random.normal(key_list[5], (F_HID, N_CLASS), jnp.float32) * F_HID ** -0.5
    labels = jax.random.randint(key_list[6], (N_TOTAL,), 0, N_CLASS).astype(jnp.int32)
    mask_draw = jax.random.randint(key_list[7], (N_TOTAL,), 0, 10)
    label_mask = jnp.where((mask_draw < 6) | (jnp.arange(N_TOTAL) == 0), 1, 0).astype(jnp.int32)
    return {"adjacency": adjacency, "features": features, "w_one": w_one, "w_two": w_two, "labels": labels, "label_mask": label_mask}


def reference(adjacency, features, w_one, w_two, labels, label_mask):
    node_count = features.shape[0]
    adj_flat = adjacency.reshape(node_count, node_count)
    w_one_lo = w_one.astype(jnp.bfloat16)
    w_two_lo = w_two.astype(jnp.bfloat16)
    y_one = jnp.dot(features, w_one_lo, preferred_element_type=jnp.float32).astype(jnp.bfloat16)
    z_one = jnp.dot(adj_flat, y_one, preferred_element_type=jnp.float32)
    h_one = jnp.maximum(z_one, 0.0).astype(jnp.bfloat16)
    y_two = jnp.dot(h_one, w_two_lo, preferred_element_type=jnp.float32).astype(jnp.bfloat16)
    z_two = jnp.dot(adj_flat, y_two, preferred_element_type=jnp.float32)
    weights = label_mask.astype(jnp.float32)
    label_count = jnp.sum(weights)
    log_probs = jax.nn.log_softmax(z_two, axis=-1)
    one_hot = (labels[:, None] == jnp.arange(N_CLASS)[None, :]).astype(jnp.float32)
    loss_value = -jnp.sum(weights * jnp.sum(one_hot * log_probs, axis=-1)) / label_count
    g_two = ((jnp.exp(log_probs) - one_hot) * (weights / label_count)[:, None]).astype(jnp.bfloat16)
    dy_two = lax.dot_general(adj_flat, g_two, (((0,), (0,)), ((), ())), preferred_element_type=jnp.float32).astype(jnp.bfloat16)
    dw_two = lax.dot_general(h_one, dy_two, (((0,), (0,)), ((), ())), preferred_element_type=jnp.float32)
    dh_one = lax.dot_general(dy_two, w_two_lo, (((1,), (1,)), ((), ())), preferred_element_type=jnp.float32)
    g_one = jnp.where(z_one > 0.0, dh_one, 0.0).astype(jnp.bfloat16)
    dy_one = lax.dot_general(adj_flat, g_one, (((0,), (0,)), ((), ())), preferred_element_type=jnp.float32).astype(jnp.bfloat16)
    dw_one = lax.dot_general(features, dy_one, (((0,), (0,)), ((), ())), preferred_element_type=jnp.float32)
    return (loss_value, dw_one, dw_two)
```

```python
import jax
import jax.numpy as jnp
from jax import lax
from jax.experimental import pallas as pl
from jax.experimental.pallas import tpu as pltpu
from jax.sharding import PartitionSpec as P

MESH = pl.DeviceIdType.MESH
F32, BF16 = jnp.float32, jnp.bfloat16
T, G, N = 2, 4, 8
LANE, HID, CLS, ROW = 128, 256, 40, 192
PK = ROW // 3
TALL, WIDE = 16 * ROW, N * ROW
PAIR = T * ROW
N_SEM = 320


def ring(v, k):
    return (v + k + G) % G


def dot(a, b, ca, cb):
    return lax.dot_general(a, b, (((ca,), (cb,)), ((), ())), preferred_element_type=F32)


def span(start, size):
    return pl.ds(start if isinstance(start, int) else pl.multiple_of(start, size), size)


class Net:
    def __init__(self, send_sem, recv_sem):
        rep, node = lax.axis_index("rep"), lax.axis_index("nodes")
        self.z, self.y, self.x, self.c = rep // G, rep % G, node // T, node % T
        self.sems, self.used, self.ends = (send_sem, recv_sem), 0, []

    def dev(self, **place):
        z, y, x, c = (place.get(k, getattr(self, k)) for k in "zyxc")
        return (z * G + y, x * T + c)

    def near(self, axis, k):
        return self.dev(**{axis: ring(getattr(self, axis), k)})

    def partner(self):
        return self.dev(c=1 - self.c)

    def copy(self, src, dst, device, k):
        send, recv = (sem.at[k] for sem in self.sems)
        return pltpu.make_async_remote_copy(src_ref=src, dst_ref=dst, send_sem=send, recv_sem=recv, device_id=device, device_id_type=MESH)

    def send(self, src, dst, device):
        copy = self.copy(src, dst, device, self.used)
        self.used += 1
        copy.start()
        self.ends.append(copy.wait_send)
        return copy

    def rep_all(self, src, dst, before=None):
        base, self.used = self.used, self.used + G * G

        def place(j, sign):
            k = (j * 5) % (G * G)
            return ring(self.z, sign * (k // G)), ring(self.y, sign * (k % G)), base + k

        def start(j, _):
            z, y, k = place(j, 1)
            if before is not None:
                before(z, y)
            self.copy(src(z, y), dst, self.dev(z=z, y=y), k).start()
            return _

        def each(fn):
            def body(j, _):
                z, y, k = place(j, -1)
                self.copy(dst, dst, self.dev(z=z, y=y), k).wait_recv()
                fn(z, y)
                return _
            lax.fori_loop(1, G * G, body, 0)

        def end(j, _):
            z, y, k = place(j, 1)
            self.copy(dst, dst, self.dev(z=z, y=y), k).wait_send()
            return _

        lax.fori_loop(1, G * G, start, 0)
        self.ends.append(lambda: lax.fori_loop(1, G * G, end, 0))
        return each

    def peers(self):
        out = [self.partner()]
        for k in (1, 2, 3):
            out += [self.near(axis, k) for axis in "xyz"]
            out.append(self.dev(x=ring(self.x, k), c=1 - self.c))
        return out


class Tree:
    def __init__(self, net, axis, at, far, near):
        self.net, self.at, self.far, self.near = net, at, far, near
        self.p = getattr(net, axis)
        self.side = net.near(axis, 1), net.near(axis, -1)

    def start(self):
        self.first = [self.net.send(self.at(ring(self.p, T), d), self.far(d), self.side[d]) for d in (0, 1)]
        self.arrive = []

    def free(self, d):
        t = ring(self.p, 1 - T * d)
        self.arrive.append(self.net.send(self.at(t, 1 - d), self.near(d, 1 - d), self.side[d]))

    def relay(self):
        for d in (0, 1):
            self.first[d].wait_recv()
            mine = self.at(ring(self.p, 1 - T * d), d)
            mine[...] = mine[...] + self.far(d)[...]
            self.arrive.append(self.net.send(mine, self.near(d, d), self.side[d]))

    def end(self):
        for copy in self.arrive:
            copy.wait_recv()


class RepSum:
    def __init__(self, net, terms, far, near, mid, last):
        self.net, self.terms, self.near, self.mid, self.last = net, terms, near, mid, last
        self.size = near.shape[-T]
        q = self.size // T
        self.parts = [(h, s) for s in (0, 1) for h in (0, 1)]
        self.tree = {}
        for h, s in self.parts:

            def at(t, d, h=h, s=s):
                row = pl.ds((h * T + s) * self.size + d * q, q)
                return terms.at[t, :, row] if h else terms.at[:, t, row]

            self.tree[h, s] = Tree(
                net, "yz"[h], at, lambda d, h=h, s=s: far.at[h, s, d], lambda d, e, h=h, s=s: near.at[h, s, d, :, pl.ds(e * q, q)]
            )

    def start(self, h):
        for s in (0, 1):
            self.tree[h, s].start()

    def free(self, h):
        for s in (0, 1):
            for d in (0, 1):
                self.tree[h, s].free(d)

    def finish(self, out):
        net, size = self.net, self.size
        for part in self.parts:
            self.tree[part].relay()
        arrivals = []
        for h, s in self.parts:
            tree, mid = self.tree[h, s], self.mid.at[h, s]
            tree.end()
            row = pl.ds((h * T + s) * size, size)
            own = self.terms[tree.p, :, row] if h else self.terms[:, tree.p, row]
            mid[...] = own + self.near[h, s, 0] + self.near[h, s, 1]
            axis = "zy"[h]
            arrivals.append(exchange(net, axis, lambda t: mid.at[t], self.last.at[h, s]))
        for (h, s), copies in zip(self.parts, arrivals):
            for copy in copies:
                copy.wait_recv()
            p = net.y if h else net.z
            total = self.mid[h, s, p]
            for k in (1, 2, 3):
                total = total + self.last[h, s, ring(p, k)]
            out[pl.ds((h * T + s) * size, size)] = total


def exchange(net, axis, src, buf):
    p = getattr(net, axis)
    return [net.send(src(ring(p, k)), buf.at[p], net.near(axis, k)) for k in (2, 1, 3)]


def gather_nodes(net, buf):
    mine = buf.at[net.x * T + net.c]
    out = []
    for k in (2, 1, 3):
        out.append(net.send(mine, mine, net.near("x", k)))
        out.append(net.send(mine, mine, net.dev(x=ring(net.x, k), c=1 - net.c)))
    return out + [net.send(mine, mine, net.partner())]


def gather_pairs(net, buf):
    block = lambda k: buf.at[ring(net.x, k) * T + net.c]
    own = block(0)
    over = [net.send(own, own, net.partner())]
    come = [(k, net.send(own, own, net.near("x", k))) for k in (1, 3, 2)]
    for k, copy in come:
        copy.wait_recv()
        over.append(net.send(block(-k), block(-k), net.partner()))
    for copy in over:
        copy.wait_recv()


def gather_rep(net, buf):
    q = buf.shape[T] // G

    def move(s, u, v, device, part=None):
        h = s["h"]
        row = pl.ds(h * T * q, T * q) if part is None else pl.ds((h * T + part) * q, q)
        ref = buf.at[u, v, row] if h else buf.at[v, u, row]
        return net.send(ref, ref, device)

    state = []
    for h in (0, 1):
        first, second = ("y", "z") if h == 0 else ("z", "y")
        p, v = getattr(net, first), getattr(net, second)
        s = dict(h=h, p=p, v=v, up=net.near(second, 1), down=net.near(second, -1), over=[])
        s["near"] = [(k, move(s, p, v, net.near(first, k))) for k in (1, 3)]
        s["near"].append((T, move(s, p, v, net.near(first, T))))
        state.append(s)

    def cross(s, k):
        u = ring(s["p"], k)
        s["over"].append((u, move(s, u, s["v"], s["up"]), move(s, u, s["v"], s["down"])))

    for s in state:
        cross(s, 0)
    for n in range(3):
        for s in state:
            k, copy = s["near"][n]
            copy.wait_recv()
            cross(s, -k)
    last = []
    for n in range(G):
        for s in state:
            u, up, down = s["over"][n]
            up.wait_recv()
            last.append(move(s, u, ring(s["v"], -1), s["up"], 0))
            down.wait_recv()
            last.append(move(s, u, ring(s["v"], 1), s["down"], 1))
    for copy in last:
        copy.wait_recv()


def lanes(shape):
    return lax.broadcasted_iota(jnp.int32, shape, len(shape) - 1)


def pack(v):
    return v[:PK] + pltpu.roll(v[PK : T * PK], CLS, 1) + pltpu.roll(v[T * PK :], T * CLS, 1)


def unpack(v):
    keep = lanes((PK, LANE)) < CLS
    parts = [v, pltpu.roll(v, LANE - CLS, 1), pltpu.roll(v, LANE - T * CLS, 1)]
    return [jnp.where(keep, part, 0.0) for part in parts]


def scratch_shapes():
    half, piece = HID // T, ROW // G
    return dict(
        a_v=((TALL, WIDE), BF16),
        xg=((N, ROW, LANE), BF16),
        cg=((N, N, LANE), F32),
        y1=((WIDE, HID), BF16),
        zp=((G, G, ROW, HID), F32),
        far=((T, T, T, G, piece // T, HID), F32),
        near=((T, T, T, G, piece, HID), F32),
        mid=((T, T, G, piece, HID), F32),
        last=((T, T, G, piece, HID), F32),
        z1=((ROW, HID), F32),
        h1=((ROW, HID), BF16),
        w2p=((LANE, HID), F32),
        y2g=((N, PK, LANE), BF16),
        y2u=((WIDE, LANE), BF16),
        zq=((G, G, PK, LANE), F32),
        zi=((G, G, PK, LANE), F32),
        g2g=((G, G, PK, LANE), BF16),
        g2u=((TALL, LANE), BF16),
        d2=((G, piece, PAIR), F32),
        d2i=((G, piece, PAIR), F32),
        d2s=((T, piece, PAIR), F32),
        d2t=((PAIR, LANE), F32),
        g1g=((G, G, ROW, HID), BF16),
        e1=((G, HID, PAIR), F32),
        e1o=((G, half, PAIR), F32),
        e1s=((G, half, PAIR), F32),
        e1far=((T, half // T, PAIR), F32),
        e1near=((T, half, PAIR), F32),
        w2s=((T, piece, LANE), F32),
        w2o=((piece, LANE), F32),
        ra=((G, G, G * G, LANE), F32),
        rai=((G, G, G * G, LANE), F32),
        rx=((G, G * G, LANE), F32),
        rf=((T, G, G, G * G, LANE), F32),
    )


def kernel(adj, x_ref, w1_ref, w2_ref, lab_ref, msk_ref, out_ref, *scratch):
    names = list(scratch_shapes())
    s = dict(zip(names, scratch))
    send_sem, recv_sem, load_sem = scratch[len(names) :]
    net = Net(send_sem, recv_sem)
    z, y, x, c = net.z, net.y, net.x, net.c
    a_v = s["a_v"]

    tall = [pl.ds(k * (TALL // G), TALL // G) for k in range(G)]
    loads = [pltpu.make_async_copy(adj.at[rows], a_v.at[rows], load_sem.at[k]) for k, rows in enumerate(tall)]
    for load in loads:
        load.start()

    barrier = pltpu.get_barrier_semaphore()
    peers = net.peers()
    for peer in peers:
        pl.semaphore_signal(barrier, inc=1, device_id=peer, device_id_type=MESH)

    me = x * T + c
    xg, cg = s["xg"], s["cg"]
    xg[me] = x_ref[...]
    mask_row = msk_ref[...].astype(F32).reshape(1, ROW)
    label_row = lab_ref[...].reshape(1, ROW)
    cg[me] = jnp.broadcast_to(jnp.sum(mask_row, axis=1, keepdims=True), (N, LANE))
    w2p = s["w2p"]
    w2p[...] = jnp.zeros((LANE, HID), F32)
    w2p[:CLS] = w2_ref[...]
    w2b = w2p[...].astype(BF16)
    w1b = w1_ref[...].astype(BF16)

    pl.semaphore_wait(barrier, len(peers))

    counts = gather_nodes(net, cg)
    gather_pairs(net, xg)
    y1 = s["y1"]
    y1[...] = dot(xg[...].reshape(WIDE, LANE), w1b, 1, 0).astype(BF16)
    for load in loads:
        load.wait()

    zp = s["zp"]

    def block(zz, yy):
        return a_v[span((zz * G + yy) * ROW, ROW)]

    def z1_loop(count, place):
        def body(k, _):
            zz, yy = place(k)
            zp[zz, yy] = dot(block(zz, yy), y1[...], 1, 0)
            return _
        lax.fori_loop(0, count, body, 0)

    sum1 = RepSum(net, zp, s["far"], s["near"], s["mid"], s["last"])
    z1_loop(G, lambda k: (k, ring(y, 2)))
    sum1.start(0)
    z1_loop(3, lambda k: (ring(z, 2), ring(y, k - 1)))
    sum1.start(1)
    z1_loop(6, lambda k: (ring(z, k // 2 - 1), ring(y, 1 + 2 * (k % 2))))
    sum1.free(0)
    z1_loop(3, lambda k: (ring(z, k - 1), y))
    sum1.free(1)
    z1 = s["z1"]
    sum1.finish(z1)

    h1 = s["h1"]
    h1[...] = jnp.maximum(z1[...], 0.0).astype(BF16)
    y2 = dot(h1[...], w2b, 1, 1).astype(BF16).astype(F32)
    y2g, y2u = s["y2g"], s["y2u"]
    y2g[me] = pack(y2).astype(BF16)
    for copy in counts + gather_nodes(net, y2g):
        copy.wait_recv()

    def spread(src, dst, base):
        for g, part in enumerate(unpack(src.astype(F32))):
            dst[span(base * ROW + g * PK, PK)] = part.astype(BF16)

    def spread_y2(j, _):
        spread(y2g[j], y2u, j)
        return _

    lax.fori_loop(0, N, spread_y2, 0)

    zq, zi = s["zq"], s["zi"]
    count = jnp.sum(cg[...], axis=0)[:1]
    at_count = lanes((PK, LANE)) == 3 * CLS
    count = jnp.where(at_count, jnp.broadcast_to(count, (PK, LANE)), 0.0)

    def z2_block(zz, yy):
        zq[zz, yy] = pack(dot(block(zz, yy), y2u[...], 1, 0)) + count

    arrivals = net.rep_all(lambda zz, yy: zq.at[zz, yy], zi.at[z, y], z2_block)
    z2_block(z, y)
    zi[z, y] = zq[z, y]
    mask_all = jnp.broadcast_to(mask_row, (LANE, ROW)).T
    classes = lax.broadcasted_iota(jnp.int32, (LANE, ROW), 0)
    one_hot = (jnp.broadcast_to(label_row, (LANE, ROW)) == classes).astype(F32).T
    arrivals(lambda zz, yy: None)
    packed = jnp.sum(zi[...].reshape(G * G, PK, LANE), axis=0)

    total = jnp.sum(jnp.where(at_count, packed, 0.0), axis=1, keepdims=True)
    total = jnp.concatenate([total, total, total], axis=0)
    logits = jnp.concatenate(unpack(packed), axis=0)
    valid = lanes((ROW, LANE)) < CLS
    top = jnp.max(jnp.where(valid, logits, -jnp.inf), axis=1, keepdims=True)
    shifted = jnp.where(valid, logits - top, 0.0)
    norm = jnp.sum(jnp.where(valid, jnp.exp(shifted), 0.0), axis=1, keepdims=True)
    log_probs = shifted - jnp.log(norm)
    picked = jnp.where(valid, -(mask_all * (one_hot * log_probs)), 0.0)
    loss_part = jnp.sum(picked, axis=0, keepdims=True)
    g2 = jnp.where(valid, (jnp.exp(log_probs) - one_hot) * (mask_all / total), 0.0).astype(BF16).astype(F32)
    g2g, g2u = s["g2g"], s["g2u"]
    g2g[z, y] = pack(g2).astype(BF16)

    def spread_g2(zz, yy):
        spread(g2g[zz, yy], g2u, zz * G + yy)

    arrivals = net.rep_all(lambda zz, yy: g2g.at[z, y], g2g.at[z, y])
    spread_g2(z, y)
    arrivals(spread_g2)

    d2, d2i, d2s, d2t = (s[k] for k in ("d2", "d2i", "d2s", "d2t"))
    rows = d2.shape[1]

    def d2_block(k, _):
        part = dot(g2u[...], a_v[:, span(k * T * PAIR, T * PAIR)], 0, 0)
        d2[T * k] = part[:rows, :PAIR]
        d2[T * k + 1] = part[:rows, PAIR:]
        return _

    lax.fori_loop(0, T, d2_block, 0)
    for copy in exchange(net, "x", lambda t: d2.at[t], d2i):
        copy.wait_recv()
    d2i[x] = d2[x]
    d2s[c] = jnp.sum(d2i[...], axis=0)
    net.send(d2s.at[c], d2s.at[c], net.partner()).wait_recv()
    d2t[...] = jnp.concatenate([d2s[0] + d2s[1], jnp.zeros((LANE - rows, PAIR), F32)], axis=0).T
    dy2 = d2t[span(c * ROW, ROW)].astype(BF16)

    dh1 = dot(dy2, w2b, 1, 0)
    g1g = s["g1g"]
    g1g[z, y] = jnp.where(z1[...] > 0.0, dh1, 0.0).astype(BF16)

    dw2_t = dot(dy2, h1[...], 0, 0)[:CLS]
    loss_tile = jnp.concatenate([loss_part, jnp.zeros((N - 1, LANE), F32)], axis=0)
    w2s, w2o = s["w2s"], s["w2o"]
    for h in (0, 1):
        w2s[h, :CLS] = dw2_t[:, h * LANE : (h + 1) * LANE]
        w2s[h, CLS:] = loss_tile
    swap = net.send(w2s.at[1 - c], w2o, net.partner())

    gather_rep(net, g1g)
    swap.wait_recv()

    e1, e1o, e1s, e1far, e1near = (s[k] for k in ("e1", "e1o", "e1s", "e1far", "e1near"))
    half = HID // T
    q = half // T
    part = lambda d: pl.ds(d * q, q)
    tree = Tree(net, "x", lambda t, d: e1s.at[t, part(d)], lambda d: e1far.at[d], lambda d, e: e1near.at[d, part(e)])

    def e1_block(k):
        t = ring(x, k)
        e1[t] = dot(g1g[...].reshape(TALL, HID), a_v[:, span(t * PAIR, PAIR)], 0, 0)
        return t, net.send(e1.at[t, span((1 - c) * half, half)], e1o.at[t], net.partner())

    def e1_join(t, copy):
        copy.wait_recv()
        e1s[t] = e1[t, span(c * half, half)] + e1o[t]

    opposite = e1_block(2)
    right = e1_block(1)
    e1_join(*opposite)
    tree.start()
    left = e1_block(3)
    e1_join(*right)
    tree.free(0)
    own = e1_block(0)
    e1_join(*left)
    tree.free(1)
    tree.relay()
    e1_join(*own)
    tree.end()
    dy1 = (e1s[x] + e1near[0] + e1near[1]).astype(BF16)
    dw1_t = dot(dy1, xg[pl.ds(x * T, T)].reshape(PAIR, LANE), 1, 0)

    ra, rai, rx, rf = (s[k] for k in ("ra", "rai", "rx", "rf"))
    tile = G * G
    ra[:T] = dw1_t.reshape(T, G, tile, LANE)
    ra[T, :3] = (w2s[c] + w2o[...]).reshape(3, tile, LANE)
    ra[T, 3] = jnp.zeros((tile, LANE), F32)
    ra[3] = jnp.zeros((G, tile, LANE), F32)
    arrivals = net.rep_all(lambda zz, yy: ra.at[zz, yy], rai.at[z, y])
    rai[z, y] = ra[z, y]
    arrivals(lambda zz, yy: None)
    rx[x] = jnp.sum(rai[...].reshape(tile, tile, LANE), axis=0)
    for copy in exchange(net, "x", lambda t: rx.at[x], rx):
        copy.wait_recv()
    rf[c, z, y] = jnp.sum(rx[...], axis=0)
    arrivals = net.rep_all(lambda zz, yy: rf.at[c, z, y], rf.at[c, z, y])
    arrivals(lambda zz, yy: None)
    net.send(rf.at[c], rf.at[c], net.partner()).wait_recv()

    out_ref[...] = rf[:, :3].reshape(T, 3 * G * tile, LANE)
    out_ref[0, span(3 * G * tile - N, N)] = jnp.broadcast_to(total[:1], (N, LANE))
    for end in net.ends:
        end()


def unpack_kernel(sums, loss_ref, dw1_ref, dw2_ref):
    for h in (0, 1):
        half = span(h * LANE, LANE)
        dw1_ref[:, half] = sums[h, :LANE].T
        dw2_ref[:, half] = sums[h, LANE : LANE + CLS]
    loss = jnp.sum(sums[0, LANE + CLS : LANE + CLS + N])
    loss_ref[0, 0] = loss / jnp.max(sums[0, sums.shape[1] - N :])


def solution(mesh):
    vmem, smem = pl.BlockSpec(memory_space=pltpu.VMEM), pl.BlockSpec(memory_space=pltpu.SMEM)
    struct = lambda *shape: jax.ShapeDtypeStruct(shape, F32)

    def device_step(adj_blk, feat_blk, w_one, w_two, label_blk, mask_blk):
        sems = [pltpu.SemaphoreType.DMA((n,)) for n in (N_SEM, N_SEM, G)]
        sums = pl.pallas_call(
            kernel,
            out_shape=struct(T, 3 * G * G * G, LANE),
            in_specs=[pl.BlockSpec(memory_space=pl.ANY)] + [vmem] * 5,
            out_specs=vmem,
            scratch_shapes=[pltpu.VMEM(shape, dtype) for shape, dtype in scratch_shapes().values()] + sems,
            compiler_params=pltpu.CompilerParams(collective_id=0, has_side_effects=True, vmem_limit_bytes=56 << 20),
        )(adj_blk.reshape(TALL, WIDE), feat_blk, w_one, w_two.T, label_blk, mask_blk)
        loss, dw1, dw2 = pl.pallas_call(
            unpack_kernel,
            out_shape=(struct(1, 1), struct(LANE, HID), struct(CLS, HID)),
            in_specs=[vmem],
            out_specs=(smem, vmem, vmem),
        )(sums)
        return loss.reshape(()), dw1, dw2.T

    row_spec = P(("rep", "nodes"))
    return jax.shard_map(
        device_step,
        mesh=mesh,
        in_specs=(P(None, "nodes", "rep"), row_spec, P(), P(), row_spec, row_spec),
        out_specs=(P(), P(), P()),
        check_vma=False,
    )
```

```python
import jax
import jax.numpy as jnp
from jax import lax
from jax.experimental import pallas as pl
from jax.experimental.pallas import tpu as pltpu
from jax.sharding import PartitionSpec as P

MESH = pl.DeviceIdType.MESH
F32, BF16 = jnp.float32, jnp.bfloat16
T, G, N = 2, 4, 8
LANE, HID, CLS, ROW = 128, 256, 40, 192
PK = ROW // 3
TALL, WIDE = 16 * ROW, N * ROW
PAIR = T * ROW
N_SEM = 320


def ring(v, k):
    return (v + k + G) % G


def dot(a, b, ca, cb):
    return lax.dot_general(a, b, (((ca,), (cb,)), ((), ())), preferred_element_type=F32)


def span(start, size):
    return pl.ds(start if isinstance(start, int) else pl.multiple_of(start, size), size)


class Net:
    def __init__(self, send_sem, recv_sem):
        rep, node = lax.axis_index("rep"), lax.axis_index("nodes")
        self.z, self.y, self.x, self.c = rep // G, rep % G, node // T, node % T
        self.sems, self.used, self.ends = (send_sem, recv_sem), 0, []

    def dev(self, **place):
        z, y, x, c = (place.get(k, getattr(self, k)) for k in "zyxc")
        return (z * G + y, x * T + c)

    def near(self, axis, k):
        return self.dev(**{axis: ring(getattr(self, axis), k)})

    def partner(self):
        return self.dev(c=1 - self.c)

    def copy(self, src, dst, device, k):
        send, recv = (sem.at[k] for sem in self.sems)
        return pltpu.make_async_remote_copy(src_ref=src, dst_ref=dst, send_sem=send, recv_sem=recv, device_id=device, device_id_type=MESH)

    def send(self, src, dst, device):
        copy = self.copy(src, dst, device, self.used)
        self.used += 1
        copy.start()
        self.ends.append(copy.wait_send)
        return copy

    def rep_all(self, src, dst, before=None, flip=False):
        base, self.used = self.used, self.used + G * G
        count = G * G if flip else G * G - 1
        core = 1 - self.c if flip else self.c

        def place(j, sign):
            k = ((j + 1) * 5) % (G * G)
            return ring(self.z, sign * (k // G)), ring(self.y, sign * (k % G)), base + k

        def start(j, _):
            z, y, k = place(j, 1)
            if before is not None:
                before(z, y)
            self.copy(src(z, y), dst, self.dev(z=z, y=y, c=core), k).start()
            return _

        def each(fn):
            def body(j, _):
                z, y, k = place(j, -1)
                self.copy(dst, dst, self.dev(z=z, y=y, c=core), k).wait_recv()
                fn(z, y)
                return _
            lax.fori_loop(0, count, body, 0)

        def end(j, _):
            z, y, k = place(j, 1)
            self.copy(dst, dst, self.dev(z=z, y=y, c=core), k).wait_send()
            return _

        lax.fori_loop(0, count, start, 0)
        self.ends.append(lambda: lax.fori_loop(0, count, end, 0))
        return each

    def peers(self):
        out = [self.partner()]
        for k in (1, 2, 3):
            out += [self.near(axis, k) for axis in "xyz"]
            out.append(self.dev(x=ring(self.x, k), c=1 - self.c))
        return out


class Tree:
    def __init__(self, net, axis, at, far, near):
        self.net, self.at, self.far, self.near = net, at, far, near
        self.p = getattr(net, axis)
        self.side = net.near(axis, 1), net.near(axis, -1)

    def start(self):
        self.first = [self.net.send(self.at(ring(self.p, T), d), self.far(d), self.side[d]) for d in (0, 1)]
        self.arrive = []

    def free(self, d):
        t = ring(self.p, 1 - T * d)
        self.arrive.append(self.net.send(self.at(t, 1 - d), self.near(d, 1 - d), self.side[d]))

    def relay(self):
        for d in (0, 1):
            self.first[d].wait_recv()
            mine = self.at(ring(self.p, 1 - T * d), d)
            mine[...] = mine[...] + self.far(d)[...]
            self.arrive.append(self.net.send(mine, self.near(d, d), self.side[d]))

    def end(self):
        for copy in self.arrive:
            copy.wait_recv()


class RepSum:
    def __init__(self, net, terms, far, near, mid, last):
        self.net, self.terms, self.near, self.mid, self.last = net, terms, near, mid, last
        self.size, slices = near.shape[-T], near.shape[1]
        self.slices = range(slices)
        q = self.size // T
        self.parts = [(h, s) for s in self.slices for h in (0, 1)]
        self.tree = {}
        for h, s in self.parts:

            def at(t, d, h=h, s=s):
                row = pl.ds((h * slices + s) * self.size + d * q, q)
                return terms.at[t, :, row] if h else terms.at[:, t, row]

            self.tree[h, s] = Tree(
                net, "yz"[h], at, lambda d, h=h, s=s: far.at[h, s, d], lambda d, e, h=h, s=s: near.at[h, s, d, :, pl.ds(e * q, q)]
            )

    def start(self, h):
        for s in self.slices:
            self.tree[h, s].start()

    def free(self, h):
        for s in self.slices:
            for d in (0, 1):
                self.tree[h, s].free(d)

    def finish(self, out):
        net, size = self.net, self.size
        for part in self.parts:
            self.tree[part].relay()
        arrivals = []
        for h, s in self.parts:
            tree, mid = self.tree[h, s], self.mid.at[h, s]
            tree.end()
            row = pl.ds((h * len(self.slices) + s) * size, size)
            own = self.terms[tree.p, :, row] if h else self.terms[:, tree.p, row]
            mid[...] = own + self.near[h, s, 0] + self.near[h, s, 1]
            axis = "zy"[h]
            arrivals.append(exchange(net, axis, lambda t: mid.at[t], self.last.at[h, s]))
        for (h, s), copies in zip(self.parts, arrivals):
            for copy in copies:
                copy.wait_recv()
            p = net.y if h else net.z
            total = self.mid[h, s, p]
            for k in (1, 2, 3):
                total = total + self.last[h, s, ring(p, k)]
            out[pl.ds((h * len(self.slices) + s) * size, size)] = total


def exchange(net, axis, src, buf):
    p = getattr(net, axis)
    return [net.send(src(ring(p, k)), buf.at[p], net.near(axis, k)) for k in (2, 1, 3)]


def wait_all(copies):
    for copy in copies:
        copy.wait_recv()


def gather_nodes(net, buf):
    node = lambda k, core: ring(net.x, k) * T + core
    mine = buf.at[node(0, net.c)]
    other = 1 - net.c
    out = []
    for k in (2, 1, 3):
        out.append((node(-k, net.c), net.send(mine, mine, net.near("x", k))))
        out.append((node(-k, other), net.send(mine, mine, net.dev(x=ring(net.x, k), c=other))))
    return [(node(0, other), net.send(mine, mine, net.partner()))] + out


def gather_pairs(net, buf, done):
    node = lambda k, core: ring(net.x, k) * T + core
    other = 1 - net.c

    def move(n, device):
        return net.send(buf.at[n], buf.at[n], device)

    me = node(0, net.c)
    over = [(node(0, other), move(me, net.partner()))]
    come = [(k, move(me, net.dev(x=ring(net.x, k), c=other))) for k in (2, 1, 3)]
    done(me)
    for k, copy in come:
        copy.wait_recv()
        over.append((node(-k, net.c), move(node(-k, other), net.partner())))
        done(node(-k, other))
    for n, copy in over:
        copy.wait_recv()
        done(n)


def gather_rep(net, buf, early):
    q = buf.shape[T] // G

    def move(s, u, v, device, part=None):
        h = s["h"]
        row = pl.ds(h * T * q, T * q) if part is None else pl.ds((h * T + part) * q, q)
        ref = buf.at[u, v, row] if h else buf.at[v, u, row]
        return net.send(ref, ref, device)

    state = []
    for h in (0, 1):
        first, second = ("y", "z") if h == 0 else ("z", "y")
        p, v = getattr(net, first), getattr(net, second)
        s = dict(h=h, p=p, v=v, up=net.near(second, 1), down=net.near(second, -1), over=[])
        s["near"] = [(k, move(s, p, v, net.near(first, k))) for k in (1, 3)]
        s["near"].append((T, move(s, p, v, net.near(first, T))))
        state.append(s)

    def cross(s, k):
        u = ring(s["p"], k)
        s["over"].append((u, move(s, u, s["v"], s["up"]), move(s, u, s["v"], s["down"])))

    for s in state:
        cross(s, 0)
    extra = early()
    for n in range(3):
        for s in state:
            k, copy = s["near"][n]
            copy.wait_recv()
            cross(s, -k)
    last = []
    for n in range(G):
        for s in state:
            u, up, down = s["over"][n]
            up.wait_recv()
            last.append(move(s, u, ring(s["v"], -1), s["up"], 0))
            down.wait_recv()
            last.append(move(s, u, ring(s["v"], 1), s["down"], 1))
    wait_all(last)
    return extra


def lanes(shape):
    return lax.broadcasted_iota(jnp.int32, shape, len(shape) - 1)


def pack(v):
    return v[:PK] + pltpu.roll(v[PK : T * PK], CLS, 1) + pltpu.roll(v[T * PK :], T * CLS, 1)


def unpack(v):
    keep = lanes((PK, LANE)) < CLS
    parts = [v, pltpu.roll(v, LANE - CLS, 1), pltpu.roll(v, LANE - T * CLS, 1)]
    return [jnp.where(keep, part, 0.0) for part in parts]


def scratch_shapes():
    half, thin, piece = HID // T, ROW // 6, CLS + N
    return dict(
        a_v=((TALL, WIDE), BF16),
        xg=((N, ROW, LANE), BF16),
        cg=((N, N, LANE), F32),
        y1=((WIDE, HID), BF16),
        zp=((G, G, ROW, HID), F32),
        far=((T, 3, T, G, thin // T, HID), F32),
        near=((T, 3, T, G, thin, HID), F32),
        mid=((T, 3, G, thin, HID), F32),
        last=((T, 3, G, thin, HID), F32),
        z1=((ROW, HID), F32),
        h1=((ROW, HID), BF16),
        w2p=((LANE, HID), F32),
        y2g=((N, PK, LANE), BF16),
        y2u=((WIDE, LANE), BF16),
        zq=((G, G, PK, LANE), F32),
        zi=((G, G, PK, LANE), F32),
        g2s=((PK, LANE), BF16),
        g2g=((G, G, PK, LANE), BF16),
        g2u=((TALL, LANE), BF16),
        d2=((G, CLS, PAIR), F32),
        d2i=((G, CLS, PAIR), F32),
        d2s=((T, CLS, PAIR), F32),
        d2t=((PAIR, LANE), F32),
        g1g=((G, G, ROW, HID), BF16),
        e1=((G, HID, PAIR), F32),
        e1o=((G, half, PAIR), F32),
        e1s=((G, half, PAIR), F32),
        e1far=((T, half // T, PAIR), F32),
        e1near=((T, half, PAIR), F32),
        w2s=((T, piece, LANE), F32),
        w2o=((piece, LANE), F32),
        wx=((G, piece, LANE), F32),
        wr=((G, G, piece, LANE), F32),
        wf=((T, piece, LANE), F32),
        ra=((G, G, N, LANE), F32),
        rai=((G, G, N, LANE), F32),
        rx=((N, LANE), F32),
        rxi=((G, N, LANE), F32),
        rs=((N, LANE), F32),
        rf=((T, G, G, N, LANE), F32),
        w1v=((LANE, HID), F32),
        lab=((ROW,), jnp.int32),
        msk=((ROW,), jnp.int32),
        lab_o=((ROW,), jnp.int32),
        msk_o=((ROW,), jnp.int32),
    )


def kernel(adj, x_ref, w1_ref, w2_ref, lab_ref, msk_ref, out_ref, *scratch):
    names = list(scratch_shapes())
    s = dict(zip(names, scratch))
    send_sem, recv_sem, load_sem = scratch[len(names) :]
    net = Net(send_sem, recv_sem)
    z, y, x, c = net.z, net.y, net.x, net.c
    a_v = s["a_v"]

    barrier = pltpu.get_barrier_semaphore()
    peers = net.peers()
    for peer in peers:
        pl.semaphore_signal(barrier, inc=1, device_id=peer, device_id_type=MESH)

    me = x * T + c
    xg, cg, w2p, w1v, y1 = (s[k] for k in ("xg", "cg", "w2p", "w1v", "y1"))
    tall = [pl.ds(k * (TALL // G), TALL // G) for k in range(G)]
    w2p[...] = jnp.zeros((LANE, HID), F32)
    pairs = [(msk_ref, s["msk"]), (lab_ref, s["lab"]), (x_ref, xg.at[me]), (w1_ref, w1v), (w2_ref, w2p.at[pl.ds(0, CLS)])]
    pairs += [(adj.at[rows], a_v.at[rows]) for rows in tall]
    loads = [pltpu.make_async_copy(src, dst, load_sem.at[k]) for k, (src, dst) in enumerate(pairs)]
    for load in loads:
        load.start()
    small = len(loads) - G
    for load in loads[:small]:
        load.wait()

    def row_of(ref, dtype):
        return ref[...].astype(dtype).reshape(1, ROW)

    cg[me] = jnp.broadcast_to(jnp.sum(row_of(s["msk"], F32), axis=1, keepdims=True), (N, LANE))
    w2b = w2p[...].astype(BF16)
    w1b = w1v[...].astype(BF16)

    pl.semaphore_wait(barrier, len(peers))

    swaps = [net.send(s[k], s[k + "_o"], net.partner()) for k in ("lab", "msk")]
    counts = [copy for _, copy in gather_nodes(net, cg)]

    def y1_block(n):
        y1[span(n * ROW, ROW)] = dot(xg[n], w1b, 1, 0).astype(BF16)

    gather_pairs(net, xg, y1_block)
    for load in loads[small:]:
        load.wait()

    zp = s["zp"]

    def block(zz, yy):
        return a_v[span((zz * G + yy) * ROW, ROW)]

    def z1_loop(count, place):
        def body(k, _):
            zz, yy = place(k)
            zp[zz, yy] = dot(block(zz, yy), y1[...], 1, 0)
            return _
        lax.fori_loop(0, count, body, 0)

    sum1 = RepSum(net, zp, s["far"], s["near"], s["mid"], s["last"])
    z1_loop(G, lambda k: (k, ring(y, 2)))
    sum1.start(0)
    z1_loop(3, lambda k: (ring(z, 2), ring(y, k - 1)))
    sum1.start(1)
    z1_loop(6, lambda k: (ring(z, k // 2 - 1), ring(y, 1 + 2 * (k % 2))))
    sum1.free(0)
    z1_loop(3, lambda k: (ring(z, k - 1), y))
    sum1.free(1)
    z1 = s["z1"]
    sum1.finish(z1)

    h1 = s["h1"]
    h1[...] = jnp.maximum(z1[...], 0.0).astype(BF16)
    y2 = dot(h1[...], w2b, 1, 1).astype(BF16).astype(F32)
    y2g, y2u = s["y2g"], s["y2u"]
    y2g[me] = pack(y2).astype(BF16)
    blocks = gather_nodes(net, y2g)

    def spread(src, dst, base):
        for g, part in enumerate(unpack(src.astype(F32))):
            dst[span(base * ROW + g * PK, PK)] = part.astype(BF16)

    spread(y2g[me], y2u, me)
    wait_all(counts + swaps)
    for n, copy in blocks:
        copy.wait_recv()
        spread(y2g[n], y2u, n)

    zq, zi = s["zq"], s["zi"]
    count = jnp.sum(cg[...], axis=0)[:1]
    at_count = lanes((PK, LANE)) == 3 * CLS
    count = jnp.where(at_count, jnp.broadcast_to(count, (PK, LANE)), 0.0)

    def z2_block(zz, yy):
        zq[zz, yy] = pack(dot(block(zz, yy), y2u[...], 1, 0)) + count

    arrivals = net.rep_all(lambda zz, yy: zq.at[zz, yy], zi.at[z, y], z2_block, flip=True)
    mask_row, label_row = row_of(s["msk_o"], F32), row_of(s["lab_o"], jnp.int32)
    mask_all = jnp.broadcast_to(mask_row, (LANE, ROW)).T
    classes = lax.broadcasted_iota(jnp.int32, (LANE, ROW), 0)
    one_hot = (jnp.broadcast_to(label_row, (LANE, ROW)) == classes).astype(F32).T
    arrivals(lambda zz, yy: None)
    packed = jnp.sum(zi[...].reshape(G * G, PK, LANE), axis=0)

    total = jnp.sum(jnp.where(at_count, packed, 0.0), axis=1, keepdims=True)
    total = jnp.concatenate([total, total, total], axis=0)
    logits = jnp.concatenate(unpack(packed), axis=0)
    valid = lanes((ROW, LANE)) < CLS
    top = jnp.max(jnp.where(valid, logits, -jnp.inf), axis=1, keepdims=True)
    shifted = jnp.where(valid, logits - top, 0.0)
    norm = jnp.sum(jnp.where(valid, jnp.exp(shifted), 0.0), axis=1, keepdims=True)
    log_probs = shifted - jnp.log(norm)
    picked = jnp.where(valid, -(mask_all * (one_hot * log_probs)), 0.0)
    loss_part = jnp.sum(picked, axis=0, keepdims=True)
    g2 = jnp.where(valid, (jnp.exp(log_probs) - one_hot) * (mask_all / total), 0.0).astype(BF16).astype(F32)
    g2s, g2g, g2u = s["g2s"], s["g2g"], s["g2u"]
    g2s[...] = pack(g2).astype(BF16)

    def spread_g2(zz, yy):
        spread(g2g[zz, yy], g2u, zz * G + yy)

    arrivals = net.rep_all(lambda zz, yy: g2s, g2g.at[z, y], flip=True)
    arrivals(spread_g2)

    d2, d2i, d2s, d2t = (s[k] for k in ("d2", "d2i", "d2s", "d2t"))

    def d2_block(k):
        part = dot(g2u[...], a_v[:, span(k * T * PAIR, T * PAIR)], 0, 0)[:CLS]
        d2[T * k] = part[:, :PAIR]
        d2[T * k + 1] = part[:, PAIR:]

    def d2_send(t):
        return net.send(d2.at[t], d2i.at[x], net.dev(x=t, c=1 - c))

    d2_block(1 - x // T)
    copies = [d2_send(ring(x, T)), d2_send(3 - x)]
    d2_block(x // T)
    copies.append(d2_send(x + 1 - T * (x % T)))
    d2i[x] = d2[x]
    wait_all(copies)
    d2s[c] = jnp.sum(d2i[...], axis=0)
    net.send(d2s.at[c], d2s.at[c], net.partner()).wait_recv()
    d2t[...] = jnp.concatenate([d2s[0] + d2s[1], jnp.zeros((LANE - CLS, PAIR), F32)], axis=0).T
    dy2 = d2t[span(c * ROW, ROW)].astype(BF16)

    dh1 = dot(dy2, w2b, 1, 0)
    g1g = s["g1g"]
    g1g[z, y] = jnp.where(z1[...] > 0.0, dh1, 0.0).astype(BF16)

    dw2_t = dot(dy2, h1[...], 0, 0)[:CLS]
    loss_tile = jnp.concatenate([loss_part, jnp.zeros((N - 1, LANE), F32)], axis=0)
    w2s, w2o = s["w2s"], s["w2o"]
    for h in (0, 1):
        w2s[h, :CLS] = dw2_t[:, h * LANE : (h + 1) * LANE]
        w2s[h, CLS:] = loss_tile
    swap = net.send(w2s.at[1 - c], w2o, net.partner())
    wx, wr, wf = s["wx"], s["wr"], s["wf"]

    def early():
        swap.wait_recv()
        wx[x] = w2s[c] + w2o[...]
        return exchange(net, "x", lambda t: wx.at[x], wx)

    wait_all(gather_rep(net, g1g, early))
    wr[z, y] = jnp.sum(wx[...], axis=0)
    w_arrivals = net.rep_all(lambda zz, yy: wr.at[z, y], wr.at[z, y])

    e1, e1o, e1s, e1far, e1near = (s[k] for k in ("e1", "e1o", "e1s", "e1far", "e1near"))
    half = HID // T
    q = half // T
    part = lambda d: pl.ds(d * q, q)
    tree = Tree(net, "x", lambda t, d: e1s.at[t, part(d)], lambda d: e1far.at[d], lambda d, e: e1near.at[d, part(e)])

    def e1_block(k):
        t = ring(x, k)
        e1[t] = dot(g1g[...].reshape(TALL, HID), a_v[:, span(t * PAIR, PAIR)], 0, 0)
        return t, net.send(e1.at[t, span((1 - c) * half, half)], e1o.at[t], net.partner())

    def e1_join(t, copy):
        copy.wait_recv()
        e1s[t] = e1[t, span(c * half, half)] + e1o[t]

    opposite = e1_block(2)
    right = e1_block(1)
    e1_join(*opposite)
    tree.start()
    left = e1_block(3)
    e1_join(*right)
    tree.free(0)
    own = e1_block(0)
    e1_join(*left)
    tree.free(1)
    tree.relay()
    e1_join(*own)
    w_arrivals(lambda zz, yy: None)
    wf[c] = jnp.sum(wr[...].reshape(G * G, CLS + N, LANE), axis=0)
    swap = net.send(wf.at[c], wf.at[c], net.partner())
    tree.end()
    dy1 = (e1s[x] + e1near[0] + e1near[1]).astype(BF16)
    dw1_t = dot(dy1, xg[pl.ds(x * T, T)].reshape(PAIR, LANE), 1, 0)

    ra, rai, rx, rxi, rs, rf = (s[k] for k in ("ra", "rai", "rx", "rxi", "rs", "rf"))
    ra[...] = dw1_t.reshape(G, G, N, LANE)
    arrivals = net.rep_all(lambda zz, yy: ra.at[zz, yy], rai.at[z, y], flip=True)
    arrivals(lambda zz, yy: None)
    rx[...] = jnp.sum(rai[...].reshape(G * G, N, LANE), axis=0)
    wait_all([net.send(rx, rxi.at[x], net.dev(x=ring(x, k), c=1 - c)) for k in (2, 1, 3, 0)])
    rs[...] = jnp.sum(rxi[...], axis=0)
    arrivals = net.rep_all(lambda zz, yy: rs, rf.at[c, z, y], flip=True)
    swap.wait_recv()
    out_ref[:, span(LANE, CLS + N)] = wf[...]
    out_ref[0, span(LANE + CLS + N, N)] = jnp.broadcast_to(total[:1], (N, LANE))
    arrivals(lambda zz, yy: None)
    net.send(rf.at[1 - c], rf.at[1 - c], net.partner()).wait_recv()
    out_ref[:, :LANE] = rf[...].reshape(T, LANE, LANE)
    for end in net.ends:
        end()


def unpack_kernel(sums, loss_ref, dw1_ref, dw2_ref):
    for h in (0, 1):
        half = span(h * LANE, LANE)
        dw1_ref[:, half] = sums[h, :LANE].T
        dw2_ref[:, half] = sums[h, LANE : LANE + CLS]
    loss = jnp.sum(sums[0, LANE + CLS : LANE + CLS + N])
    loss_ref[0, 0] = loss / jnp.max(sums[0, LANE + CLS + N :])


def solution(mesh):
    vmem, smem = pl.BlockSpec(memory_space=pltpu.VMEM), pl.BlockSpec(memory_space=pltpu.SMEM)
    struct = lambda *shape: jax.ShapeDtypeStruct(shape, F32)

    def device_step(adj_blk, feat_blk, w_one, w_two, label_blk, mask_blk):
        sems = [pltpu.SemaphoreType.DMA((n,)) for n in (N_SEM, N_SEM, N + 1)]
        sums = pl.pallas_call(
            kernel,
            out_shape=struct(T, LANE + CLS + T * N, LANE),
            in_specs=[pl.BlockSpec(memory_space=pl.ANY)] * 6,
            out_specs=vmem,
            scratch_shapes=[pltpu.VMEM(shape, dtype) for shape, dtype in scratch_shapes().values()] + sems,
            compiler_params=pltpu.CompilerParams(collective_id=0, has_side_effects=True, vmem_limit_bytes=56 << 20),
        )(adj_blk.reshape(TALL, WIDE), feat_blk, w_one, w_two.T, label_blk, mask_blk)
        loss, dw1, dw2 = pl.pallas_call(
            unpack_kernel,
            out_shape=(struct(1, 1), struct(LANE, HID), struct(CLS, HID)),
            in_specs=[vmem],
            out_specs=(smem, vmem, vmem),
        )(sums)
        return loss.reshape(()), dw1, dw2.T

    row_spec = P(("rep", "nodes"))
    return jax.shard_map(
        device_step,
        mesh=mesh,
        in_specs=(P(None, "nodes", "rep"), row_spec, P(), P(), row_spec, row_spec),
        out_specs=(P(), P(), P()),
        check_vma=False,
    )
```

```python
import jax
import jax.numpy as jnp
from jax import lax
from jax.experimental import pallas as pl
from jax.experimental.pallas import tpu as pltpu
from jax.sharding import PartitionSpec as P

MESH = pl.DeviceIdType.MESH
F32, BF16 = jnp.float32, jnp.bfloat16
T, G, N = 2, 4, 8
LANE, HID, CLS, ROW = 128, 256, 40, 192
PK = ROW // 3
TALL, WIDE = 16 * ROW, N * ROW
PAIR = T * ROW
N_SEND, N_RECV = 61, 90


def ring(v, k):
    return (v + k + G) % G


def dot(a, b, ca, cb):
    return lax.dot_general(a, b, (((ca,), (cb,)), ((), ())), preferred_element_type=F32)


def span(start, size):
    return pl.ds(start if isinstance(start, int) else pl.multiple_of(start, size), size)


class Net:
    def __init__(self, send_sem, recv_sem):
        rep, node = lax.axis_index("rep"), lax.axis_index("nodes")
        self.z, self.y, self.x, self.c = rep // G, rep % G, node // T, node % T
        self.send_sem, self.recv_sem = send_sem, recv_sem
        self.used, self.spare, self.ends = 0, [], []

    def dev(self, **place):
        z, y, x, c = (place.get(k, getattr(self, k)) for k in "zyxc")
        return (z * G + y, x * T + c)

    def near(self, axis, k):
        return self.dev(**{axis: ring(getattr(self, axis), k)})

    def partner(self):
        return self.dev(c=1 - self.c)

    def recv_index(self):
        if self.spare:
            return self.spare.pop()
        self.used += 1
        return self.used - 1

    def copy(self, src, dst, device, k, n):
        send, recv = self.send_sem.at[k], self.recv_sem.at[n]
        return pltpu.make_async_remote_copy(src_ref=src, dst_ref=dst, send_sem=send, recv_sem=recv, device_id=device, device_id_type=MESH)

    def send(self, src, dst, device):
        copy = self.copy(src, dst, device, len(self.ends), self.recv_index())
        copy.start()
        self.ends.append(copy)
        return copy

    def flush(self):
        for copy in self.ends:
            copy.wait_send()
        self.ends = []

    def rep_all(self, src, buf):
        k, n = len(self.ends), self.recv_index()
        mine = buf.at[self.z, self.y]
        whole = self.copy(buf, buf, self.partner(), k, n)
        self.ends.append(whole)

        def start(dz, dy):
            z, y = ring(self.z, dz), ring(self.y, dy)
            self.copy(src(z, y), mine, self.dev(z=z, y=y, c=1 - self.c), k, n).start()

        return start, whole

    def rep_send(self, src, buf):
        start, whole = self.rep_all(src, buf)
        for j in range(G * G):
            k = (j + 1) * 5 % (G * G)
            start(k // G, k % G)
        return whole

    def peers(self):
        out = [self.partner()]
        for k in (1, 2, 3):
            out += [self.near(axis, k) for axis in "xyz"]
            out.append(self.dev(x=ring(self.x, k), c=1 - self.c))
        return out


class Tree:
    def __init__(self, net, axis, at, far, near):
        self.net, self.at, self.far, self.near = net, at, far, near
        self.p = getattr(net, axis)
        self.side = net.near(axis, 1), net.near(axis, -1)

    def start(self):
        self.first = [self.net.send(self.at(ring(self.p, T), d), self.far(d), self.side[d]) for d in (0, 1)]
        self.arrive = []

    def free(self, d):
        t = ring(self.p, 1 - T * d)
        self.arrive.append(self.net.send(self.at(t, 1 - d), self.near(d, 1 - d), self.side[d]))

    def relay(self):
        for d in (0, 1):
            self.first[d].wait_recv()
            mine = self.at(ring(self.p, 1 - T * d), d)
            mine[...] = mine[...] + self.far(d)[...]
            self.arrive.append(self.net.send(mine, self.near(d, d), self.side[d]))

    def end(self):
        for copy in self.arrive:
            copy.wait_recv()


class RepSum:
    def __init__(self, net, terms, far, near, mid, last):
        self.net, self.terms, self.near, self.mid, self.last = net, terms, near, mid, last
        self.size, slices = near.shape[-T], near.shape[1]
        self.slices = range(slices)
        q = self.size // T
        self.parts = [(h, s) for s in self.slices for h in (0, 1)]
        self.tree = {}
        for h, s in self.parts:

            def at(t, d, h=h, s=s):
                row = pl.ds((h * slices + s) * self.size + d * q, q)
                return terms.at[t, :, row] if h else terms.at[:, t, row]

            self.tree[h, s] = Tree(
                net, "yz"[h], at, lambda d, h=h, s=s: far.at[h, s, d], lambda d, e, h=h, s=s: near.at[h, s, d, :, pl.ds(e * q, q)]
            )

    def start(self, h):
        for s in self.slices:
            self.tree[h, s].start()

    def free(self, h, d):
        for s in self.slices:
            self.tree[h, s].free(d)

    def finish(self, out):
        net, size = self.net, self.size
        for part in self.parts:
            self.tree[part].relay()
        arrivals = []
        for h, s in self.parts:
            tree, mid = self.tree[h, s], self.mid.at[h, s]
            tree.end()
            row = pl.ds((h * len(self.slices) + s) * size, size)
            own = self.terms[tree.p, :, row] if h else self.terms[:, tree.p, row]
            mid[...] = own + self.near[h, s, 0] + self.near[h, s, 1]
            axis = "zy"[h]
            arrivals.append(exchange(net, axis, lambda t: mid.at[t], self.last.at[h, s]))
        for (h, s), copies in zip(self.parts, arrivals):
            for copy in copies:
                copy.wait_recv()
            p = net.y if h else net.z
            total = self.mid[h, s, p]
            for k in (1, 2, 3):
                total = total + self.last[h, s, ring(p, k)]
            out[pl.ds((h * len(self.slices) + s) * size, size)] = total


def exchange(net, axis, src, buf):
    p = getattr(net, axis)
    return [net.send(src(ring(p, k)), buf.at[p], net.near(axis, k)) for k in (2, 1, 3)]


def wait_all(copies):
    for copy in copies:
        copy.wait_recv()


def gather_nodes(net, buf):
    node = lambda k, core: ring(net.x, k) * T + core
    mine = buf.at[node(0, net.c)]
    other = 1 - net.c
    out = []
    for k in (2, 1, 3):
        out.append((node(-k, net.c), net.send(mine, mine, net.near("x", k))))
        out.append((node(-k, other), net.send(mine, mine, net.dev(x=ring(net.x, k), c=other))))
    return [(node(0, other), net.send(mine, mine, net.partner()))] + out


def gather_pairs(net, buf, done):
    node = lambda k, core: ring(net.x, k) * T + core
    other = 1 - net.c

    def move(n, device):
        return net.send(buf.at[n], buf.at[n], device)

    me = node(0, net.c)
    over = [(node(0, other), move(me, net.partner()))]
    come = [(k, move(me, net.dev(x=ring(net.x, k), c=other))) for k in (2, 1, 3)]
    done(me)
    for k, copy in come:
        copy.wait_recv()
        over.append((node(-k, net.c), move(node(-k, other), net.partner())))
        done(node(-k, other))
    for n, copy in over:
        copy.wait_recv()
        done(n)


def gather_rep(net, buf, early, spare):
    q = buf.shape[T] // G

    def move(s, u, v, device, part=None):
        h = s["h"]
        row = pl.ds(h * T * q, T * q) if part is None else pl.ds((h * T + part) * q, q)
        ref = buf.at[u, v, row] if h else buf.at[v, u, row]
        net.spare = spare
        copy = net.send(ref, ref, device)
        net.spare = []
        return copy

    state = []
    for h in (0, 1):
        first, second = ("y", "z") if h == 0 else ("z", "y")
        p, v = getattr(net, first), getattr(net, second)
        s = dict(h=h, p=p, v=v, up=net.near(second, 1), down=net.near(second, -1), over=[])
        s["near"] = [(k, move(s, p, v, net.near(first, k))) for k in (1, 3)]
        s["near"].append((T, move(s, p, v, net.near(first, T))))
        state.append(s)

    def cross(s, k):
        u = ring(s["p"], k)
        s["over"].append((u, move(s, u, s["v"], s["up"]), move(s, u, s["v"], s["down"])))

    for s in state:
        cross(s, 0)
    later = early()
    for n in range(3):
        for s in state:
            k, copy = s["near"][n]
            copy.wait_recv()
            cross(s, -k)
    extra = later()
    last = []
    for n in range(G):
        for s in state:
            u, up, down = s["over"][n]
            up.wait_recv()
            last.append(move(s, u, ring(s["v"], -1), s["up"], 0))
            down.wait_recv()
            last.append(move(s, u, ring(s["v"], 1), s["down"], 1))
    wait_all(last)
    return extra


def lanes(shape):
    return lax.broadcasted_iota(jnp.int32, shape, len(shape) - 1)


def pack(v):
    return v[:PK] + pltpu.roll(v[PK : T * PK], CLS, 1) + pltpu.roll(v[T * PK :], T * CLS, 1)


def unpack(v):
    keep = lanes((PK, LANE)) < CLS
    parts = [v, pltpu.roll(v, LANE - CLS, 1), pltpu.roll(v, LANE - T * CLS, 1)]
    return [jnp.where(keep, part, 0.0) for part in parts]


def scratch_shapes():
    half, thin, piece = HID // T, ROW // G, CLS + N
    return dict(
        a_v=((G, G, ROW, WIDE), BF16),
        xg=((N, ROW, LANE), BF16),
        cg=((N, N, LANE), F32),
        y1=((WIDE, HID), BF16),
        zp=((G, G, ROW, HID), F32),
        far=((T, T, T, G, thin // T, HID), F32),
        near=((T, T, T, G, thin, HID), F32),
        mid=((T, T, G, thin, HID), F32),
        last=((T, T, G, thin, HID), F32),
        z1=((ROW, HID), F32),
        h1=((ROW, HID), BF16),
        w2p=((LANE, HID), F32),
        y2g=((N, PK, LANE), BF16),
        y2u=((WIDE, LANE), BF16),
        zq=((G, G, PK, LANE), F32),
        zi=((G, G, PK, LANE), F32),
        g2s=((PK, LANE), BF16),
        g2g=((G, G, PK, LANE), BF16),
        g2u=((TALL, LANE), BF16),
        d2=((G, CLS, PAIR), F32),
        d2i=((G, CLS, PAIR), F32),
        d2s=((T, CLS, PAIR), F32),
        d2t=((PAIR, LANE), F32),
        g1g=((G, G, ROW, HID), BF16),
        e1=((G, HID, PAIR), F32),
        e1o=((G, half, PAIR), F32),
        e1s=((G, half, PAIR), F32),
        e1far=((T, half // T, PAIR), F32),
        e1near=((T, half, PAIR), F32),
        w2s=((T, piece, LANE), F32),
        w2o=((piece, LANE), F32),
        wx=((G, piece, LANE), F32),
        wr_own=((piece, LANE), F32),
        wr=((G, G, piece, LANE), F32),
        wf=((T, piece, LANE), F32),
        ra=((G, G, N, LANE), F32),
        rai=((G, G, N, LANE), F32),
        rx=((N, LANE), F32),
        rxi=((G, N, LANE), F32),
        rs=((N, LANE), F32),
        rf=((T, G, G, N, LANE), F32),
        w1v=((LANE, HID), F32),
        lab=((ROW,), jnp.int32),
        msk=((ROW,), jnp.int32),
        lab_o=((ROW,), jnp.int32),
        msk_o=((ROW,), jnp.int32),
    )


def kernel(adj, x_ref, w1_ref, w2_ref, lab_ref, msk_ref, out_ref, *scratch):
    names = list(scratch_shapes())
    s = dict(zip(names, scratch))
    send_sem, recv_sem, load_sem = scratch[len(names) :]
    net = Net(send_sem, recv_sem)
    z, y, x, c = net.z, net.y, net.x, net.c
    a_v = s["a_v"]

    barrier = pltpu.get_barrier_semaphore()
    peers = net.peers()
    for peer in peers:
        pl.semaphore_signal(barrier, inc=1, device_id=peer, device_id_type=MESH)

    me = x * T + c
    xg, cg, w2p, w1v, y1 = (s[k] for k in ("xg", "cg", "w2p", "w1v", "y1"))
    w2p[...] = jnp.zeros((LANE, HID), F32)
    pairs = [(msk_ref, s["msk"]), (lab_ref, s["lab"]), (x_ref, xg.at[me]), (w1_ref, w1v), (w2_ref, w2p.at[pl.ds(0, CLS)])]
    pairs += [(adj.at[k], a_v.at[k]) for k in range(G)]
    loads = [pltpu.make_async_copy(src, dst, load_sem.at[k]) for k, (src, dst) in enumerate(pairs)]
    for load in loads:
        load.start()
    small = len(loads) - G
    for load in loads[:small]:
        load.wait()

    def row_of(ref, dtype):
        return ref[...].astype(dtype).reshape(1, ROW)

    cg[me] = jnp.broadcast_to(jnp.sum(row_of(s["msk"], F32), axis=1, keepdims=True), (N, LANE))
    w2b = w2p[...].astype(BF16)
    w1b = w1v[...].astype(BF16)

    pl.semaphore_wait(barrier, len(peers))

    swaps = [net.send(s[k], s[k + "_o"], net.partner()) for k in ("lab", "msk")]
    counts = [copy for _, copy in gather_nodes(net, cg)]

    def y1_block(n):
        y1[span(n * ROW, ROW)] = dot(xg[n], w1b, 1, 0).astype(BF16)

    gather_pairs(net, xg, y1_block)
    for load in loads[small:]:
        load.wait()

    zp = s["zp"]

    sum1 = RepSum(net, zp, s["far"], s["near"], s["mid"], s["last"])

    def z1_block(h, t):
        row = pl.ds(h * ROW // T, ROW // T)
        a = a_v[t, :, row] if h else a_v[:, t, row]
        term = dot(a.reshape(TALL // N, WIDE), y1[...], 1, 0).reshape(G, ROW // T, HID)
        if h:
            zp[t, :, row] = term
        else:
            zp[:, t, row] = term

    base = net.used
    for k in (2, 1, 3, 0):
        for h, p in enumerate((y, z)):
            z1_block(h, ring(p, k))
            if k == T:
                sum1.start(h)
            elif k > 0:
                sum1.free(h, k // T)
    z1 = s["z1"]
    sum1.finish(z1)
    z1_used = list(range(base, net.used))

    h1 = s["h1"]
    h1[...] = jnp.maximum(z1[...], 0.0).astype(BF16)
    y2 = dot(h1[...], w2b, 1, 1).astype(BF16).astype(F32)
    y2g, y2u = s["y2g"], s["y2u"]
    y2g[me] = pack(y2).astype(BF16)
    blocks = gather_nodes(net, y2g)

    def spread(src, dst, base):
        for g, part in enumerate(unpack(src.astype(F32))):
            dst[span(base * ROW + g * PK, PK)] = part.astype(BF16)

    def spread_y2(j, _):
        spread(y2g[j], y2u, j)
        return _

    wait_all(counts + swaps + [copy for _, copy in blocks])
    lax.fori_loop(0, N, spread_y2, 0)
    net.flush()

    zq, zi = s["zq"], s["zi"]
    count = jnp.sum(cg[...], axis=0)[:1]
    at_count = lanes((PK, LANE)) == 3 * CLS
    count = jnp.where(at_count, jnp.broadcast_to(count, (PK, LANE)), 0.0)

    start, arrivals = net.rep_all(lambda zz, yy: zq.at[zz, yy], zi)

    def z2_blocks(j, _):
        dz, p = j // T + 1, T * (j % T)
        zz = ring(z, dz)
        term = dot(a_v[zz, pl.ds(p, T)].reshape(PAIR, WIDE), y2u[...], 1, 0)
        for k in (0, 1):
            zq[zz, p + k] = pack(term[k * ROW : (k + 1) * ROW]) + count
            start(dz, p + k - y)
        return _

    lax.fori_loop(0, N, z2_blocks, 0)
    mask_row, label_row = row_of(s["msk_o"], F32), row_of(s["lab_o"], jnp.int32)
    mask_all = jnp.broadcast_to(mask_row, (LANE, ROW)).T
    classes = lax.broadcasted_iota(jnp.int32, (LANE, ROW), 0)
    one_hot = (jnp.broadcast_to(label_row, (LANE, ROW)) == classes).astype(F32).T
    arrivals.wait_recv()
    packed = jnp.sum(zi[...].reshape(G * G, PK, LANE), axis=0)

    total = jnp.sum(jnp.where(at_count, packed, 0.0), axis=1, keepdims=True)
    total = jnp.concatenate([total, total, total], axis=0)
    logits = jnp.concatenate(unpack(packed), axis=0)
    valid = lanes((ROW, LANE)) < CLS
    top = jnp.max(jnp.where(valid, logits, -jnp.inf), axis=1, keepdims=True)
    shifted = jnp.where(valid, logits - top, 0.0)
    norm = jnp.sum(jnp.where(valid, jnp.exp(shifted), 0.0), axis=1, keepdims=True)
    log_probs = shifted - jnp.log(norm)
    picked = jnp.where(valid, -(mask_all * (one_hot * log_probs)), 0.0)
    loss_part = jnp.sum(picked, axis=0, keepdims=True)
    g2 = jnp.where(valid, (jnp.exp(log_probs) - one_hot) * (mask_all / total), 0.0).astype(BF16).astype(F32)
    g2s, g2g, g2u = s["g2s"], s["g2g"], s["g2u"]
    g2s[...] = pack(g2).astype(BF16)

    def spread_g2(k, _):
        spread(g2g[k // G, k % G], g2u, k)
        return _

    net.rep_send(lambda zz, yy: g2s, g2g).wait_recv()
    lax.fori_loop(0, G * G, spread_g2, 0)

    d2, d2i, d2s, d2t = (s[k] for k in ("d2", "d2i", "d2s", "d2t"))

    def a_cols(k, size):
        return a_v[:, :, :, span(k * size, size)].reshape(TALL, size)

    def d2_block(k):
        part = dot(g2u[...], a_cols(k, T * PAIR), 0, 0)[:CLS]
        d2[T * k] = part[:, :PAIR]
        d2[T * k + 1] = part[:, PAIR:]

    def d2_send(t):
        return net.send(d2.at[t], d2i.at[x], net.dev(x=t, c=1 - c))

    d2_block(1 - x // T)
    copies = [d2_send(ring(x, T)), d2_send(3 - x)]
    d2_block(x // T)
    copies.append(d2_send(x + 1 - T * (x % T)))
    d2i[x] = d2[x]
    wait_all(copies)
    d2s[c] = jnp.sum(d2i[...], axis=0)
    net.send(d2s.at[c], d2s.at[c], net.partner()).wait_recv()
    d2t[...] = jnp.concatenate([d2s[0] + d2s[1], jnp.zeros((LANE - CLS, PAIR), F32)], axis=0).T
    dy2 = d2t[span(c * ROW, ROW)].astype(BF16)

    dh1 = dot(dy2, w2b, 1, 0)
    g1g = s["g1g"]
    g1g[z, y] = jnp.where(z1[...] > 0.0, dh1, 0.0).astype(BF16)

    w2s, w2o, wx, wr, wf = (s[k] for k in ("w2s", "w2o", "wx", "wr", "wf"))
    loss_tile = jnp.concatenate([loss_part, jnp.zeros((N - 1, LANE), F32)], axis=0)

    def early():
        dw2_t = dot(dy2, h1[...], 0, 0)[:CLS]
        for h in (0, 1):
            w2s[h, :CLS] = dw2_t[:, h * LANE : (h + 1) * LANE]
            w2s[h, CLS:] = loss_tile
        swap = net.send(w2s.at[1 - c], w2o, net.partner())

        def later():
            swap.wait_recv()
            wx[x] = w2s[c] + w2o[...]
            return exchange(net, "x", lambda t: wx.at[x], wx)

        return later

    net.flush()
    swaps = gather_rep(net, g1g, early, z1_used)

    e1, e1o, e1s, e1far, e1near = (s[k] for k in ("e1", "e1o", "e1s", "e1far", "e1near"))
    half = HID // T
    q = half // T
    part = lambda d: pl.ds(d * q, q)
    tree = Tree(net, "x", lambda t, d: e1s.at[t, part(d)], lambda d: e1far.at[d], lambda d, e: e1near.at[d, part(e)])

    def e1_block(k):
        t = ring(x, k)
        e1[t] = dot(g1g[...].reshape(TALL, HID), a_cols(t, PAIR), 0, 0)
        return t, net.send(e1.at[t, span((1 - c) * half, half)], e1o.at[t], net.partner())

    def e1_join(t, copy):
        copy.wait_recv()
        e1s[t] = e1[t, span(c * half, half)] + e1o[t]

    opposite = e1_block(2)
    right = e1_block(1)
    e1_join(*opposite)
    tree.start()
    left = e1_block(3)
    e1_join(*right)
    tree.free(0)
    wait_all(swaps)
    wr_own = s["wr_own"]
    wr_own[...] = jnp.sum(wx[...], axis=0)
    w_arrivals = net.rep_send(lambda zz, yy: wr_own, wr)
    own = e1_block(0)
    e1_join(*left)
    tree.free(1)
    tree.relay()
    e1_join(*own)
    tree.end()
    dy1 = (e1s[x] + e1near[0] + e1near[1]).astype(BF16)
    dw1_t = dot(dy1, xg[pl.ds(x * T, T)].reshape(PAIR, LANE), 1, 0)

    ra, rai, rx, rxi, rs, rf = (s[k] for k in ("ra", "rai", "rx", "rxi", "rs", "rf"))
    ra[...] = dw1_t.reshape(G, G, N, LANE)
    arrivals = net.rep_send(lambda zz, yy: ra.at[zz, yy], rai)
    w_arrivals.wait_recv()
    wf[1 - c] = jnp.sum(wr[...].reshape(G * G, CLS + N, LANE), axis=0)
    swap = net.send(wf.at[1 - c], wf.at[1 - c], net.partner())
    arrivals.wait_recv()
    rx[...] = jnp.sum(rai[...].reshape(G * G, N, LANE), axis=0)
    wait_all([net.send(rx, rxi.at[x], net.dev(x=ring(x, k), c=1 - c)) for k in (2, 1, 3, 0)])
    rs[...] = jnp.sum(rxi[...], axis=0)
    arrivals = net.rep_send(lambda zz, yy: rs, rf.at[c])
    swap.wait_recv()
    out_ref[:, span(LANE, CLS + N)] = wf[...]
    out_ref[0, span(LANE + CLS + N, N)] = jnp.broadcast_to(total[:1], (N, LANE))
    arrivals.wait_recv()
    net.send(rf.at[1 - c], rf.at[1 - c], net.partner()).wait_recv()
    out_ref[:, :LANE] = rf[...].reshape(T, LANE, LANE)
    net.flush()


def unpack_kernel(sums, loss_ref, dw1_ref, dw2_ref):
    for h in (0, 1):
        half = span(h * LANE, LANE)
        dw1_ref[:, half] = sums[h, :LANE].T
        dw2_ref[:, half] = sums[h, LANE : LANE + CLS]
    loss = jnp.sum(sums[0, LANE + CLS : LANE + CLS + N])
    loss_ref[0, 0] = loss / jnp.max(sums[0, LANE + CLS + N :])


def solution(mesh):
    vmem, smem = pl.BlockSpec(memory_space=pltpu.VMEM), pl.BlockSpec(memory_space=pltpu.SMEM)
    struct = lambda *shape: jax.ShapeDtypeStruct(shape, F32)

    def device_step(adj_blk, feat_blk, w_one, w_two, label_blk, mask_blk):
        sems = [pltpu.SemaphoreType.DMA((n,)) for n in (N_SEND, N_RECV, N + 1)]
        sums = pl.pallas_call(
            kernel,
            out_shape=struct(T, LANE + CLS + T * N, LANE),
            in_specs=[pl.BlockSpec(memory_space=pl.ANY)] * 6,
            out_specs=vmem,
            scratch_shapes=[pltpu.VMEM(shape, dtype) for shape, dtype in scratch_shapes().values()] + sems,
            compiler_params=pltpu.CompilerParams(collective_id=0, has_side_effects=True, vmem_limit_bytes=56 << 20),
        )(adj_blk.reshape(G, G, ROW, WIDE), feat_blk, w_one, w_two.T, label_blk, mask_blk)
        loss, dw1, dw2 = pl.pallas_call(
            unpack_kernel,
            out_shape=(struct(1, 1), struct(LANE, HID), struct(CLS, HID)),
            in_specs=[vmem],
            out_specs=(smem, vmem, vmem),
        )(sums)
        return loss.reshape(()), dw1, dw2.T

    row_spec = P(("rep", "nodes"))
    return jax.shard_map(
        device_step,
        mesh=mesh,
        in_specs=(P(None, "nodes", "rep"), row_spec, P(), P(), row_spec, row_spec),
        out_specs=(P(), P(), P()),
        check_vma=False,
    )
```

```python
import jax
import jax.numpy as jnp
from jax import lax
from jax.experimental import pallas as pl
from jax.experimental.pallas import tpu as pltpu
from jax.sharding import PartitionSpec as P

MESH = pl.DeviceIdType.MESH
F32, BF16 = jnp.float32, jnp.bfloat16
T, G, N = 2, 4, 8
LANE, HID, CLS, ROW = 128, 256, 40, 192
PK = ROW // 3
TALL, WIDE = 16 * ROW, N * ROW
PAIR = T * ROW
N_SEND, N_RECV = 92, 156


def ring(v, k):
    return (v + k + G) % G


def dot(a, b, ca, cb):
    return lax.dot_general(a, b, (((ca,), (cb,)), ((), ())), preferred_element_type=F32)


def span(start, size):
    return pl.ds(start if isinstance(start, int) else pl.multiple_of(start, size), size)


class Net:
    def __init__(self, send_sem, recv_sem):
        rep, node = lax.axis_index("rep"), lax.axis_index("nodes")
        self.z, self.y, self.x, self.c = rep // G, rep % G, node // T, node % T
        self.send_sem, self.recv_sem = send_sem, recv_sem
        self.used, self.spare, self.ends = 0, [], []

    def dev(self, **place):
        z, y, x, c = (place.get(k, getattr(self, k)) for k in "zyxc")
        return (z * G + y, x * T + c)

    def near(self, axis, k):
        return self.dev(**{axis: ring(getattr(self, axis), k)})

    def partner(self):
        return self.dev(c=1 - self.c)

    def recv_index(self):
        if self.spare:
            return self.spare.pop()
        self.used += 1
        return self.used - 1

    def copy(self, src, dst, device, k, n):
        send, recv = self.send_sem.at[k], self.recv_sem.at[n]
        return pltpu.make_async_remote_copy(src_ref=src, dst_ref=dst, send_sem=send, recv_sem=recv, device_id=device, device_id_type=MESH)

    def send(self, src, dst, device):
        copy = self.copy(src, dst, device, len(self.ends), self.recv_index())
        copy.start()
        self.ends.append(copy)
        return copy

    def flush(self):
        for copy in self.ends:
            copy.wait_send()
        self.ends = []

    def rep_each(self, src, buf):
        k, n = len(self.ends), self.used
        self.used += G * G
        mine = buf.at[self.z, self.y]
        self.ends.append(self.copy(buf, buf, self.partner(), k, n))
        for j in range(G * G):
            m = (j + 1) * 5 % (G * G)
            z, y = ring(self.z, m // G), ring(self.y, m % G)
            self.copy(src, mine, self.dev(z=z, y=y, c=1 - self.c), k, n + m).start()

        def each(fn):
            def body(j, _):
                m = (j + 1) * 5 % (G * G)
                self.copy(mine, mine, self.partner(), k, n + m).wait_recv()
                fn(ring(self.z, -(m // G)), ring(self.y, -(m % G)))
                return _

            lax.fori_loop(0, G * G, body, 0)

        return each

    def rep_all(self, src, buf):
        k, n = len(self.ends), self.recv_index()
        mine = buf.at[self.z, self.y]
        whole = self.copy(buf, buf, self.partner(), k, n)
        self.ends.append(whole)

        def start(dz, dy):
            z, y = ring(self.z, dz), ring(self.y, dy)
            self.copy(src(z, y), mine, self.dev(z=z, y=y, c=1 - self.c), k, n).start()

        return start, whole

    def rep_send(self, src, buf):
        start, whole = self.rep_all(src, buf)
        for j in range(G * G):
            k = (j + 1) * 5 % (G * G)
            start(k // G, k % G)
        return whole

    def peers(self):
        out = [self.partner()]
        for k in (1, 2, 3):
            out += [self.near(axis, k) for axis in "xyz"]
            out.append(self.dev(x=ring(self.x, k), c=1 - self.c))
        return out


class Tree:
    def __init__(self, net, axis, at, far, near):
        self.net, self.at, self.far, self.near = net, at, far, near
        self.p = getattr(net, axis)
        self.side = net.near(axis, 1), net.near(axis, -1)

    def start(self):
        self.first = [self.net.send(self.at(ring(self.p, T), d), self.far(d), self.side[d]) for d in (0, 1)]
        self.arrive = []

    def free(self, d):
        t = ring(self.p, 1 - T * d)
        self.arrive.append(self.net.send(self.at(t, 1 - d), self.near(d, 1 - d), self.side[d]))

    def relay(self):
        for d in (0, 1):
            self.first[d].wait_recv()
            mine = self.at(ring(self.p, 1 - T * d), d)
            mine[...] = mine[...] + self.far(d)[...]
            self.arrive.append(self.net.send(mine, self.near(d, d), self.side[d]))

    def end(self):
        for copy in self.arrive:
            copy.wait_recv()


class RepSum:
    def __init__(self, net, terms, far, near, mid, last):
        self.net, self.terms, self.near, self.mid, self.last = net, terms, near, mid, last
        self.size, slices = near.shape[-T], near.shape[1]
        self.slices = range(slices)
        q = self.size // T
        self.parts = [(h, s) for s in self.slices for h in (0, 1)]
        self.tree = {}
        for h, s in self.parts:

            def at(t, d, h=h, s=s):
                row = pl.ds((h * slices + s) * self.size + d * q, q)
                return terms.at[t, :, row] if h else terms.at[:, t, row]

            self.tree[h, s] = Tree(
                net, "yz"[h], at, lambda d, h=h, s=s: far.at[h, s, d], lambda d, e, h=h, s=s: near.at[h, s, d, :, pl.ds(e * q, q)]
            )

    def start(self, h):
        for s in self.slices:
            self.tree[h, s].start()

    def free(self, h, d):
        for s in self.slices:
            self.tree[h, s].free(d)

    def finish(self, out):
        net, size = self.net, self.size
        for part in self.parts:
            self.tree[part].relay()
        arrivals = []
        for h, s in self.parts:
            tree, mid = self.tree[h, s], self.mid.at[h, s]
            tree.end()
            row = pl.ds((h * len(self.slices) + s) * size, size)
            own = self.terms[tree.p, :, row] if h else self.terms[:, tree.p, row]
            mid[...] = own + self.near[h, s, 0] + self.near[h, s, 1]
            axis = "zy"[h]
            arrivals.append(exchange(net, axis, lambda t: mid.at[t], self.last.at[h, s]))
        for (h, s), copies in zip(self.parts, arrivals):
            for copy in copies:
                copy.wait_recv()
            p = net.y if h else net.z
            total = self.mid[h, s, p]
            for k in (1, 2, 3):
                total = total + self.last[h, s, ring(p, k)]
            out[pl.ds((h * len(self.slices) + s) * size, size)] = total


def exchange(net, axis, src, buf):
    p = getattr(net, axis)
    return [net.send(src(ring(p, k)), buf.at[p], net.near(axis, k)) for k in (2, 1, 3)]


def wait_all(copies):
    for copy in copies:
        copy.wait_recv()


def gather_nodes(net, buf):
    node = lambda k, core: ring(net.x, k) * T + core
    mine = buf.at[node(0, net.c)]
    other = 1 - net.c
    out = []
    for k in (2, 1, 3):
        out.append((node(-k, net.c), net.send(mine, mine, net.near("x", k))))
        out.append((node(-k, other), net.send(mine, mine, net.dev(x=ring(net.x, k), c=other))))
    return [(node(0, other), net.send(mine, mine, net.partner()))] + out


def gather_pairs(net, buf, done, extra):
    node = lambda k, core: ring(net.x, k) * T + core
    other = 1 - net.c

    def move(n, device):
        return net.send(buf.at[n], buf.at[n], device)

    me = node(0, net.c)
    over = [(node(0, other), move(me, net.partner()))]
    come = [(k, move(me, net.dev(x=ring(net.x, k), c=other))) for k in (2, 1, 3)]
    out = extra()
    done(me)
    for k, copy in come:
        copy.wait_recv()
        over.append((node(-k, net.c), move(node(-k, other), net.partner())))
        done(node(-k, other))
    for n, copy in over:
        copy.wait_recv()
        done(n)
    return out


class Spread:
    def __init__(self, net, buf):
        self.net, self.buf = net, buf
        self.first = [self.along(h, "yz"[h], net.z, net.y) for h in (0, 1)]
        self.rest = [copy for h in (0, 1) for _, copy in self.along(h, "zy"[h], net.z, net.y)]

    def along(self, h, axis, z, y):
        size = self.buf.shape[T] // T
        ref = self.buf.at[z, y, pl.ds(h * size, size)]
        return [(k, self.net.send(ref, ref, self.net.near(axis, k))) for k in (2, 1, 3)]

    def second(self):
        net = self.net
        for n in range(3):
            for h in (0, 1):
                k, copy = self.first[h][n]
                copy.wait_recv()
                z, y = (ring(net.z, -k), net.y) if h else (net.z, ring(net.y, -k))
                self.rest += [copy for _, copy in self.along(h, "zy"[h], z, y)]


def lanes(shape):
    return lax.broadcasted_iota(jnp.int32, shape, len(shape) - 1)


def pack(v):
    return v[:PK] + pltpu.roll(v[PK : T * PK], CLS, 1) + pltpu.roll(v[T * PK :], T * CLS, 1)


def unpack(v):
    keep = lanes((PK, LANE)) < CLS
    parts = [v, pltpu.roll(v, LANE - CLS, 1), pltpu.roll(v, LANE - T * CLS, 1)]
    return [jnp.where(keep, part, 0.0) for part in parts]


def scratch_shapes():
    half, thin, piece = HID // T, ROW // 6, CLS + N
    return dict(
        a_v=((G, G, ROW, WIDE), BF16),
        xg=((N, ROW, LANE), BF16),
        cg=((N, N, LANE), F32),
        y1=((WIDE, HID), BF16),
        zp=((G, G, ROW, HID), F32),
        far=((T, 3, T, G, thin // T, HID), F32),
        near=((T, 3, T, G, thin, HID), F32),
        mid=((T, 3, G, thin, HID), F32),
        last=((T, 3, G, thin, HID), F32),
        z1=((ROW, HID), F32),
        h1=((ROW, HID), BF16),
        w2p=((LANE, HID), F32),
        y2g=((N, PK, LANE), BF16),
        y2u=((WIDE, LANE), BF16),
        zq=((G, G, PK, LANE), F32),
        zi=((G, G, PK, LANE), F32),
        g2s=((PK, LANE), BF16),
        g2g=((G, G, PK, LANE), BF16),
        g2u=((TALL, LANE), BF16),
        d2=((G, CLS, PAIR), F32),
        d2i=((G, CLS, PAIR), F32),
        d2s=((T, CLS, PAIR), F32),
        d2t=((PAIR, LANE), F32),
        g1g=((G, G, ROW, HID), BF16),
        mg=((G, G, ROW, HID), BF16),
        dys=((PK, LANE), BF16),
        dyg=((G, G, PK, LANE), BF16),
        e1=((G, HID, PAIR), F32),
        e1o=((G, half, PAIR), F32),
        e1s=((G, half, PAIR), F32),
        e1far=((T, T, half // G, PAIR), F32),
        e1near=((T, half, PAIR), F32),
        w2s=((T, piece, LANE), F32),
        w2o=((piece, LANE), F32),
        wx=((G, piece, LANE), F32),
        wr_own=((piece, LANE), F32),
        wr=((G, G, piece, LANE), F32),
        wf=((T, piece, LANE), F32),
        ra=((G, G, N, LANE), F32),
        rai=((G, G, N, LANE), F32),
        rx=((N, LANE), F32),
        rxi=((G, N, LANE), F32),
        rs=((N, LANE), F32),
        rf=((T, G, G, N, LANE), F32),
        w1v=((LANE, HID), F32),
        lab=((ROW,), jnp.int32),
        msk=((ROW,), jnp.int32),
        lab_o=((ROW,), jnp.int32),
        msk_o=((ROW,), jnp.int32),
    )


def kernel(adj, x_ref, w1_ref, w2_ref, lab_ref, msk_ref, out_ref, *scratch):
    names = list(scratch_shapes())
    s = dict(zip(names, scratch))
    send_sem, recv_sem, load_sem = scratch[len(names) :]
    net = Net(send_sem, recv_sem)
    z, y, x, c = net.z, net.y, net.x, net.c
    a_v = s["a_v"]

    barrier = pltpu.get_barrier_semaphore()
    peers = net.peers()
    for peer in peers:
        pl.semaphore_signal(barrier, inc=1, device_id=peer, device_id_type=MESH)

    me = x * T + c
    xg, cg, w2p, w1v, y1 = (s[k] for k in ("xg", "cg", "w2p", "w1v", "y1"))
    w2p[...] = jnp.zeros((LANE, HID), F32)
    pairs = [(msk_ref, s["msk"]), (lab_ref, s["lab"]), (x_ref, xg.at[me]), (w1_ref, w1v), (w2_ref, w2p.at[pl.ds(0, CLS)])]
    pairs += [(adj.at[k], a_v.at[k]) for k in range(G)]
    loads = [pltpu.make_async_copy(src, dst, load_sem.at[k]) for k, (src, dst) in enumerate(pairs)]
    for load in loads:
        load.start()
    small = len(loads) - G
    for load in loads[:small]:
        load.wait()

    def row_of(ref, dtype):
        return ref[...].astype(dtype).reshape(1, ROW)

    cg[me] = jnp.broadcast_to(jnp.sum(row_of(s["msk"], F32), axis=1, keepdims=True), (N, LANE))
    w2b = w2p[...].astype(BF16)
    w1b = w1v[...].astype(BF16)

    pl.semaphore_wait(barrier, len(peers))

    def y1_block(n):
        y1[span(n * ROW, ROW)] = dot(xg[n], w1b, 1, 0).astype(BF16)

    def small_copies():
        swaps = [net.send(s[k], s[k + "_o"], net.partner()) for k in ("lab", "msk")]
        return swaps + [copy for _, copy in gather_nodes(net, cg)]

    counts = gather_pairs(net, xg, y1_block, small_copies)
    for load in loads[small:]:
        load.wait()

    zp = s["zp"]

    sum1 = RepSum(net, zp, s["far"], s["near"], s["mid"], s["last"])

    def z1_block(h, t):
        row = pl.ds(h * ROW // T, ROW // T)
        a = a_v[t, :, row] if h else a_v[:, t, row]
        term = dot(a.reshape(TALL // N, WIDE), y1[...], 1, 0).reshape(G, ROW // T, HID)
        if h:
            zp[t, :, row] = term
        else:
            zp[:, t, row] = term

    base = net.used
    for k in (2, 1, 3, 0):
        for h, p in enumerate((y, z)):
            z1_block(h, ring(p, k))
            if k == T:
                sum1.start(h)
            elif k > 0:
                sum1.free(h, k // T)
    z1 = s["z1"]
    sum1.finish(z1)
    z1_used = list(range(base, net.used))

    h1 = s["h1"]
    h1[...] = jnp.maximum(z1[...], 0.0).astype(BF16)
    y2 = dot(h1[...], w2b, 1, 1).astype(BF16).astype(F32)
    y2g, y2u = s["y2g"], s["y2u"]
    y2g[me] = pack(y2).astype(BF16)
    blocks = gather_nodes(net, y2g)
    mg = s["mg"]
    mg[z, y] = jnp.where(z1[...] > 0.0, 1.0, 0.0).astype(BF16)
    masks = Spread(net, mg)

    def spread(src, dst, base):
        for g, part in enumerate(unpack(src.astype(F32))):
            dst[span(base * ROW + g * PK, PK)] = part.astype(BF16)

    def spread_y2(j, _):
        spread(y2g[j], y2u, j)
        return _

    wait_all(counts + [copy for _, copy in blocks])
    lax.fori_loop(0, N, spread_y2, 0)

    zq, zi = s["zq"], s["zi"]
    count = jnp.sum(cg[...], axis=0)[:1]
    at_count = lanes((PK, LANE)) == 3 * CLS
    count = jnp.where(at_count, jnp.broadcast_to(count, (PK, LANE)), 0.0)

    start, arrivals = net.rep_all(lambda zz, yy: zq.at[zz, yy], zi)

    def z2_blocks(j, _):
        dz, p = j // T + 1, T * (j % T)
        zz = ring(z, dz)
        term = dot(a_v[zz, pl.ds(p, T)].reshape(PAIR, WIDE), y2u[...], 1, 0)
        for k in (0, 1):
            zq[zz, p + k] = pack(term[k * ROW : (k + 1) * ROW]) + count
            start(dz, p + k - y)
        return _

    lax.fori_loop(0, N, z2_blocks, 0)
    mask_row, label_row = row_of(s["msk_o"], F32), row_of(s["lab_o"], jnp.int32)
    mask_all = jnp.broadcast_to(mask_row, (LANE, ROW)).T
    classes = lax.broadcasted_iota(jnp.int32, (LANE, ROW), 0)
    one_hot = (jnp.broadcast_to(label_row, (LANE, ROW)) == classes).astype(F32).T
    arrivals.wait_recv()
    net.flush()
    packed = jnp.sum(zi[...].reshape(G * G, PK, LANE), axis=0)

    total = jnp.sum(jnp.where(at_count, packed, 0.0), axis=1, keepdims=True)
    total = jnp.concatenate([total, total, total], axis=0)
    logits = jnp.concatenate(unpack(packed), axis=0)
    valid = lanes((ROW, LANE)) < CLS
    top = jnp.max(jnp.where(valid, logits, -jnp.inf), axis=1, keepdims=True)
    shifted = jnp.where(valid, logits - top, 0.0)
    norm = jnp.sum(jnp.where(valid, jnp.exp(shifted), 0.0), axis=1, keepdims=True)
    log_probs = shifted - jnp.log(norm)
    picked = jnp.where(valid, -(mask_all * (one_hot * log_probs)), 0.0)
    loss_part = jnp.sum(picked, axis=0, keepdims=True)
    g2 = jnp.where(valid, (jnp.exp(log_probs) - one_hot) * (mask_all / total), 0.0).astype(BF16).astype(F32)
    g2s, g2g, g2u = s["g2s"], s["g2g"], s["g2u"]
    g2s[...] = pack(g2).astype(BF16)

    arrivals = net.rep_each(g2s, g2g)
    net.spare = z1_used
    masks.second()
    net.spare = []
    arrivals(lambda zz, yy: spread(g2g[zz, yy], g2u, zz * G + yy))

    d2, d2i, d2s, d2t = (s[k] for k in ("d2", "d2i", "d2s", "d2t"))

    def a_cols(k, size):
        return a_v[:, :, :, span(k * size, size)].reshape(TALL, size)

    def d2_block(k):
        part = dot(g2u[...], a_cols(k, T * PAIR), 0, 0)[:CLS]
        d2[T * k] = part[:, :PAIR]
        d2[T * k + 1] = part[:, PAIR:]

    def d2_send(t):
        return net.send(d2.at[t], d2i.at[x], net.dev(x=t, c=1 - c))

    d2_block(1 - x // T)
    copies = [d2_send(ring(x, T)), d2_send(3 - x)]
    d2_block(x // T)
    copies.append(d2_send(x + 1 - T * (x % T)))
    d2i[x] = d2[x]
    wait_all(copies)
    d2s[c] = jnp.sum(d2i[...], axis=0)
    net.send(d2s.at[c], d2s.at[c], net.partner()).wait_recv()
    d2t[...] = jnp.concatenate([d2s[0] + d2s[1], jnp.zeros((LANE - CLS, PAIR), F32)], axis=0).T

    dys, dyg, g1g = s["dys"], s["dyg"], s["g1g"]
    dys[...] = pack(d2t[span((1 - c) * ROW, ROW)].astype(BF16).astype(F32)).astype(BF16)
    arrivals = net.rep_each(dys, dyg)

    w2s, w2o, wx, wr, wf = (s[k] for k in ("w2s", "w2o", "wx", "wr", "wf"))
    dy2 = d2t[span(c * ROW, ROW)].astype(BF16)
    dw2_t = dot(dy2, h1[...], 0, 0)[:CLS]
    loss_tile = jnp.concatenate([loss_part, jnp.zeros((N - 1, LANE), F32)], axis=0)
    for h in (0, 1):
        w2s[h, :CLS] = dw2_t[:, h * LANE : (h + 1) * LANE]
        w2s[h, CLS:] = loss_tile
    swap = net.send(w2s.at[1 - c], w2o, net.partner())
    wait_all(masks.rest)
    swap.wait_recv()
    wx[x] = w2s[c] + w2o[...]
    swaps = exchange(net, "x", lambda t: wx.at[x], wx)

    def g1_block(zz, yy):
        dy = jnp.concatenate(unpack(dyg[zz, yy].astype(F32)), axis=0).astype(BF16)
        dh1 = dot(dy, w2b, 1, 0)
        g1g[zz, yy] = jnp.where(mg[zz, yy].astype(F32) > 0.0, dh1, 0.0).astype(BF16)

    arrivals(g1_block)
    net.flush()

    e1, e1o, e1s, e1far, e1near = (s[k] for k in ("e1", "e1o", "e1s", "e1far", "e1near"))
    half = HID // T
    q = half // G

    def tree_of(n):
        part = lambda d: pl.ds((T * n + d) * q, q)
        return Tree(net, "x", lambda t, d: e1s.at[t, part(d)], lambda d: e1far.at[n, d], lambda d, e: e1near.at[d, part(e)])

    trees = [tree_of(n) for n in (0, 1)]

    def e1_block(k):
        t = ring(x, k)
        e1[t] = dot(g1g[...].reshape(TALL, HID), a_cols(t, PAIR), 0, 0)
        return t, net.send(e1.at[t, span((1 - c) * half, half)], e1o.at[t], net.partner())

    def e1_join(t, copy):
        copy.wait_recv()
        e1s[t] = e1[t, span(c * half, half)] + e1o[t]

    opposite = e1_block(2)
    right = e1_block(1)
    e1_join(*opposite)
    for tree in trees:
        tree.start()
    left = e1_block(3)
    e1_join(*right)
    for tree in trees:
        tree.free(0)
    own = e1_block(0)
    e1_join(*left)
    for tree in trees:
        tree.free(1)
    e1_join(*own)
    for tree in trees:
        tree.relay()
    wait_all(swaps)
    wr_own = s["wr_own"]
    wr_own[...] = jnp.sum(wx[...], axis=0)
    w_arrivals = net.rep_send(lambda zz, yy: wr_own, wr)
    for tree in trees:
        tree.end()
    dy1 = (e1s[x] + e1near[0] + e1near[1]).astype(BF16)
    dw1_t = dot(dy1, xg[pl.ds(x * T, T)].reshape(PAIR, LANE), 1, 0)

    ra, rai, rx, rxi, rs, rf = (s[k] for k in ("ra", "rai", "rx", "rxi", "rs", "rf"))
    ra[...] = dw1_t.reshape(G, G, N, LANE)
    arrivals = net.rep_send(lambda zz, yy: ra.at[zz, yy], rai)
    w_arrivals.wait_recv()
    wf[1 - c] = jnp.sum(wr[...].reshape(G * G, CLS + N, LANE), axis=0)
    swap = net.send(wf.at[1 - c], wf.at[1 - c], net.partner())
    arrivals.wait_recv()
    rx[...] = jnp.sum(rai[...].reshape(G * G, N, LANE), axis=0)
    wait_all([net.send(rx, rxi.at[x], net.dev(x=ring(x, k), c=1 - c)) for k in (2, 1, 3, 0)])
    rs[...] = jnp.sum(rxi[...], axis=0)
    arrivals = net.rep_send(lambda zz, yy: rs, rf.at[c])
    swap.wait_recv()
    out_ref[:, span(LANE, CLS + N)] = wf[...]
    out_ref[0, span(LANE + CLS + N, N)] = jnp.broadcast_to(total[:1], (N, LANE))
    arrivals.wait_recv()
    net.send(rf.at[1 - c], rf.at[1 - c], net.partner()).wait_recv()
    out_ref[:, :LANE] = rf[...].reshape(T, LANE, LANE)
    net.flush()


def unpack_kernel(sums, loss_ref, dw1_ref, dw2_ref):
    for h in (0, 1):
        half = span(h * LANE, LANE)
        dw1_ref[:, half] = sums[h, :LANE].T
        dw2_ref[:, half] = sums[h, LANE : LANE + CLS]
    loss = jnp.sum(sums[0, LANE + CLS : LANE + CLS + N])
    loss_ref[0, 0] = loss / jnp.max(sums[0, LANE + CLS + N :])


def solution(mesh):
    vmem, smem = pl.BlockSpec(memory_space=pltpu.VMEM), pl.BlockSpec(memory_space=pltpu.SMEM)
    struct = lambda *shape: jax.ShapeDtypeStruct(shape, F32)

    def device_step(adj_blk, feat_blk, w_one, w_two, label_blk, mask_blk):
        sems = [pltpu.SemaphoreType.DMA((n,)) for n in (N_SEND, N_RECV, N + 1)]
        sums = pl.pallas_call(
            kernel,
            out_shape=struct(T, LANE + CLS + T * N, LANE),
            in_specs=[pl.BlockSpec(memory_space=pl.ANY)] * 6,
            out_specs=vmem,
            scratch_shapes=[pltpu.VMEM(shape, dtype) for shape, dtype in scratch_shapes().values()] + sems,
            compiler_params=pltpu.CompilerParams(collective_id=0, has_side_effects=True, vmem_limit_bytes=56 << 20),
        )(adj_blk.reshape(G, G, ROW, WIDE), feat_blk, w_one, w_two.T, label_blk, mask_blk)
        loss, dw1, dw2 = pl.pallas_call(
            unpack_kernel,
            out_shape=(struct(1, 1), struct(LANE, HID), struct(CLS, HID)),
            in_specs=[vmem],
            out_specs=(smem, vmem, vmem),
        )(sums)
        return loss.reshape(()), dw1, dw2.T

    row_spec = P(("rep", "nodes"))
    return jax.shard_map(
        device_step,
        mesh=mesh,
        in_specs=(P(None, "nodes", "rep"), row_spec, P(), P(), row_spec, row_spec),
        out_specs=(P(), P(), P()),
        check_vma=False,
    )
```

```python
import jax
import jax.numpy as jnp
from jax import lax
from jax.experimental import pallas as pl
from jax.experimental.pallas import tpu as pltpu
from jax.sharding import PartitionSpec as P

MESH = pl.DeviceIdType.MESH
F32, BF16 = jnp.float32, jnp.bfloat16
T, G, N = 2, 4, 8
LANE, HID, CLS, ROW = 128, 256, 40, 192
PK = ROW // 3
TALL, WIDE = 16 * ROW, N * ROW
PAIR = T * ROW
N_SEND, N_RECV = 41, 63


def ring(v, k):
    return (v + k + G) % G


def dot(a, b, ca, cb):
    return lax.dot_general(a, b, (((ca,), (cb,)), ((), ())), preferred_element_type=F32)


def span(start, size):
    return pl.ds(start if isinstance(start, int) else pl.multiple_of(start, size), size)


class Net:
    def __init__(self, send_sem, recv_sem):
        rep, node = lax.axis_index("rep"), lax.axis_index("nodes")
        self.z, self.y, self.x, self.c = rep // G, rep % G, node // T, node % T
        self.send_sem, self.recv_sem = send_sem, recv_sem
        self.used, self.ends = 0, []

    def dev(self, **place):
        z, y, x, c = (place.get(k, getattr(self, k)) for k in "zyxc")
        return (z * G + y, x * T + c)

    def near(self, axis, k):
        return self.dev(**{axis: ring(getattr(self, axis), k)})

    def partner(self):
        return self.dev(c=1 - self.c)

    def recv_index(self):
        self.used += 1
        return self.used - 1

    def copy(self, src, dst, device, k, n):
        send, recv = self.send_sem.at[k], self.recv_sem.at[n]
        return pltpu.make_async_remote_copy(src_ref=src, dst_ref=dst, send_sem=send, recv_sem=recv, device_id=device, device_id_type=MESH)

    def send(self, src, dst, device):
        copy = self.copy(src, dst, device, len(self.ends), self.recv_index())
        copy.start()
        self.ends.append(copy)
        return copy

    def flush(self):
        for copy in self.ends:
            copy.wait_send()
        self.ends = []

    def places(self):
        for j in range(G * G):
            m = (j + 1) * 5 % (G * G)
            yield ring(self.z, m // G), ring(self.y, m % G)

    def rep_each(self, src, buf):
        k, n = len(self.ends), self.used
        self.used += G
        mine = buf.at[self.z, self.y]
        self.ends.append(self.copy(buf, buf, self.partner(), k, n))
        for j, (z, y) in enumerate(self.places()):
            self.copy(src, mine, self.dev(z=z, y=y, c=1 - self.c), k, n + j // G).start()

        def each(fn):
            def body(j, _):
                self.copy(buf.at[0], buf.at[0], self.partner(), k, n + j).wait_recv()
                for i in range(G):
                    m = (j * G + i + 1) * 5 % (G * G)
                    fn(ring(self.z, -(m // G)), ring(self.y, -(m % G)))
                return _

            lax.fori_loop(0, G, body, 0)

        return each

    def rep_send(self, src, buf):
        group = Group(self, buf)
        for z, y in self.places():
            group.send(src(z, y), buf.at[self.z, self.y], self.dev(z=z, y=y, c=1 - self.c))
        return group

    def peers(self):
        out = [self.partner()]
        for k in (1, 2, 3):
            out += [self.near(axis, k) for axis in "xyz"]
            out.append(self.dev(x=ring(self.x, k), c=1 - self.c))
        return out


class Group:
    def __init__(self, net, whole):
        self.net, self.k, self.n = net, len(net.ends), net.recv_index()
        self.all = net.copy(whole, whole, net.partner(), self.k, self.n)
        net.ends.append(self.all)

    def send(self, src, dst, device):
        self.net.copy(src, dst, device, self.k, self.n).start()

    def wait_recv(self):
        self.all.wait_recv()


class Tree:
    def __init__(self, net, axis, at, far, near, whole):
        self.net, self.at, self.far, self.near = net, at, far, near
        self.p = getattr(net, axis)
        self.side = net.near(axis, 1), net.near(axis, -1)
        self.whole = whole

    def start(self):
        self.first = [self.net.send(self.at(ring(self.p, T), d), self.far(d), self.side[d]) for d in (0, 1)]
        self.arrive = Group(self.net, self.whole)

    def free(self, d):
        t = ring(self.p, 1 - T * d)
        self.arrive.send(self.at(t, 1 - d), self.near(d, 1 - d), self.side[d])

    def relay(self):
        for d in (0, 1):
            self.first[d].wait_recv()
            mine = self.at(ring(self.p, 1 - T * d), d)
            mine[...] = mine[...] + self.far(d)[...]
            self.arrive.send(mine, self.near(d, d), self.side[d])

    def end(self):
        self.arrive.wait_recv()


class RepSum:
    def __init__(self, net, terms, far, near, mid, last):
        self.net, self.terms, self.near, self.mid, self.last = net, terms, near, mid, last
        self.size, slices = near.shape[-T], near.shape[1]
        self.slices = range(slices)
        q = self.size // T
        self.parts = [(h, s) for s in self.slices for h in (0, 1)]
        self.tree = {}
        for h, s in self.parts:

            def at(t, d, h=h, s=s):
                row = pl.ds((h * slices + s) * self.size + d * q, q)
                return terms.at[t, :, row] if h else terms.at[:, t, row]

            def part(d, e, h=h, s=s):
                return near.at[h, s, d, :, pl.ds(e * q, q)]

            self.tree[h, s] = Tree(net, "yz"[h], at, lambda d, h=h, s=s: far.at[h, s, d], part, near.at[h, s])

    def start(self, h):
        for s in self.slices:
            self.tree[h, s].start()

    def free(self, h, d):
        for s in self.slices:
            self.tree[h, s].free(d)

    def finish(self, out):
        net, size = self.net, self.size
        for part in self.parts:
            self.tree[part].relay()
        arrivals = []
        for h, s in self.parts:
            tree, mid = self.tree[h, s], self.mid.at[h, s]
            tree.end()
            row = pl.ds((h * len(self.slices) + s) * size, size)
            own = self.terms[tree.p, :, row] if h else self.terms[:, tree.p, row]
            mid[...] = own + self.near[h, s, 0] + self.near[h, s, 1]
            axis = "zy"[h]
            arrivals.append(exchange(net, axis, lambda t: mid.at[t], self.last.at[h, s]))
        for (h, s), group in zip(self.parts, arrivals):
            group.wait_recv()
            p = net.y if h else net.z
            total = self.mid[h, s, p]
            for k in (1, 2, 3):
                total = total + self.last[h, s, ring(p, k)]
            out[pl.ds((h * len(self.slices) + s) * size, size)] = total


def exchange(net, axis, src, buf):
    p = getattr(net, axis)
    group = Group(net, buf.at[pl.ds(0, 3)])
    for k in (2, 1, 3):
        group.send(src(ring(p, k)), buf.at[p], net.near(axis, k))
    return group


def wait_all(copies):
    for copy in copies:
        copy.wait_recv()


def gather_nodes(net, buf):
    mine = buf.at[net.x * T + net.c]
    group = Group(net, buf.at[pl.ds(0, N - 1)])
    for k in (2, 1, 3):
        for core in (net.c, 1 - net.c):
            group.send(mine, mine, net.dev(x=ring(net.x, k), c=core))
    group.send(mine, mine, net.partner())
    return group


def gather_pairs(net, buf, done, extra):
    node = lambda k, core: ring(net.x, k) * T + core
    other = 1 - net.c

    def move(n, device):
        return net.send(buf.at[n], buf.at[n], device)

    me = node(0, net.c)
    over = [(node(0, other), move(me, net.partner()))]
    come = [(k, move(me, net.dev(x=ring(net.x, k), c=other))) for k in (2, 1, 3)]
    out = extra()
    done(me)
    for k, copy in come:
        copy.wait_recv()
        over.append((node(-k, net.c), move(node(-k, other), net.partner())))
        done(node(-k, other))
    for n, copy in over:
        copy.wait_recv()
        done(n)
    return out


class Spread:
    def __init__(self, net, buf):
        self.net, self.buf = net, buf
        self.first = [[(k, net.send(ref, ref, device)) for k, ref, device in self.along(h, "yz"[h], net.z, net.y)] for h in (0, 1)]
        self.rest = Group(net, buf.at[pl.ds(0, 3)])
        for h in (0, 1):
            self.cross(h, net.z, net.y)

    def along(self, h, axis, z, y):
        size = self.buf.shape[T] // T
        ref = self.buf.at[z, y, pl.ds(h * size, size)]
        return [(k, ref, self.net.near(axis, k)) for k in (2, 1, 3)]

    def cross(self, h, z, y):
        for _, ref, device in self.along(h, "zy"[h], z, y):
            self.rest.send(ref, ref, device)

    def second(self):
        net = self.net
        for n in range(3):
            for h in (0, 1):
                k, copy = self.first[h][n]
                copy.wait_recv()
                self.cross(h, ring(net.z, -k) if h else net.z, net.y if h else ring(net.y, -k))


def lanes(shape):
    return lax.broadcasted_iota(jnp.int32, shape, len(shape) - 1)


def pack(v):
    return v[:PK] + pltpu.roll(v[PK : T * PK], CLS, 1) + pltpu.roll(v[T * PK :], T * CLS, 1)


def unpack(v):
    keep = lanes((PK, LANE)) < CLS
    parts = [v, pltpu.roll(v, LANE - CLS, 1), pltpu.roll(v, LANE - T * CLS, 1)]
    return [jnp.where(keep, part, 0.0) for part in parts]


def scratch_shapes():
    half, thin, piece = HID // T, ROW // G, CLS + N
    return dict(
        a_v=((G, G, ROW, WIDE), BF16),
        xg=((N, ROW, LANE), BF16),
        cg=((N, N, LANE), F32),
        y1=((WIDE, HID), BF16),
        zp=((G, G, ROW, HID), F32),
        far=((T, T, T, G, thin // T, HID), F32),
        near=((T, T, T, G, thin, HID), F32),
        mid=((T, T, G, thin, HID), F32),
        last=((T, T, G, thin, HID), F32),
        z1=((ROW, HID), F32),
        h1=((ROW, HID), BF16),
        w2p=((LANE, HID), F32),
        y2g=((N, PK, LANE), BF16),
        y2u=((WIDE, LANE), BF16),
        zq=((G, G, PK, LANE), F32),
        zi=((G, G, PK, LANE), F32),
        g2s=((PK, LANE), BF16),
        g2g=((G, G, PK, LANE), BF16),
        g2u=((TALL, LANE), BF16),
        d2=((G, CLS, PAIR), F32),
        d2i=((G, CLS, PAIR), F32),
        d2s=((T, CLS, PAIR), F32),
        d2t=((PAIR, LANE), F32),
        g1g=((G, G, ROW, HID), BF16),
        mg=((G, G, ROW, HID), BF16),
        dys=((PK, LANE), BF16),
        dyg=((G, G, PK, LANE), BF16),
        e1=((G, HID, PAIR), F32),
        e1o=((G, half, PAIR), F32),
        e1s=((G, half, PAIR), F32),
        e1far=((T, T, half // G, PAIR), F32),
        e1near=((T, half, PAIR), F32),
        w2s=((T, piece, LANE), F32),
        w2o=((piece, LANE), F32),
        wx=((G, piece, LANE), F32),
        wr_own=((piece, LANE), F32),
        wr=((G, G, piece, LANE), F32),
        wf=((T, piece, LANE), F32),
        ra=((G, G, N, LANE), F32),
        rai=((G, G, N, LANE), F32),
        rx=((N, LANE), F32),
        rxi=((G, N, LANE), F32),
        rs=((N, LANE), F32),
        rf=((T, G, G, N, LANE), F32),
        w1v=((LANE, HID), F32),
        lab=((ROW,), jnp.int32),
        msk=((ROW,), jnp.int32),
        lab_o=((ROW,), jnp.int32),
        msk_o=((ROW,), jnp.int32),
    )


def kernel(adj, x_ref, w1_ref, w2_ref, lab_ref, msk_ref, out_ref, *scratch):
    names = list(scratch_shapes())
    s = dict(zip(names, scratch))
    send_sem, recv_sem, load_sem = scratch[len(names) :]
    net = Net(send_sem, recv_sem)
    z, y, x, c = net.z, net.y, net.x, net.c
    a_v = s["a_v"]

    barrier = pltpu.get_barrier_semaphore()
    peers = net.peers()
    for peer in peers:
        pl.semaphore_signal(barrier, inc=1, device_id=peer, device_id_type=MESH)

    me = x * T + c
    xg, cg, w2p, w1v, y1 = (s[k] for k in ("xg", "cg", "w2p", "w1v", "y1"))
    w2p[...] = jnp.zeros((LANE, HID), F32)
    pairs = [(msk_ref, s["msk"]), (lab_ref, s["lab"]), (x_ref, xg.at[me]), (w1_ref, w1v), (w2_ref, w2p.at[pl.ds(0, CLS)])]
    pairs += [(adj.at[k], a_v.at[k]) for k in range(G)]
    loads = [pltpu.make_async_copy(src, dst, load_sem.at[k]) for k, (src, dst) in enumerate(pairs)]
    for load in loads:
        load.start()
    small = len(loads) - G
    for load in loads[:small]:
        load.wait()

    def row_of(ref, dtype):
        return ref[...].astype(dtype).reshape(1, ROW)

    cg[me] = jnp.broadcast_to(jnp.sum(row_of(s["msk"], F32), axis=1, keepdims=True), (N, LANE))
    w2b = w2p[...].astype(BF16)
    w1b = w1v[...].astype(BF16)

    pl.semaphore_wait(barrier, len(peers))

    def y1_block(n):
        y1[span(n * ROW, ROW)] = dot(xg[n], w1b, 1, 0).astype(BF16)

    def small_copies():
        swaps = [net.send(s[k], s[k + "_o"], net.partner()) for k in ("lab", "msk")]
        return swaps + [gather_nodes(net, cg)]

    counts = gather_pairs(net, xg, y1_block, small_copies)
    for load in loads[small:]:
        load.wait()

    zp = s["zp"]

    sum1 = RepSum(net, zp, s["far"], s["near"], s["mid"], s["last"])

    def z1_block(h, t):
        row = pl.ds(h * ROW // T, ROW // T)
        a = a_v[t, :, row] if h else a_v[:, t, row]
        term = dot(a.reshape(TALL // N, WIDE), y1[...], 1, 0).reshape(G, ROW // T, HID)
        if h:
            zp[t, :, row] = term
        else:
            zp[:, t, row] = term

    for k in (2, 1, 3, 0):
        for h, p in enumerate((y, z)):
            z1_block(h, ring(p, k))
            if k == T:
                sum1.start(h)
            elif k > 0:
                sum1.free(h, k // T)
    z1 = s["z1"]
    sum1.finish(z1)

    h1 = s["h1"]
    h1[...] = jnp.maximum(z1[...], 0.0).astype(BF16)
    y2 = dot(h1[...], w2b, 1, 1).astype(BF16).astype(F32)
    y2g, y2u = s["y2g"], s["y2u"]
    y2g[me] = pack(y2).astype(BF16)
    blocks = gather_nodes(net, y2g)
    mg = s["mg"]
    mg[z, y] = jnp.where(z1[...] > 0.0, 1.0, 0.0).astype(BF16)
    masks = Spread(net, mg)

    def spread(src, dst, base):
        for g, part in enumerate(unpack(src.astype(F32))):
            dst[span(base * ROW + g * PK, PK)] = part.astype(BF16)

    def spread_y2(j, _):
        spread(y2g[j], y2u, j)
        return _

    wait_all(counts + [blocks])
    lax.fori_loop(0, N, spread_y2, 0)

    zq, zi = s["zq"], s["zi"]
    count = jnp.sum(cg[...], axis=0)[:1]
    at_count = lanes((PK, LANE)) == 3 * CLS
    count = jnp.where(at_count, jnp.broadcast_to(count, (PK, LANE)), 0.0)

    arrivals = Group(net, zi)

    def z2_blocks(j, _):
        dz, p = j // T + 1, T * (j % T)
        zz = ring(z, dz)
        term = dot(a_v[zz, pl.ds(p, T)].reshape(PAIR, WIDE), y2u[...], 1, 0)
        for k in (0, 1):
            zq[zz, p + k] = pack(term[k * ROW : (k + 1) * ROW]) + count
            arrivals.send(zq.at[zz, p + k], zi.at[z, y], net.dev(z=zz, y=p + k, c=1 - c))
        return _

    lax.fori_loop(0, N, z2_blocks, 0)
    mask_row, label_row = row_of(s["msk_o"], F32), row_of(s["lab_o"], jnp.int32)
    mask_all = jnp.broadcast_to(mask_row, (LANE, ROW)).T
    classes = lax.broadcasted_iota(jnp.int32, (LANE, ROW), 0)
    one_hot = (jnp.broadcast_to(label_row, (LANE, ROW)) == classes).astype(F32).T
    arrivals.wait_recv()
    packed = jnp.sum(zi[...].reshape(G * G, PK, LANE), axis=0)

    total = jnp.sum(jnp.where(at_count, packed, 0.0), axis=1, keepdims=True)
    total = jnp.concatenate([total, total, total], axis=0)
    logits = jnp.concatenate(unpack(packed), axis=0)
    valid = lanes((ROW, LANE)) < CLS
    top = jnp.max(jnp.where(valid, logits, -jnp.inf), axis=1, keepdims=True)
    shifted = jnp.where(valid, logits - top, 0.0)
    norm = jnp.sum(jnp.where(valid, jnp.exp(shifted), 0.0), axis=1, keepdims=True)
    log_probs = shifted - jnp.log(norm)
    picked = jnp.where(valid, -(mask_all * (one_hot * log_probs)), 0.0)
    loss_part = jnp.sum(picked, axis=0, keepdims=True)
    g2 = jnp.where(valid, (jnp.exp(log_probs) - one_hot) * (mask_all / total), 0.0).astype(BF16).astype(F32)
    g2s, g2g, g2u = s["g2s"], s["g2g"], s["g2u"]
    g2s[...] = pack(g2).astype(BF16)

    arrivals = net.rep_each(g2s, g2g)
    masks.second()
    arrivals(lambda zz, yy: spread(g2g[zz, yy], g2u, zz * G + yy))

    d2, d2i, d2s, d2t = (s[k] for k in ("d2", "d2i", "d2s", "d2t"))

    def a_cols(k, size):
        return a_v[:, :, :, span(k * size, size)].reshape(TALL, size)

    def d2_block(k):
        part = dot(g2u[...], a_cols(k, T * PAIR), 0, 0)[:CLS]
        d2[T * k] = part[:, :PAIR]
        d2[T * k + 1] = part[:, PAIR:]

    arrivals = Group(net, d2i.at[pl.ds(0, 3)])

    def d2_send(t):
        arrivals.send(d2.at[t], d2i.at[x], net.dev(x=t, c=1 - c))

    d2_block(1 - x // T)
    d2_send(ring(x, T))
    d2_send(3 - x)
    d2_block(x // T)
    d2_send(x + 1 - T * (x % T))
    d2i[x] = d2[x]
    arrivals.wait_recv()
    d2s[c] = jnp.sum(d2i[...], axis=0)
    net.send(d2s.at[c], d2s.at[c], net.partner()).wait_recv()
    d2t[...] = jnp.concatenate([d2s[0] + d2s[1], jnp.zeros((LANE - CLS, PAIR), F32)], axis=0).T

    dys, dyg, g1g = s["dys"], s["dyg"], s["g1g"]
    dys[...] = pack(d2t[span((1 - c) * ROW, ROW)].astype(BF16).astype(F32)).astype(BF16)
    arrivals = net.rep_each(dys, dyg)

    w2s, w2o, wx, wr, wf = (s[k] for k in ("w2s", "w2o", "wx", "wr", "wf"))
    dy2 = d2t[span(c * ROW, ROW)].astype(BF16)
    dw2_t = dot(dy2, h1[...], 0, 0)[:CLS]
    loss_tile = jnp.concatenate([loss_part, jnp.zeros((N - 1, LANE), F32)], axis=0)
    for h in (0, 1):
        w2s[h, :CLS] = dw2_t[:, h * LANE : (h + 1) * LANE]
        w2s[h, CLS:] = loss_tile
    swap = net.send(w2s.at[1 - c], w2o, net.partner())
    masks.rest.wait_recv()
    swap.wait_recv()
    wx[x] = w2s[c] + w2o[...]
    swaps = exchange(net, "x", lambda t: wx.at[x], wx)
    net.flush()

    def g1_block(zz, yy):
        dy = jnp.concatenate(unpack(dyg[zz, yy].astype(F32)), axis=0).astype(BF16)
        dh1 = dot(dy, w2b, 1, 0)
        g1g[zz, yy] = jnp.where(mg[zz, yy].astype(F32) > 0.0, dh1, 0.0).astype(BF16)

    arrivals(g1_block)

    e1, e1o, e1s, e1far, e1near = (s[k] for k in ("e1", "e1o", "e1s", "e1far", "e1near"))
    half = HID // T
    q = half // G

    def tree_of(n):
        part = lambda d: pl.ds((T * n + d) * q, q)
        return Tree(net, "x", lambda t, d: e1s.at[t, part(d)], lambda d: e1far.at[n, d], lambda d, e: e1near.at[d, part(e)], e1near.at[0])

    trees = [tree_of(n) for n in (0, 1)]

    def e1_block(k):
        t = ring(x, k)
        e1[t] = dot(g1g[...].reshape(TALL, HID), a_cols(t, PAIR), 0, 0)
        return t, net.send(e1.at[t, span((1 - c) * half, half)], e1o.at[t], net.partner())

    def e1_join(t, copy):
        copy.wait_recv()
        e1s[t] = e1[t, span(c * half, half)] + e1o[t]

    opposite = e1_block(2)
    right = e1_block(1)
    e1_join(*opposite)
    for tree in trees:
        tree.start()
    left = e1_block(3)
    e1_join(*right)
    for tree in trees:
        tree.free(0)
    own = e1_block(0)
    e1_join(*left)
    for tree in trees:
        tree.free(1)
    e1_join(*own)
    for tree in trees:
        tree.relay()
    swaps.wait_recv()
    wr_own = s["wr_own"]
    wr_own[...] = jnp.sum(wx[...], axis=0)
    w_arrivals = net.rep_send(lambda zz, yy: wr_own, wr)
    for tree in trees:
        tree.end()
    dy1 = (e1s[x] + e1near[0] + e1near[1]).astype(BF16)
    dw1_t = dot(dy1, xg[pl.ds(x * T, T)].reshape(PAIR, LANE), 1, 0)

    ra, rai, rx, rxi, rs, rf = (s[k] for k in ("ra", "rai", "rx", "rxi", "rs", "rf"))
    ra[...] = dw1_t.reshape(G, G, N, LANE)
    arrivals = net.rep_send(lambda zz, yy: ra.at[zz, yy], rai)
    w_arrivals.wait_recv()
    wf[1 - c] = jnp.sum(wr[...].reshape(G * G, CLS + N, LANE), axis=0)
    swap = net.send(wf.at[1 - c], wf.at[1 - c], net.partner())
    arrivals.wait_recv()
    rx[...] = jnp.sum(rai[...].reshape(G * G, N, LANE), axis=0)
    arrivals = Group(net, rxi)
    for k in (2, 1, 3, 0):
        arrivals.send(rx, rxi.at[x], net.dev(x=ring(x, k), c=1 - c))
    arrivals.wait_recv()
    rs[...] = jnp.sum(rxi[...], axis=0)
    arrivals = net.rep_send(lambda zz, yy: rs, rf.at[c])
    swap.wait_recv()
    out_ref[:, span(LANE, CLS + N)] = wf[...]
    out_ref[0, span(LANE + CLS + N, N)] = jnp.broadcast_to(total[:1], (N, LANE))
    arrivals.wait_recv()
    net.send(rf.at[1 - c], rf.at[1 - c], net.partner()).wait_recv()
    out_ref[:, :LANE] = rf[...].reshape(T, LANE, LANE)
    net.flush()


def unpack_kernel(sums, loss_ref, dw1_ref, dw2_ref):
    for h in (0, 1):
        half = span(h * LANE, LANE)
        dw1_ref[:, half] = sums[h, :LANE].T
        dw2_ref[:, half] = sums[h, LANE : LANE + CLS]
    loss = jnp.sum(sums[0, LANE + CLS : LANE + CLS + N])
    loss_ref[0, 0] = loss / jnp.max(sums[0, LANE + CLS + N :])


def solution(mesh):
    vmem, smem = pl.BlockSpec(memory_space=pltpu.VMEM), pl.BlockSpec(memory_space=pltpu.SMEM)
    struct = lambda *shape: jax.ShapeDtypeStruct(shape, F32)

    def device_step(adj_blk, feat_blk, w_one, w_two, label_blk, mask_blk):
        sems = [pltpu.SemaphoreType.DMA((n,)) for n in (N_SEND, N_RECV, N + 1)]
        sums = pl.pallas_call(
            kernel,
            out_shape=struct(T, LANE + CLS + T * N, LANE),
            in_specs=[pl.BlockSpec(memory_space=pl.ANY)] * 6,
            out_specs=vmem,
            scratch_shapes=[pltpu.VMEM(shape, dtype) for shape, dtype in scratch_shapes().values()] + sems,
            compiler_params=pltpu.CompilerParams(collective_id=0, has_side_effects=True, vmem_limit_bytes=56 << 20),
        )(adj_blk.reshape(G, G, ROW, WIDE), feat_blk, w_one, w_two.T, label_blk, mask_blk)
        loss, dw1, dw2 = pl.pallas_call(
            unpack_kernel,
            out_shape=(struct(1, 1), struct(LANE, HID), struct(CLS, HID)),
            in_specs=[vmem],
            out_specs=(smem, vmem, vmem),
        )(sums)
        return loss.reshape(()), dw1, dw2.T

    row_spec = P(("rep", "nodes"))
    return jax.shard_map(
        device_step,
        mesh=mesh,
        in_specs=(P(None, "nodes", "rep"), row_spec, P(), P(), row_spec, row_spec),
        out_specs=(P(), P(), P()),
        check_vma=False,
    )
```

```python
import jax
import jax.numpy as jnp
from jax import lax
from jax.experimental import pallas as pl
from jax.experimental.pallas import tpu as pltpu
from jax.sharding import PartitionSpec as P

MESH = pl.DeviceIdType.MESH
F32, BF16 = jnp.float32, jnp.bfloat16
T, G, N = 2, 4, 8
LANE, HID, CLS, ROW = 128, 256, 40, 192
PK = ROW // 3
TALL, WIDE = 16 * ROW, N * ROW
PAIR = T * ROW
N_SEND, N_RECV = 41, 66


def ring(v, k):
    return (v + k + G) % G


def dot(a, b, ca, cb):
    return lax.dot_general(a, b, (((ca,), (cb,)), ((), ())), preferred_element_type=F32)


def span(start, size):
    return pl.ds(start if isinstance(start, int) else pl.multiple_of(start, size), size)


class Net:
    def __init__(self, send_sem, recv_sem):
        rep, node = lax.axis_index("rep"), lax.axis_index("nodes")
        self.z, self.y, self.x, self.c = rep // G, rep % G, node // T, node % T
        self.send_sem, self.recv_sem = send_sem, recv_sem
        self.used, self.ends = 0, []

    def dev(self, **place):
        z, y, x, c = (place.get(k, getattr(self, k)) for k in "zyxc")
        return (z * G + y, x * T + c)

    def near(self, axis, k):
        return self.dev(**{axis: ring(getattr(self, axis), k)})

    def partner(self):
        return self.dev(c=1 - self.c)

    def recv_index(self):
        self.used += 1
        return self.used - 1

    def copy(self, src, dst, device, k, n):
        send, recv = self.send_sem.at[k], self.recv_sem.at[n]
        return pltpu.make_async_remote_copy(src_ref=src, dst_ref=dst, send_sem=send, recv_sem=recv, device_id=device, device_id_type=MESH)

    def send(self, src, dst, device):
        copy = self.copy(src, dst, device, len(self.ends), self.recv_index())
        copy.start()
        self.ends.append(copy)
        return copy

    def flush(self):
        for copy in self.ends:
            copy.wait_send()
        self.ends = []

    def places(self):
        for j in range(G * G):
            m = (j + 1) * 5 % (G * G)
            yield ring(self.z, m // G), ring(self.y, m % G)

    def rep_each(self, src, buf):
        k, n = len(self.ends), self.used
        self.used += G
        mine = buf.at[self.z, self.y]
        self.ends.append(self.copy(buf, buf, self.partner(), k, n))
        for j, (z, y) in enumerate(self.places()):
            self.copy(src, mine, self.dev(z=z, y=y, c=1 - self.c), k, n + j // G).start()

        def each(fn):
            def body(j, _):
                self.copy(buf.at[0], buf.at[0], self.partner(), k, n + j).wait_recv()
                for i in range(G):
                    m = (j * G + i + 1) * 5 % (G * G)
                    fn(ring(self.z, -(m // G)), ring(self.y, -(m % G)))
                return _

            for j in range(G):
                body(j, 0)

        return each

    def rep_send(self, src, buf):
        group = Group(self, buf)
        for z, y in self.places():
            group.send(src(z, y), buf.at[self.z, self.y], self.dev(z=z, y=y, c=1 - self.c))
        return group

    def peers(self):
        out = [self.partner()]
        for k in (1, 2, 3):
            out += [self.near(axis, k) for axis in "xyz"]
            out.append(self.dev(x=ring(self.x, k), c=1 - self.c))
        return out


class Group:
    def __init__(self, net, whole):
        self.net, self.k, self.n = net, len(net.ends), net.recv_index()
        self.all = net.copy(whole, whole, net.partner(), self.k, self.n)
        net.ends.append(self.all)

    def send(self, src, dst, device):
        self.net.copy(src, dst, device, self.k, self.n).start()

    def wait_recv(self):
        self.all.wait_recv()


class Tree:
    def __init__(self, net, axis, at, far, near, whole):
        self.net, self.at, self.far, self.near = net, at, far, near
        self.p = getattr(net, axis)
        self.side = net.near(axis, 1), net.near(axis, -1)
        self.whole = whole

    def start(self):
        self.first = [self.net.send(self.at(ring(self.p, T), d), self.far(d), self.side[d]) for d in (0, 1)]
        self.arrive = Group(self.net, self.whole)

    def free(self, d):
        t = ring(self.p, 1 - T * d)
        self.arrive.send(self.at(t, 1 - d), self.near(d, 1 - d), self.side[d])

    def relay(self):
        for d in (0, 1):
            self.first[d].wait_recv()
            mine = self.at(ring(self.p, 1 - T * d), d)
            mine[...] = mine[...] + self.far(d)[...]
            self.arrive.send(mine, self.near(d, d), self.side[d])

    def end(self):
        self.arrive.wait_recv()


class RepSum:
    def __init__(self, net, terms, far, near, mid, last):
        self.net, self.terms, self.near, self.mid, self.last = net, terms, near, mid, last
        self.size, slices = near.shape[-T], near.shape[1]
        self.slices = range(slices)
        q = self.size // T
        self.parts = [(h, s) for s in self.slices for h in (0, 1)]
        self.tree = {}
        for h, s in self.parts:

            def at(t, d, h=h, s=s):
                row = pl.ds((h * slices + s) * self.size + d * q, q)
                return terms.at[t, :, row] if h else terms.at[:, t, row]

            def part(d, e, h=h, s=s):
                return near.at[h, s, d, :, pl.ds(e * q, q)]

            self.tree[h, s] = Tree(net, "yz"[h], at, lambda d, h=h, s=s: far.at[h, s, d], part, near.at[h, s])

    def start(self, h):
        for s in self.slices:
            self.tree[h, s].start()

    def free(self, h, d):
        for s in self.slices:
            self.tree[h, s].free(d)

    def finish(self, out):
        net, size = self.net, self.size
        for part in self.parts:
            self.tree[part].relay()
        arrivals = []
        for h, s in self.parts:
            tree, mid = self.tree[h, s], self.mid.at[h, s]
            tree.end()
            row = pl.ds((h * len(self.slices) + s) * size, size)
            own = self.terms[tree.p, :, row] if h else self.terms[:, tree.p, row]
            mid[...] = own + self.near[h, s, 0] + self.near[h, s, 1]
            axis = "zy"[h]
            arrivals.append(exchange(net, axis, lambda t: mid.at[t], self.last.at[h, s]))
        for (h, s), group in zip(self.parts, arrivals):
            group.wait_recv()
            p = net.y if h else net.z
            total = self.mid[h, s, p]
            for k in (1, 2, 3):
                total = total + self.last[h, s, ring(p, k)]
            out[pl.ds((h * len(self.slices) + s) * size, size)] = total


def exchange(net, axis, src, buf):
    p = getattr(net, axis)
    group = Group(net, buf.at[pl.ds(0, 3)])
    for k in (2, 1, 3):
        group.send(src(ring(p, k)), buf.at[p], net.near(axis, k))
    return group


def wait_all(copies):
    for copy in copies:
        copy.wait_recv()


def gather_nodes(net, buf):
    mine = buf.at[net.x * T + net.c]
    group = Group(net, buf.at[pl.ds(0, N - 1)])
    for k in (2, 1, 3):
        for core in (net.c, 1 - net.c):
            group.send(mine, mine, net.dev(x=ring(net.x, k), c=core))
    group.send(mine, mine, net.partner())
    return group


def gather_pairs(net, buf, done, extra):
    node = lambda k, core: ring(net.x, k) * T + core
    other = 1 - net.c

    def move(n, device):
        return net.send(buf.at[n], buf.at[n], device)

    me = node(0, net.c)
    over = [(node(0, other), move(me, net.partner()))]
    come = [(k, move(me, net.dev(x=ring(net.x, k), c=other))) for k in (2, 1, 3)]
    out = extra()
    done(me)
    for k, copy in come:
        copy.wait_recv()
        over.append((node(-k, net.c), move(node(-k, other), net.partner())))
        done(node(-k, other))
    for n, copy in over:
        copy.wait_recv()
        done(n)
    return out


class Spread:
    def __init__(self, net, buf):
        self.net, self.buf = net, buf
        self.first = [[(k, net.send(ref, ref, device)) for k, ref, device in self.along(h, "yz"[h], net.z, net.y)] for h in (0, 1)]
        self.rest = Group(net, buf.at[pl.ds(0, 3)])
        for h in (0, 1):
            self.cross(h, net.z, net.y)

    def along(self, h, axis, z, y):
        size = self.buf.shape[T] // T
        ref = self.buf.at[z, y, pl.ds(h * size, size)]
        return [(k, ref, self.net.near(axis, k)) for k in (2, 1, 3)]

    def cross(self, h, z, y):
        for _, ref, device in self.along(h, "zy"[h], z, y):
            self.rest.send(ref, ref, device)

    def second(self):
        net = self.net
        for n in range(3):
            for h in (0, 1):
                k, copy = self.first[h][n]
                copy.wait_recv()
                self.cross(h, ring(net.z, -k) if h else net.z, net.y if h else ring(net.y, -k))


def lanes(shape):
    return lax.broadcasted_iota(jnp.int32, shape, len(shape) - 1)


def pack(v):
    return v[:PK] + pltpu.roll(v[PK : T * PK], CLS, 1) + pltpu.roll(v[T * PK :], T * CLS, 1)


def unpack(v):
    keep = lanes((PK, LANE)) < CLS
    parts = [v, pltpu.roll(v, LANE - CLS, 1), pltpu.roll(v, LANE - T * CLS, 1)]
    return [jnp.where(keep, part, 0.0) for part in parts]


def scratch_shapes():
    half, thin, piece = HID // T, ROW // G, CLS + N
    return dict(
        a_v=((G, G, ROW, WIDE), BF16),
        xg=((N, ROW, LANE), BF16),
        cg=((N, N, LANE), F32),
        y1=((WIDE, HID), BF16),
        zp=((G, G, ROW, HID), F32),
        far=((T, T, T, G, thin // T, HID), F32),
        near=((T, T, T, G, thin, HID), F32),
        mid=((T, T, G, thin, HID), F32),
        last=((T, T, G, thin, HID), F32),
        z1=((ROW, HID), F32),
        h1=((ROW, HID), BF16),
        w2p=((LANE, HID), F32),
        y2g=((N, PK, LANE), BF16),
        y2u=((WIDE, LANE), BF16),
        zq=((G, G, PK, LANE), F32),
        zi=((G, G, PK, LANE), F32),
        g2s=((PK, LANE), BF16),
        g2g=((G, G, PK, LANE), BF16),
        g2u=((TALL, LANE), BF16),
        d2=((G, CLS, PAIR), F32),
        d2i=((G, CLS, PAIR), F32),
        d2s=((T, CLS, PAIR), F32),
        d2t=((PAIR, LANE), F32),
        g1g=((G, G, ROW, HID), BF16),
        mg=((G, G, ROW, HID), BF16),
        dys=((PK, LANE), BF16),
        dyg=((G, G, PK, LANE), BF16),
        e1=((G, HID, PAIR), F32),
        e1o=((G, half, PAIR), F32),
        e1s=((G, half, PAIR), F32),
        e1far=((T, T, half // G, PAIR), F32),
        e1near=((T, half, PAIR), F32),
        w2s=((T, piece, LANE), F32),
        w2o=((piece, LANE), F32),
        wx=((G, piece, LANE), F32),
        wr_own=((piece, LANE), F32),
        wr=((G, G, piece, LANE), F32),
        wf=((T, piece, LANE), F32),
        ra=((G, G, N, LANE), F32),
        rai=((G, G, N, LANE), F32),
        rx=((N, LANE), F32),
        rxi=((G, N, LANE), F32),
        rs=((N, LANE), F32),
        rf=((T, G, G, N, LANE), F32),
        w1v=((LANE, HID), F32),
        lab=((ROW,), jnp.int32),
        msk=((ROW,), jnp.int32),
        lab_o=((ROW,), jnp.int32),
        msk_o=((ROW,), jnp.int32),
    )


def kernel(adj, x_ref, w1_ref, w2_ref, lab_ref, msk_ref, out_ref, *scratch):
    names = list(scratch_shapes())
    s = dict(zip(names, scratch))
    send_sem, recv_sem, load_sem = scratch[len(names) :]
    net = Net(send_sem, recv_sem)
    z, y, x, c = net.z, net.y, net.x, net.c
    a_v = s["a_v"]

    barrier = pltpu.get_barrier_semaphore()
    peers = net.peers()
    for peer in peers:
        pl.semaphore_signal(barrier, inc=1, device_id=peer, device_id_type=MESH)

    me = x * T + c
    xg, cg, w2p, w1v, y1 = (s[k] for k in ("xg", "cg", "w2p", "w1v", "y1"))
    w2p[...] = jnp.zeros((LANE, HID), F32)
    pairs = [(msk_ref, s["msk"]), (lab_ref, s["lab"]), (x_ref, xg.at[me]), (w1_ref, w1v), (w2_ref, w2p.at[pl.ds(0, CLS)])]
    pairs += [(adj.at[k], a_v.at[k]) for k in range(G)]
    loads = [pltpu.make_async_copy(src, dst, load_sem.at[k]) for k, (src, dst) in enumerate(pairs)]
    for load in loads:
        load.start()
    small = len(loads) - G
    for load in loads[:small]:
        load.wait()

    def row_of(ref, dtype):
        return ref[...].astype(dtype).reshape(1, ROW)

    cg[me] = jnp.broadcast_to(jnp.sum(row_of(s["msk"], F32), axis=1, keepdims=True), (N, LANE))
    w2b = w2p[...].astype(BF16)
    w1b = w1v[...].astype(BF16)

    pl.semaphore_wait(barrier, len(peers))

    def y1_block(n):
        y1[span(n * ROW, ROW)] = dot(xg[n], w1b, 1, 0).astype(BF16)

    def small_copies():
        swaps = [net.send(s[k], s[k + "_o"], net.partner()) for k in ("lab", "msk")]
        return swaps + [gather_nodes(net, cg)]

    counts = gather_pairs(net, xg, y1_block, small_copies)
    for load in loads[small:]:
        load.wait()

    zp = s["zp"]

    sum1 = RepSum(net, zp, s["far"], s["near"], s["mid"], s["last"])

    def z1_block(h, t):
        row = pl.ds(h * ROW // T, ROW // T)
        a = a_v[t, :, row] if h else a_v[:, t, row]
        term = dot(a.reshape(TALL // N, WIDE), y1[...], 1, 0).reshape(G, ROW // T, HID)
        if h:
            zp[t, :, row] = term
        else:
            zp[:, t, row] = term

    for k in (2, 1, 3, 0):
        for h, p in enumerate((y, z)):
            z1_block(h, ring(p, k))
            if k == T:
                sum1.start(h)
            elif k > 0:
                sum1.free(h, k // T)
    z1 = s["z1"]
    sum1.finish(z1)

    h1 = s["h1"]
    h1[...] = jnp.maximum(z1[...], 0.0).astype(BF16)
    y2 = dot(h1[...], w2b, 1, 1).astype(BF16).astype(F32)
    y2g, y2u = s["y2g"], s["y2u"]
    y2g[me] = pack(y2).astype(BF16)
    blocks = gather_nodes(net, y2g)
    mg = s["mg"]
    mg[z, y] = jnp.where(z1[...] > 0.0, 1.0, 0.0).astype(BF16)
    masks = Spread(net, mg)

    def spread(src, dst, base):
        for g, part in enumerate(unpack(src.astype(F32))):
            dst[span(base * ROW + g * PK, PK)] = part.astype(BF16)

    def spread_y2(j, _):
        for i in range(G):
            spread(y2g[j * G + i], y2u, j * G + i)
        return _

    wait_all(counts + [blocks])
    lax.fori_loop(0, T, spread_y2, 0)

    zq, zi = s["zq"], s["zi"]
    count = jnp.sum(cg[...], axis=0)[:1]
    at_count = lanes((PK, LANE)) == 3 * CLS
    count = jnp.where(at_count, jnp.broadcast_to(count, (PK, LANE)), 0.0)

    arrivals = Group(net, zi)

    def z2_blocks(j, _):
        dz, p = j // T + 1, T * (j % T)
        zz = ring(z, dz)
        term = dot(a_v[zz, pl.ds(p, T)].reshape(PAIR, WIDE), y2u[...], 1, 0)
        for k in (0, 1):
            zq[zz, p + k] = pack(term[k * ROW : (k + 1) * ROW]) + count
            arrivals.send(zq.at[zz, p + k], zi.at[z, y], net.dev(z=zz, y=p + k, c=1 - c))
        return _

    lax.fori_loop(0, N, z2_blocks, 0)
    mask_row, label_row = row_of(s["msk_o"], F32), row_of(s["lab_o"], jnp.int32)
    mask_all = jnp.broadcast_to(mask_row, (LANE, ROW)).T
    classes = lax.broadcasted_iota(jnp.int32, (LANE, ROW), 0)
    one_hot = (jnp.broadcast_to(label_row, (LANE, ROW)) == classes).astype(F32).T
    arrivals.wait_recv()
    packed = jnp.sum(zi[...].reshape(G * G, PK, LANE), axis=0)

    total = jnp.sum(jnp.where(at_count, packed, 0.0), axis=1, keepdims=True)
    total = jnp.concatenate([total, total, total], axis=0)
    logits = jnp.concatenate(unpack(packed), axis=0)
    valid = lanes((ROW, LANE)) < CLS
    top = jnp.max(jnp.where(valid, logits, -jnp.inf), axis=1, keepdims=True)
    shifted = jnp.where(valid, logits - top, 0.0)
    norm = jnp.sum(jnp.where(valid, jnp.exp(shifted), 0.0), axis=1, keepdims=True)
    log_probs = shifted - jnp.log(norm)
    picked = jnp.where(valid, -(mask_all * (one_hot * log_probs)), 0.0)
    loss_part = jnp.sum(picked, axis=0, keepdims=True)
    g2 = jnp.where(valid, (jnp.exp(log_probs) - one_hot) * (mask_all / total), 0.0).astype(BF16).astype(F32)
    g2s, g2g, g2u = s["g2s"], s["g2g"], s["g2u"]
    g2s[...] = pack(g2).astype(BF16)

    arrivals = net.rep_each(g2s, g2g)
    masks.second()
    arrivals(lambda zz, yy: spread(g2g[zz, yy], g2u, zz * G + yy))

    d2, d2i, d2s, d2t = (s[k] for k in ("d2", "d2i", "d2s", "d2t"))

    def a_cols(k, size):
        return a_v[:, :, :, span(k * size, size)].reshape(TALL, size)

    def d2_block(k):
        part = dot(g2u[...], a_cols(k, T * PAIR), 0, 0)[:CLS]
        d2[T * k] = part[:, :PAIR]
        d2[T * k + 1] = part[:, PAIR:]

    arrivals = Group(net, d2i.at[pl.ds(0, 3)])

    def d2_send(t):
        arrivals.send(d2.at[t], d2i.at[x], net.dev(x=t, c=1 - c))

    d2_block(1 - x // T)
    d2_send(ring(x, T))
    d2_send(3 - x)
    d2_block(x // T)
    d2_send(x + 1 - T * (x % T))
    d2i[x] = d2[x]
    arrivals.wait_recv()
    d2s[c] = jnp.sum(d2i[...], axis=0)
    net.send(d2s.at[c], d2s.at[c], net.partner()).wait_recv()
    d2t[...] = jnp.concatenate([d2s[0] + d2s[1], jnp.zeros((LANE - CLS, PAIR), F32)], axis=0).T

    dys, dyg, g1g = s["dys"], s["dyg"], s["g1g"]
    dys[...] = pack(d2t[span((1 - c) * ROW, ROW)].astype(BF16).astype(F32)).astype(BF16)
    arrivals = net.rep_each(dys, dyg)

    w2s, w2o, wx, wr, wf = (s[k] for k in ("w2s", "w2o", "wx", "wr", "wf"))
    dy2 = d2t[span(c * ROW, ROW)].astype(BF16)
    dw2_t = dot(dy2, h1[...], 0, 0)[:CLS]
    loss_tile = jnp.concatenate([loss_part, jnp.zeros((N - 1, LANE), F32)], axis=0)
    for h in (0, 1):
        w2s[h, :CLS] = dw2_t[:, h * LANE : (h + 1) * LANE]
        w2s[h, CLS:] = loss_tile
    swap = net.send(w2s.at[1 - c], w2o, net.partner())
    masks.rest.wait_recv()
    swap.wait_recv()
    wx[x] = w2s[c] + w2o[...]
    swaps = exchange(net, "x", lambda t: wx.at[x], wx)
    net.flush()

    def g1_block(zz, yy):
        dy = jnp.concatenate(unpack(dyg[zz, yy].astype(F32)), axis=0).astype(BF16)
        dh1 = dot(dy, w2b, 1, 0)
        g1g[zz, yy] = jnp.where(mg[zz, yy].astype(F32) > 0.0, dh1, 0.0).astype(BF16)

    arrivals(g1_block)

    e1, e1o, e1s, e1far, e1near = (s[k] for k in ("e1", "e1o", "e1s", "e1far", "e1near"))
    half = HID // T
    q = half // G

    def tree_of(n):
        part = lambda d: pl.ds((T * n + d) * q, q)
        return Tree(net, "x", lambda t, d: e1s.at[t, part(d)], lambda d: e1far.at[n, d], lambda d, e: e1near.at[d, part(e)], e1near.at[0])

    trees = [tree_of(n) for n in (0, 1)]

    def e1_block(k):
        t = ring(x, k)
        e1[t] = dot(g1g[...].reshape(TALL, HID), a_cols(t, PAIR), 0, 0)
        return t, net.send(e1.at[t, span((1 - c) * half, half)], e1o.at[t], net.partner())

    def e1_join(t, copy):
        copy.wait_recv()
        e1s[t] = e1[t, span(c * half, half)] + e1o[t]

    opposite = e1_block(2)
    right = e1_block(1)
    e1_join(*opposite)
    for tree in trees:
        tree.start()
    left = e1_block(3)
    e1_join(*right)
    for tree in trees:
        tree.free(0)
    own = e1_block(0)
    e1_join(*left)
    for tree in trees:
        tree.free(1)
    e1_join(*own)
    for tree in trees:
        tree.relay()
    swaps.wait_recv()
    wr_own = s["wr_own"]
    wr_own[...] = jnp.sum(wx[...], axis=0)
    w_arrivals = net.rep_send(lambda zz, yy: wr_own, wr)
    for tree in trees:
        tree.end()
    dy1 = (e1s[x] + e1near[0] + e1near[1]).astype(BF16)
    dw1_t = dot(dy1, xg[pl.ds(x * T, T)].reshape(PAIR, LANE), 1, 0)

    ra, rai, rx, rxi, rs, rf = (s[k] for k in ("ra", "rai", "rx", "rxi", "rs", "rf"))
    ra[...] = dw1_t.reshape(G, G, N, LANE)
    arrivals = net.rep_send(lambda zz, yy: ra.at[zz, yy], rai)
    w_arrivals.wait_recv()
    wf[1 - c] = jnp.sum(wr[...].reshape(G * G, CLS + N, LANE), axis=0)
    swap = net.send(wf.at[1 - c], wf.at[1 - c], net.partner())
    arrivals.wait_recv()
    rx[...] = jnp.sum(rai[...].reshape(G * G, N, LANE), axis=0)
    arrivals = Group(net, rxi)
    for k in (2, 1, 3, 0):
        arrivals.send(rx, rxi.at[x], net.dev(x=ring(x, k), c=1 - c))
    arrivals.wait_recv()
    rs[...] = jnp.sum(rxi[...], axis=0)
    mine = rf.at[c]
    rf[c, z, y] = rs[...]
    arrivals = net.rep_send(lambda zz, yy: rs, mine)
    rows = [Group(net, mine.at[0]) for _ in range(3)] + [Group(net, mine.at[0, pl.ds(0, 3)])]
    for j in range(G * G - 1):
        m = (j + 1) * 5 % (G * G)
        rows[m // G - 1].send(rs, mine.at[z, y], net.dev(z=ring(z, m // G), y=ring(y, m % G)))
    swap.wait_recv()
    out_ref[:, span(LANE, CLS + N)] = wf[...]
    out_ref[0, span(LANE + CLS + N, N)] = jnp.broadcast_to(total[:1], (N, LANE))
    arrivals.wait_recv()
    wait_all(rows)
    out_ref[:, :LANE] = rf[...].reshape(T, LANE, LANE)
    net.flush()


def unpack_kernel(sums, loss_ref, dw1_ref, dw2_ref):
    for h in (0, 1):
        half = span(h * LANE, LANE)
        dw1_ref[:, half] = sums[h, :LANE].T
        dw2_ref[:, half] = sums[h, LANE : LANE + CLS]
    loss = jnp.sum(sums[0, LANE + CLS : LANE + CLS + N])
    loss_ref[0, 0] = loss / jnp.max(sums[0, LANE + CLS + N :])


def solution(mesh):
    vmem, smem = pl.BlockSpec(memory_space=pltpu.VMEM), pl.BlockSpec(memory_space=pltpu.SMEM)
    struct = lambda *shape: jax.ShapeDtypeStruct(shape, F32)

    def device_step(adj_blk, feat_blk, w_one, w_two, label_blk, mask_blk):
        sems = [pltpu.SemaphoreType.DMA((n,)) for n in (N_SEND, N_RECV, N + 1)]
        sums = pl.pallas_call(
            kernel,
            out_shape=struct(T, LANE + CLS + T * N, LANE),
            in_specs=[pl.BlockSpec(memory_space=pl.ANY)] * 6,
            out_specs=vmem,
            scratch_shapes=[pltpu.VMEM(shape, dtype) for shape, dtype in scratch_shapes().values()] + sems,
            compiler_params=pltpu.CompilerParams(collective_id=0, has_side_effects=True, vmem_limit_bytes=56 << 20),
        )(adj_blk.reshape(G, G, ROW, WIDE), feat_blk, w_one, w_two.T, label_blk, mask_blk)
        loss, dw1, dw2 = pl.pallas_call(
            unpack_kernel,
            out_shape=(struct(1, 1), struct(LANE, HID), struct(CLS, HID)),
            in_specs=[vmem],
            out_specs=(smem, vmem, vmem),
        )(sums)
        return loss.reshape(()), dw1, dw2.T

    row_spec = P(("rep", "nodes"))
    return jax.shard_map(
        device_step,
        mesh=mesh,
        in_specs=(P(None, "nodes", "rep"), row_spec, P(), P(), row_spec, row_spec),
        out_specs=(P(), P(), P()),
        check_vma=False,
    )
```

```python
import jax
import jax.numpy as jnp
from jax import lax
from jax.experimental import pallas as pl
from jax.experimental.pallas import tpu as pltpu
from jax.sharding import PartitionSpec as P

MESH = pl.DeviceIdType.MESH
F32, BF16 = jnp.float32, jnp.bfloat16
T, G, N = 2, 4, 8
LANE, HID, CLS, ROW = 128, 256, 40, 192
PK = ROW // 3
TALL, WIDE = 16 * ROW, N * ROW
PAIR = T * ROW
N_SEND, N_RECV = 41, 63


def ring(v, k):
    return (v + k + G) % G


def dot(a, b, ca, cb):
    return lax.dot_general(a, b, (((ca,), (cb,)), ((), ())), preferred_element_type=F32)


def span(start, size):
    return pl.ds(start if isinstance(start, int) else pl.multiple_of(start, size), size)


class Net:
    def __init__(self, send_sem, recv_sem):
        rep, node = lax.axis_index("rep"), lax.axis_index("nodes")
        self.z, self.y, self.x, self.c = rep // G, rep % G, node // T, node % T
        self.send_sem, self.recv_sem = send_sem, recv_sem
        self.used, self.ends = 0, []

    def dev(self, **place):
        z, y, x, c = (place.get(k, getattr(self, k)) for k in "zyxc")
        return (z * G + y, x * T + c)

    def near(self, axis, k):
        return self.dev(**{axis: ring(getattr(self, axis), k)})

    def partner(self):
        return self.dev(c=1 - self.c)

    def recv_index(self):
        self.used += 1
        return self.used - 1

    def copy(self, src, dst, device, k, n):
        send, recv = self.send_sem.at[k], self.recv_sem.at[n]
        return pltpu.make_async_remote_copy(src_ref=src, dst_ref=dst, send_sem=send, recv_sem=recv, device_id=device, device_id_type=MESH)

    def send(self, src, dst, device):
        copy = self.copy(src, dst, device, len(self.ends), self.recv_index())
        copy.start()
        self.ends.append(copy)
        return copy

    def flush(self):
        for copy in self.ends:
            copy.wait_send()
        self.ends = []

    def places(self):
        for j in range(G * G):
            m = (j + 1) * 5 % (G * G)
            yield ring(self.z, m // G), ring(self.y, m % G)

    def rep_each(self, src, buf):
        k, n = len(self.ends), self.used
        self.used += G
        mine = buf.at[self.z, self.y]
        self.ends.append(self.copy(buf, buf, self.partner(), k, n))
        for j, (z, y) in enumerate(self.places()):
            self.copy(src, mine, self.dev(z=z, y=y, c=1 - self.c), k, n + j // G).start()

        def each(fn):
            def body(j, _):
                self.copy(buf.at[0], buf.at[0], self.partner(), k, n + j).wait_recv()
                for i in range(G):
                    m = (j * G + i + 1) * 5 % (G * G)
                    fn(ring(self.z, -(m // G)), ring(self.y, -(m % G)))
                return _

            for j in range(G):
                body(j, 0)

        return each

    def rep_send(self, src, buf):
        group = Group(self, buf)
        for z, y in self.places():
            group.send(src(z, y), buf.at[self.z, self.y], self.dev(z=z, y=y, c=1 - self.c))
        return group

    def peers(self):
        out = [self.partner()]
        for k in (1, 2, 3):
            out += [self.near(axis, k) for axis in "xyz"]
            out.append(self.dev(x=ring(self.x, k), c=1 - self.c))
        return out


class Group:
    def __init__(self, net, whole):
        self.net, self.k, self.n = net, len(net.ends), net.recv_index()
        self.all = net.copy(whole, whole, net.partner(), self.k, self.n)
        net.ends.append(self.all)

    def send(self, src, dst, device):
        self.net.copy(src, dst, device, self.k, self.n).start()

    def wait_recv(self):
        self.all.wait_recv()


class Tree:
    def __init__(self, net, axis, at, far, near, whole):
        self.net, self.at, self.far, self.near = net, at, far, near
        self.p = getattr(net, axis)
        self.side = net.near(axis, 1), net.near(axis, -1)
        self.whole = whole

    def start(self):
        self.first = [self.net.send(self.at(ring(self.p, T), d), self.far(d), self.side[d]) for d in (0, 1)]
        self.arrive = Group(self.net, self.whole)

    def free(self, d):
        t = ring(self.p, 1 - T * d)
        self.arrive.send(self.at(t, 1 - d), self.near(d, 1 - d), self.side[d])

    def relay(self):
        for d in (0, 1):
            self.first[d].wait_recv()
            mine = self.at(ring(self.p, 1 - T * d), d)
            mine[...] = mine[...] + self.far(d)[...]
            self.arrive.send(mine, self.near(d, d), self.side[d])

    def end(self):
        self.arrive.wait_recv()


class RepSum:
    def __init__(self, net, terms, far, near, mid, last):
        self.net, self.terms, self.near, self.mid, self.last = net, terms, near, mid, last
        self.size, slices = near.shape[-T], near.shape[1]
        self.slices = range(slices)
        q = self.size // T
        self.parts = [(h, s) for s in self.slices for h in (0, 1)]
        self.tree = {}
        for h, s in self.parts:

            def at(t, d, h=h, s=s):
                row = pl.ds((h * slices + s) * self.size + d * q, q)
                return terms.at[t, :, row] if h else terms.at[:, t, row]

            def part(d, e, h=h, s=s):
                return near.at[h, s, d, :, pl.ds(e * q, q)]

            self.tree[h, s] = Tree(net, "yz"[h], at, lambda d, h=h, s=s: far.at[h, s, d], part, near.at[h, s])

    def start(self, h):
        for s in self.slices:
            self.tree[h, s].start()

    def free(self, h, d):
        for s in self.slices:
            self.tree[h, s].free(d)

    def finish(self, out):
        net, size = self.net, self.size
        for part in self.parts:
            self.tree[part].relay()
        arrivals = []
        for h, s in self.parts:
            tree, mid = self.tree[h, s], self.mid.at[h, s]
            tree.end()
            row = pl.ds((h * len(self.slices) + s) * size, size)
            own = self.terms[tree.p, :, row] if h else self.terms[:, tree.p, row]
            mid[...] = own + self.near[h, s, 0] + self.near[h, s, 1]
            axis = "zy"[h]
            arrivals.append(exchange(net, axis, lambda t: mid.at[t], self.last.at[h, s]))
        for (h, s), group in zip(self.parts, arrivals):
            group.wait_recv()
            p = net.y if h else net.z
            total = self.mid[h, s, p]
            for k in (1, 2, 3):
                total = total + self.last[h, s, ring(p, k)]
            out[pl.ds((h * len(self.slices) + s) * size, size)] = total


def exchange(net, axis, src, buf):
    p = getattr(net, axis)
    group = Group(net, buf.at[pl.ds(0, 3)])
    for k in (2, 1, 3):
        group.send(src(ring(p, k)), buf.at[p], net.near(axis, k))
    return group


def wait_all(copies):
    for copy in copies:
        copy.wait_recv()


def gather_nodes(net, buf, place=None):
    mine = buf.at[net.x * T + net.c if place is None else place]
    group = Group(net, buf.at[pl.ds(0, N - 1)])
    for k in (2, 1, 3):
        for core in (net.c, 1 - net.c):
            group.send(mine, mine, net.dev(x=ring(net.x, k), c=core))
    group.send(mine, mine, net.partner())
    return group


def gather_pairs(net, buf, done, extra):
    node = lambda k, core: ring(net.x, k) * T + core
    other = 1 - net.c

    def move(n, device):
        return net.send(buf.at[n], buf.at[n], device)

    me = node(0, net.c)
    over = [(node(0, other), move(me, net.partner()))]
    come = [(k, move(me, net.dev(x=ring(net.x, k), c=other))) for k in (2, 1, 3)]
    out = extra()
    done(me)
    for k, copy in come:
        copy.wait_recv()
        over.append((node(-k, net.c), move(node(-k, other), net.partner())))
        done(node(-k, other))
    for n, copy in over:
        copy.wait_recv()
        done(n)
    return out


class Spread:
    def __init__(self, net, buf):
        self.net, self.buf = net, buf
        self.first = [[(k, net.send(ref, ref, device)) for k, ref, device in self.along(h, "yz"[h], net.z, net.y)] for h in (0, 1)]
        self.rest = Group(net, buf.at[pl.ds(0, 3)])
        for h in (0, 1):
            self.cross(h, net.z, net.y)

    def along(self, h, axis, z, y):
        size = self.buf.shape[T] // T
        ref = self.buf.at[z, y, pl.ds(h * size, size)]
        return [(k, ref, self.net.near(axis, k)) for k in (2, 1, 3)]

    def cross(self, h, z, y):
        for _, ref, device in self.along(h, "zy"[h], z, y):
            self.rest.send(ref, ref, device)

    def second(self):
        net = self.net
        for n in range(3):
            for h in (0, 1):
                k, copy = self.first[h][n]
                copy.wait_recv()
                self.cross(h, ring(net.z, -k) if h else net.z, net.y if h else ring(net.y, -k))


def lanes(shape):
    return lax.broadcasted_iota(jnp.int32, shape, len(shape) - 1)


def pack(v):
    return v[:PK] + pltpu.roll(v[PK : T * PK], CLS, 1) + pltpu.roll(v[T * PK :], T * CLS, 1)


def unpack(v):
    keep = lanes((PK, LANE)) < CLS
    parts = [v, pltpu.roll(v, LANE - CLS, 1), pltpu.roll(v, LANE - T * CLS, 1)]
    return [jnp.where(keep, part, 0.0) for part in parts]


def scratch_shapes():
    half, thin, piece = HID // T, ROW // G, CLS + N
    return dict(
        a_v=((G, G, ROW, WIDE), BF16),
        xg=((N, ROW, LANE), BF16),
        cg=((N, N, LANE), F32),
        y1=((WIDE, HID), BF16),
        zp=((G, G, ROW, HID), F32),
        far=((T, T, T, G, thin // T, HID), F32),
        near=((T, T, T, G, thin, HID), F32),
        mid=((T, T, G, thin, HID), F32),
        last=((T, T, G, thin, HID), F32),
        z1=((ROW, HID), F32),
        h1=((ROW, HID), BF16),
        w2p=((LANE, HID), F32),
        y2g=((N, PK, LANE), BF16),
        y2u=((WIDE, LANE), BF16),
        zq=((G, G, PK, LANE), F32),
        zi=((G, G, PK, LANE), F32),
        g2s=((PK, LANE), BF16),
        g2g=((G, G, PK, LANE), BF16),
        g2u=((TALL, LANE), BF16),
        d2=((G, CLS, PAIR), F32),
        d2i=((G, CLS, PAIR), F32),
        d2s=((T, CLS, PAIR), F32),
        d2t=((PAIR, LANE), F32),
        g1g=((G, G, ROW, HID), BF16),
        mg=((G, G, ROW, HID), BF16),
        dys=((PK, LANE), BF16),
        dyg=((G, G, PK, LANE), BF16),
        e1=((3, HID, WIDE // 3), F32),
        e1o=((3, half, WIDE // 3), F32),
        e1s=((3, half, WIDE // 3), F32),
        e1far=((3, T, half // N, WIDE // 3), F32),
        e1near=((3, T, half // G, WIDE // 3), F32),
        w2s=((T, piece, LANE), F32),
        w2o=((piece, LANE), F32),
        wx=((G, piece, LANE), F32),
        wr_own=((piece, LANE), F32),
        wr=((G, G, piece, LANE), F32),
        wf=((T, piece, LANE), F32),
        ra=((half // G, LANE), F32),
        rai=((G, G, half // G, LANE), F32),
        rf=((N, half // G, LANE), F32),
        w1v=((LANE, HID), F32),
        lab=((ROW,), jnp.int32),
        msk=((ROW,), jnp.int32),
        lab_o=((ROW,), jnp.int32),
        msk_o=((ROW,), jnp.int32),
    )


def kernel(adj, x_ref, w1_ref, w2_ref, lab_ref, msk_ref, out_ref, *scratch):
    names = list(scratch_shapes())
    s = dict(zip(names, scratch))
    send_sem, recv_sem, load_sem = scratch[len(names) :]
    net = Net(send_sem, recv_sem)
    z, y, x, c = net.z, net.y, net.x, net.c
    a_v = s["a_v"]

    barrier = pltpu.get_barrier_semaphore()
    peers = net.peers()
    for peer in peers:
        pl.semaphore_signal(barrier, inc=1, device_id=peer, device_id_type=MESH)

    me = x * T + c
    xg, cg, w2p, w1v, y1 = (s[k] for k in ("xg", "cg", "w2p", "w1v", "y1"))
    w2p[...] = jnp.zeros((LANE, HID), F32)
    pairs = [(msk_ref, s["msk"]), (lab_ref, s["lab"]), (x_ref, xg.at[me]), (w1_ref, w1v), (w2_ref, w2p.at[pl.ds(0, CLS)])]
    pairs += [(adj.at[k], a_v.at[k]) for k in range(G)]
    loads = [pltpu.make_async_copy(src, dst, load_sem.at[k]) for k, (src, dst) in enumerate(pairs)]
    for load in loads:
        load.start()
    small = len(loads) - G
    for load in loads[:small]:
        load.wait()

    def row_of(ref, dtype):
        return ref[...].astype(dtype).reshape(1, ROW)

    cg[me] = jnp.broadcast_to(jnp.sum(row_of(s["msk"], F32), axis=1, keepdims=True), (N, LANE))
    w2b = w2p[...].astype(BF16)
    w1b = w1v[...].astype(BF16)

    pl.semaphore_wait(barrier, len(peers))

    def y1_block(n):
        y1[span(n * ROW, ROW)] = dot(xg[n], w1b, 1, 0).astype(BF16)

    def small_copies():
        swaps = [net.send(s[k], s[k + "_o"], net.partner()) for k in ("lab", "msk")]
        return swaps + [gather_nodes(net, cg)]

    counts = gather_pairs(net, xg, y1_block, small_copies)
    for load in loads[small:]:
        load.wait()

    zp = s["zp"]

    sum1 = RepSum(net, zp, s["far"], s["near"], s["mid"], s["last"])

    def z1_block(h, t):
        row = pl.ds(h * ROW // T, ROW // T)
        a = a_v[t, :, row] if h else a_v[:, t, row]
        term = dot(a.reshape(TALL // N, WIDE), y1[...], 1, 0).reshape(G, ROW // T, HID)
        if h:
            zp[t, :, row] = term
        else:
            zp[:, t, row] = term

    for k in (2, 1, 3, 0):
        for h, p in enumerate((y, z)):
            z1_block(h, ring(p, k))
            if k == T:
                sum1.start(h)
            elif k > 0:
                sum1.free(h, k // T)
    z1 = s["z1"]
    sum1.finish(z1)

    h1 = s["h1"]
    h1[...] = jnp.maximum(z1[...], 0.0).astype(BF16)
    y2 = dot(h1[...], w2b, 1, 1).astype(BF16).astype(F32)
    y2g, y2u = s["y2g"], s["y2u"]
    y2g[me] = pack(y2).astype(BF16)
    blocks = gather_nodes(net, y2g)
    mg = s["mg"]
    mg[z, y] = jnp.where(z1[...] > 0.0, 1.0, 0.0).astype(BF16)
    masks = Spread(net, mg)

    def spread(src, dst, base):
        for g, part in enumerate(unpack(src.astype(F32))):
            dst[span(base * ROW + g * PK, PK)] = part.astype(BF16)

    def spread_y2(j, _):
        for i in range(G):
            spread(y2g[j * G + i], y2u, j * G + i)
        return _

    wait_all(counts + [blocks])
    lax.fori_loop(0, T, spread_y2, 0)

    zq, zi = s["zq"], s["zi"]
    count = jnp.sum(cg[...], axis=0)[:1]
    at_count = lanes((PK, LANE)) == 3 * CLS
    count = jnp.where(at_count, jnp.broadcast_to(count, (PK, LANE)), 0.0)

    arrivals = Group(net, zi)

    def z2_blocks(j, _):
        dz, p = j // T + 1, T * (j % T)
        zz = ring(z, dz)
        term = dot(a_v[zz, pl.ds(p, T)].reshape(PAIR, WIDE), y2u[...], 1, 0)
        for k in (0, 1):
            zq[zz, p + k] = pack(term[k * ROW : (k + 1) * ROW]) + count
            arrivals.send(zq.at[zz, p + k], zi.at[z, y], net.dev(z=zz, y=p + k, c=1 - c))
        return _

    lax.fori_loop(0, N, z2_blocks, 0)
    mask_row, label_row = row_of(s["msk_o"], F32), row_of(s["lab_o"], jnp.int32)
    mask_all = jnp.broadcast_to(mask_row, (LANE, ROW)).T
    classes = lax.broadcasted_iota(jnp.int32, (LANE, ROW), 0)
    one_hot = (jnp.broadcast_to(label_row, (LANE, ROW)) == classes).astype(F32).T
    arrivals.wait_recv()
    packed = jnp.sum(zi[...].reshape(G * G, PK, LANE), axis=0)

    total = jnp.sum(jnp.where(at_count, packed, 0.0), axis=1, keepdims=True)
    total = jnp.concatenate([total, total, total], axis=0)
    logits = jnp.concatenate(unpack(packed), axis=0)
    valid = lanes((ROW, LANE)) < CLS
    top = jnp.max(jnp.where(valid, logits, -jnp.inf), axis=1, keepdims=True)
    shifted = jnp.where(valid, logits - top, 0.0)
    norm = jnp.sum(jnp.where(valid, jnp.exp(shifted), 0.0), axis=1, keepdims=True)
    log_probs = shifted - jnp.log(norm)
    picked = jnp.where(valid, -(mask_all * (one_hot * log_probs)), 0.0)
    loss_part = jnp.sum(picked, axis=0, keepdims=True)
    g2 = jnp.where(valid, (jnp.exp(log_probs) - one_hot) * (mask_all / total), 0.0).astype(BF16).astype(F32)
    g2s, g2g, g2u = s["g2s"], s["g2g"], s["g2u"]
    g2s[...] = pack(g2).astype(BF16)

    arrivals = net.rep_each(g2s, g2g)
    masks.second()
    arrivals(lambda zz, yy: spread(g2g[zz, yy], g2u, zz * G + yy))

    d2, d2i, d2s, d2t = (s[k] for k in ("d2", "d2i", "d2s", "d2t"))

    def a_cols(k, size):
        return a_v[:, :, :, span(k * size, size)].reshape(TALL, size)

    def d2_block(k):
        part = dot(g2u[...], a_cols(k, T * PAIR), 0, 0)[:CLS]
        d2[T * k] = part[:, :PAIR]
        d2[T * k + 1] = part[:, PAIR:]

    arrivals = Group(net, d2i.at[pl.ds(0, 3)])

    def d2_send(t):
        arrivals.send(d2.at[t], d2i.at[x], net.dev(x=t, c=1 - c))

    d2_block(1 - x // T)
    d2_send(ring(x, T))
    d2_send(3 - x)
    d2_block(x // T)
    d2_send(x + 1 - T * (x % T))
    d2i[x] = d2[x]
    arrivals.wait_recv()
    d2s[c] = jnp.sum(d2i[...], axis=0)
    net.send(d2s.at[c], d2s.at[c], net.partner()).wait_recv()
    d2t[...] = jnp.concatenate([d2s[0] + d2s[1], jnp.zeros((LANE - CLS, PAIR), F32)], axis=0).T

    dys, dyg, g1g = s["dys"], s["dyg"], s["g1g"]
    dys[...] = pack(d2t[span((1 - c) * ROW, ROW)].astype(BF16).astype(F32)).astype(BF16)
    arrivals = net.rep_each(dys, dyg)

    w2s, w2o, wx, wr, wf = (s[k] for k in ("w2s", "w2o", "wx", "wr", "wf"))
    dy2 = d2t[span(c * ROW, ROW)].astype(BF16)
    dw2_t = dot(dy2, h1[...], 0, 0)[:CLS]
    loss_tile = jnp.concatenate([loss_part, jnp.zeros((N - 1, LANE), F32)], axis=0)
    for h in (0, 1):
        w2s[h, :CLS] = dw2_t[:, h * LANE : (h + 1) * LANE]
        w2s[h, CLS:] = loss_tile
    swap = net.send(w2s.at[1 - c], w2o, net.partner())
    masks.rest.wait_recv()
    swap.wait_recv()
    wx[x] = w2s[c] + w2o[...]
    swaps = exchange(net, "x", lambda t: wx.at[x], wx)
    net.flush()

    def g1_block(zz, yy):
        dy = jnp.concatenate(unpack(dyg[zz, yy].astype(F32)), axis=0).astype(BF16)
        dh1 = dot(dy, w2b, 1, 0)
        g1g[zz, yy] = jnp.where(mg[zz, yy].astype(F32) > 0.0, dh1, 0.0).astype(BF16)

    arrivals(g1_block)

    e1, e1o, e1s, e1far, e1near = (s[k] for k in ("e1", "e1o", "e1s", "e1far", "e1near"))
    half, size = HID // T, HID // N
    q = size // T

    def tree_of(n):
        part = lambda t, d: span(t * size + d * q, q)
        at = lambda t, d: e1s.at[n, part(t, d)]
        return Tree(net, "x", at, lambda d: e1far.at[n, d], lambda d, e: e1near.at[n, d, pl.ds(e * q, q)], e1near.at[n])

    trees = [tree_of(n) for n in range(3)]
    wide = WIDE // 3

    def e1_block(n):
        e1[n] = dot(g1g[...].reshape(TALL, HID), a_cols(n, wide), 0, 0)
        return net.send(e1.at[n, span((1 - c) * half, half)], e1o.at[n], net.partner())

    def e1_join(n, copy):
        copy.wait_recv()
        e1s[n] = e1[n, span(c * half, half)] + e1o[n]
        trees[n].start()

    def free(tree):
        tree.free(0)
        tree.free(1)

    ahead = e1_block(0)
    for n in (1, 2):
        later = e1_block(n)
        e1_join(n - 1, ahead)
        ahead = later
    free(trees[0])
    e1_join(2, ahead)
    free(trees[1])
    free(trees[2])
    for tree in trees:
        tree.relay()
    swaps.wait_recv()
    wr_own = s["wr_own"]
    wr_own[...] = jnp.sum(wx[...], axis=0)
    w_arrivals = net.rep_send(lambda zz, yy: wr_own, wr)
    dw1_t = []
    for n, tree in enumerate(trees):
        tree.end()
        dy1 = (e1s[n, span(x * size, size)] + e1near[n, 0] + e1near[n, 1]).astype(BF16)
        dw1_t.append(dot(dy1, xg[...].reshape(WIDE, LANE)[n * wide : (n + 1) * wide], 1, 0))

    ra, rai, rf = s["ra"], s["rai"], s["rf"]
    ra[...] = dw1_t[0] + dw1_t[1] + dw1_t[2]
    arrivals = net.rep_send(lambda zz, yy: ra, rai)
    w_arrivals.wait_recv()
    wf[1 - c] = jnp.sum(wr[...].reshape(G * G, CLS + N, LANE), axis=0)
    swap = net.send(wf.at[1 - c], wf.at[1 - c], net.partner())
    arrivals.wait_recv()
    place = (1 - c) * G + x
    rf[place] = jnp.sum(rai[...].reshape(G * G, size, LANE), axis=0)
    arrivals = gather_nodes(net, rf, place)
    swap.wait_recv()
    out_ref[:, span(LANE, CLS + N)] = wf[...]
    out_ref[0, span(LANE + CLS + N, N)] = jnp.broadcast_to(total[:1], (N, LANE))
    arrivals.wait_recv()
    out_ref[:, :LANE] = rf[...].reshape(T, LANE, LANE)
    net.flush()


def unpack_kernel(sums, loss_ref, dw1_ref, dw2_ref):
    for h in (0, 1):
        half = span(h * LANE, LANE)
        dw1_ref[:, half] = sums[h, :LANE].T
        dw2_ref[:, half] = sums[h, LANE : LANE + CLS]
    loss = jnp.sum(sums[0, LANE + CLS : LANE + CLS + N])
    loss_ref[0, 0] = loss / jnp.max(sums[0, LANE + CLS + N :])


def solution(mesh):
    vmem, smem = pl.BlockSpec(memory_space=pltpu.VMEM), pl.BlockSpec(memory_space=pltpu.SMEM)
    struct = lambda *shape: jax.ShapeDtypeStruct(shape, F32)

    def device_step(adj_blk, feat_blk, w_one, w_two, label_blk, mask_blk):
        sems = [pltpu.SemaphoreType.DMA((n,)) for n in (N_SEND, N_RECV, N + 1)]
        sums = pl.pallas_call(
            kernel,
            out_shape=struct(T, LANE + CLS + T * N, LANE),
            in_specs=[pl.BlockSpec(memory_space=pl.ANY)] * 6,
            out_specs=vmem,
            scratch_shapes=[pltpu.VMEM(shape, dtype) for shape, dtype in scratch_shapes().values()] + sems,
            compiler_params=pltpu.CompilerParams(collective_id=0, has_side_effects=True, vmem_limit_bytes=56 << 20),
        )(adj_blk.reshape(G, G, ROW, WIDE), feat_blk, w_one, w_two.T, label_blk, mask_blk)
        loss, dw1, dw2 = pl.pallas_call(
            unpack_kernel,
            out_shape=(struct(1, 1), struct(LANE, HID), struct(CLS, HID)),
            in_specs=[vmem],
            out_specs=(smem, vmem, vmem),
        )(sums)
        return loss.reshape(()), dw1, dw2.T

    row_spec = P(("rep", "nodes"))
    return jax.shard_map(
        device_step,
        mesh=mesh,
        in_specs=(P(None, "nodes", "rep"), row_spec, P(), P(), row_spec, row_spec),
        out_specs=(P(), P(), P()),
        check_vma=False,
    )
```

```python
import jax
import jax.numpy as jnp
from jax import lax
from jax.experimental import pallas as pl
from jax.experimental.pallas import tpu as pltpu
from jax.sharding import PartitionSpec as P

MESH = pl.DeviceIdType.MESH
F32, BF16 = jnp.float32, jnp.bfloat16
T, G, N = 2, 4, 8
LANE, HID, CLS, ROW = 128, 256, 40, 192
PK = ROW // 3
TALL, WIDE = 16 * ROW, N * ROW
PAIR = T * ROW
N_SEND, N_RECV = 41, 63


def ring(v, k):
    return (v + k + G) % G


def dot(a, b, ca, cb):
    return lax.dot_general(a, b, (((ca,), (cb,)), ((), ())), preferred_element_type=F32)


def span(start, size):
    return pl.ds(start if isinstance(start, int) else pl.multiple_of(start, size), size)


class Net:
    def __init__(self, send_sem, recv_sem):
        rep, node = lax.axis_index("rep"), lax.axis_index("nodes")
        self.z, self.y, self.x, self.c = rep // G, rep % G, node // T, node % T
        self.send_sem, self.recv_sem = send_sem, recv_sem
        self.used, self.ends = 0, []

    def dev(self, **place):
        z, y, x, c = (place.get(k, getattr(self, k)) for k in "zyxc")
        return (z * G + y, x * T + c)

    def near(self, axis, k):
        return self.dev(**{axis: ring(getattr(self, axis), k)})

    def partner(self):
        return self.dev(c=1 - self.c)

    def recv_index(self):
        self.used += 1
        return self.used - 1

    def copy(self, src, dst, device, k, n):
        send, recv = self.send_sem.at[k], self.recv_sem.at[n]
        return pltpu.make_async_remote_copy(src_ref=src, dst_ref=dst, send_sem=send, recv_sem=recv, device_id=device, device_id_type=MESH)

    def send(self, src, dst, device):
        copy = self.copy(src, dst, device, len(self.ends), self.recv_index())
        copy.start()
        self.ends.append(copy)
        return copy

    def flush(self):
        for copy in self.ends:
            copy.wait_send()
        self.ends = []

    def places(self):
        for j in range(G * G):
            m = (j + 1) * 5 % (G * G)
            yield ring(self.z, m // G), ring(self.y, m % G)

    def rep_each(self, src, buf):
        k, n = len(self.ends), self.used
        self.used += G
        mine = buf.at[self.z, self.y]
        self.ends.append(self.copy(buf, buf, self.partner(), k, n))
        for j, (z, y) in enumerate(self.places()):
            self.copy(src, mine, self.dev(z=z, y=y, c=1 - self.c), k, n + j // G).start()

        def each(fn):
            def body(j, _):
                self.copy(buf.at[0], buf.at[0], self.partner(), k, n + j).wait_recv()
                for i in range(G):
                    m = (j * G + i + 1) * 5 % (G * G)
                    fn(ring(self.z, -(m // G)), ring(self.y, -(m % G)))
                return _

            for j in range(G):
                body(j, 0)

        return each

    def rep_send(self, src, buf):
        group = Group(self, buf)
        for z, y in self.places():
            group.send(src(z, y), buf.at[self.z, self.y], self.dev(z=z, y=y, c=1 - self.c))
        return group

    def peers(self):
        out = [self.partner()]
        for k in (1, 2, 3):
            out += [self.near(axis, k) for axis in "xyz"]
            out.append(self.dev(x=ring(self.x, k), c=1 - self.c))
        return out


class Group:
    def __init__(self, net, whole):
        self.net, self.k, self.n = net, len(net.ends), net.recv_index()
        self.all = net.copy(whole, whole, net.partner(), self.k, self.n)
        net.ends.append(self.all)

    def send(self, src, dst, device):
        self.net.copy(src, dst, device, self.k, self.n).start()

    def wait_recv(self):
        self.all.wait_recv()


class Tree:
    def __init__(self, net, axis, at, far, near, whole):
        self.net, self.at, self.far, self.near = net, at, far, near
        self.p = getattr(net, axis)
        self.side = net.near(axis, 1), net.near(axis, -1)
        self.whole = whole

    def start(self):
        self.first = [self.net.send(self.at(ring(self.p, T), d), self.far(d), self.side[d]) for d in (0, 1)]
        self.arrive = Group(self.net, self.whole)

    def free(self, d):
        t = ring(self.p, 1 - T * d)
        self.arrive.send(self.at(t, 1 - d), self.near(d, 1 - d), self.side[d])

    def relay(self):
        for d in (0, 1):
            self.first[d].wait_recv()
            mine = self.at(ring(self.p, 1 - T * d), d)
            mine[...] = mine[...] + self.far(d)[...]
            self.arrive.send(mine, self.near(d, d), self.side[d])

    def end(self):
        self.arrive.wait_recv()


class RepSum:
    def __init__(self, net, terms, far, near, mid, last):
        self.net, self.terms, self.near, self.mid, self.last = net, terms, near, mid, last
        self.size, slices = near.shape[-T], near.shape[1]
        self.slices = range(slices)
        q = self.size // T
        self.parts = [(h, s) for s in self.slices for h in (0, 1)]
        self.tree = {}
        for h, s in self.parts:

            def at(t, d, h=h, s=s):
                row = pl.ds((h * slices + s) * self.size + d * q, q)
                return terms.at[t, :, row] if h else terms.at[:, t, row]

            def part(d, e, h=h, s=s):
                return near.at[h, s, d, :, pl.ds(e * q, q)]

            self.tree[h, s] = Tree(net, "yz"[h], at, lambda d, h=h, s=s: far.at[h, s, d], part, near.at[h, s])

    def start(self, h):
        for s in self.slices:
            self.tree[h, s].start()

    def free(self, h, d):
        for s in self.slices:
            self.tree[h, s].free(d)

    def finish(self, out):
        net, size = self.net, self.size
        for part in self.parts:
            self.tree[part].relay()
        arrivals = []
        for h, s in self.parts:
            tree, mid = self.tree[h, s], self.mid.at[h, s]
            tree.end()
            row = pl.ds((h * len(self.slices) + s) * size, size)
            own = self.terms[tree.p, :, row] if h else self.terms[:, tree.p, row]
            mid[...] = own + self.near[h, s, 0] + self.near[h, s, 1]
            axis = "zy"[h]
            arrivals.append(exchange(net, axis, lambda t: mid.at[t], self.last.at[h, s]))
        for (h, s), group in zip(self.parts, arrivals):
            group.wait_recv()
            p = net.y if h else net.z
            total = self.mid[h, s, p]
            for k in (1, 2, 3):
                total = total + self.last[h, s, ring(p, k)]
            out[pl.ds((h * len(self.slices) + s) * size, size)] = total


def exchange(net, axis, src, buf):
    p = getattr(net, axis)
    group = Group(net, buf.at[pl.ds(0, 3)])
    for k in (2, 1, 3):
        group.send(src(ring(p, k)), buf.at[p], net.near(axis, k))
    return group


def wait_all(copies):
    for copy in copies:
        copy.wait_recv()


def gather_nodes(net, buf, place=None):
    mine = buf.at[net.x * T + net.c if place is None else place]
    group = Group(net, buf.at[pl.ds(0, N - 1)])
    for k in (2, 1, 3):
        for core in (net.c, 1 - net.c):
            group.send(mine, mine, net.dev(x=ring(net.x, k), c=core))
    group.send(mine, mine, net.partner())
    return group


def gather_pairs(net, buf, done, extra):
    node = lambda k, core: ring(net.x, k) * T + core
    other = 1 - net.c

    def move(n, device):
        return net.send(buf.at[n], buf.at[n], device)

    me = node(0, net.c)
    over = [(node(0, other), move(me, net.partner()))]
    come = [(k, move(me, net.dev(x=ring(net.x, k), c=other))) for k in (2, 1, 3)]
    out = extra()
    done(me)
    for k, copy in come:
        copy.wait_recv()
        over.append((node(-k, net.c), move(node(-k, other), net.partner())))
        done(node(-k, other))
    for n, copy in over:
        copy.wait_recv()
        done(n)
    return out


class Spread:
    def __init__(self, net, buf):
        self.net, self.buf = net, buf
        self.first = [[(k, net.send(ref, ref, device)) for k, ref, device in self.along(h, "yz"[h], net.z, net.y)] for h in (0, 1)]
        self.rest = Group(net, buf.at[pl.ds(0, 3)])
        for h in (0, 1):
            self.cross(h, net.z, net.y)

    def along(self, h, axis, z, y):
        size = self.buf.shape[T] // T
        ref = self.buf.at[z, y, pl.ds(h * size, size)]
        return [(k, ref, self.net.near(axis, k)) for k in (2, 1, 3)]

    def cross(self, h, z, y):
        for _, ref, device in self.along(h, "zy"[h], z, y):
            self.rest.send(ref, ref, device)

    def second(self):
        net = self.net
        for n in range(3):
            for h in (0, 1):
                k, copy = self.first[h][n]
                copy.wait_recv()
                self.cross(h, ring(net.z, -k) if h else net.z, net.y if h else ring(net.y, -k))


def lanes(shape):
    return lax.broadcasted_iota(jnp.int32, shape, len(shape) - 1)


def pack(v):
    return v[:PK] + pltpu.roll(v[PK : T * PK], CLS, 1) + pltpu.roll(v[T * PK :], T * CLS, 1)


def unpack(v):
    keep = lanes((PK, LANE)) < CLS
    parts = [v, pltpu.roll(v, LANE - CLS, 1), pltpu.roll(v, LANE - T * CLS, 1)]
    return [jnp.where(keep, part, 0.0) for part in parts]


def scratch_shapes():
    half, thin, piece = HID // T, ROW // G, CLS + N
    return dict(
        a_v=((G, G, ROW, WIDE), BF16),
        xg=((N, ROW, LANE), BF16),
        cg=((N, N, LANE), F32),
        y1=((WIDE, HID), BF16),
        zp=((G, G, ROW, HID), F32),
        far=((T, T, T, G, thin // T, HID), F32),
        near=((T, T, T, G, thin, HID), F32),
        mid=((T, T, G, thin, HID), F32),
        last=((T, T, G, thin, HID), F32),
        z1=((ROW, HID), F32),
        h1=((ROW, HID), BF16),
        w2p=((LANE, HID), F32),
        y2g=((N, PK, LANE), BF16),
        y2u=((WIDE, LANE), BF16),
        zq=((G, G, PK, LANE), F32),
        zi=((G, G, PK, LANE), F32),
        g2s=((PK, LANE), BF16),
        g2g=((G, G, PK, LANE), BF16),
        g2u=((TALL, LANE), BF16),
        d2=((G, CLS, PAIR), F32),
        d2i=((G, CLS, PAIR), F32),
        d2s=((T, CLS, PAIR), F32),
        d2t=((PAIR, LANE), F32),
        g1g=((G, G, ROW, HID), BF16),
        mg=((G, G, ROW, HID), BF16),
        dys=((PK, LANE), BF16),
        dyg=((G, G, PK, LANE), BF16),
        e1=((3, HID, WIDE // 3), F32),
        e1o=((3, half, WIDE // 3), F32),
        e1s=((3, half, WIDE // 3), F32),
        e1far=((3, T, half // N, WIDE // 3), F32),
        e1near=((3, T, half // G, WIDE // 3), F32),
        w2s=((T, piece, LANE), F32),
        w2o=((piece, LANE), F32),
        wx=((G, piece, LANE), F32),
        wr_own=((piece, LANE), F32),
        wr=((G, G, piece, LANE), F32),
        wf=((T, piece, LANE), F32),
        ra=((half // G, LANE), F32),
        rai=((G, G, half // G, LANE), F32),
        rf=((N, half // G, LANE), F32),
        w1v=((LANE, HID), F32),
        lab=((ROW,), jnp.int32),
        msk=((ROW,), jnp.int32),
        lab_o=((ROW,), jnp.int32),
        msk_o=((ROW,), jnp.int32),
    )


def kernel(adj, x_ref, w1_ref, w2_ref, lab_ref, msk_ref, out_ref, *scratch):
    names = list(scratch_shapes())
    s = dict(zip(names, scratch))
    send_sem, recv_sem, load_sem = scratch[len(names) :]
    net = Net(send_sem, recv_sem)
    z, y, x, c = net.z, net.y, net.x, net.c
    a_v = s["a_v"]

    barrier = pltpu.get_barrier_semaphore()
    peers = net.peers()
    for peer in peers:
        pl.semaphore_signal(barrier, inc=1, device_id=peer, device_id_type=MESH)

    me = x * T + c
    xg, cg, w2p, w1v, y1 = (s[k] for k in ("xg", "cg", "w2p", "w1v", "y1"))
    w2p[...] = jnp.zeros((LANE, HID), F32)
    pairs = [(msk_ref, s["msk"]), (lab_ref, s["lab"]), (x_ref, xg.at[me]), (w1_ref, w1v), (w2_ref, w2p.at[pl.ds(0, CLS)])]
    pairs += [(adj.at[k], a_v.at[k]) for k in range(G)]
    loads = [pltpu.make_async_copy(src, dst, load_sem.at[k]) for k, (src, dst) in enumerate(pairs)]
    for load in loads:
        load.start()
    small = len(loads) - G
    for load in loads[:small]:
        load.wait()

    def row_of(ref, dtype):
        return ref[...].astype(dtype).reshape(1, ROW)

    cg[me] = jnp.broadcast_to(jnp.sum(row_of(s["msk"], F32), axis=1, keepdims=True), (N, LANE))
    w2b = w2p[...].astype(BF16)
    w1b = w1v[...].astype(BF16)

    pl.semaphore_wait(barrier, len(peers))

    def y1_block(n):
        y1[span(n * ROW, ROW)] = dot(xg[n], w1b, 1, 0).astype(BF16)

    def small_copies():
        swaps = [net.send(s[k], s[k + "_o"], net.partner()) for k in ("lab", "msk")]
        return swaps + [gather_nodes(net, cg)]

    counts = gather_pairs(net, xg, y1_block, small_copies)
    for load in loads[small:]:
        load.wait()

    zp = s["zp"]

    sum1 = RepSum(net, zp, s["far"], s["near"], s["mid"], s["last"])

    def z1_block(h, t):
        row = pl.ds(h * ROW // T, ROW // T)
        a = a_v[t, :, row] if h else a_v[:, t, row]
        term = dot(a.reshape(TALL // N, WIDE), y1[...], 1, 0).reshape(G, ROW // T, HID)
        if h:
            zp[t, :, row] = term
        else:
            zp[:, t, row] = term

    for k in (2, 1, 3, 0):
        for h, p in enumerate((y, z)):
            z1_block(h, ring(p, k))
            if k == T:
                sum1.start(h)
            elif k > 0:
                sum1.free(h, k // T)
    z1 = s["z1"]
    sum1.finish(z1)

    h1 = s["h1"]
    h1[...] = jnp.maximum(z1[...], 0.0).astype(BF16)
    y2 = dot(h1[...], w2b, 1, 1).astype(BF16).astype(F32)
    y2g, y2u = s["y2g"], s["y2u"]
    y2g[me] = pack(y2).astype(BF16)
    blocks = gather_nodes(net, y2g)
    mg = s["mg"]
    mg[z, y] = jnp.where(z1[...] > 0.0, 1.0, 0.0).astype(BF16)
    masks = Spread(net, mg)

    def spread(src, dst, base):
        for g, part in enumerate(unpack(src.astype(F32))):
            dst[span(base * ROW + g * PK, PK)] = part.astype(BF16)

    def spread_y2(j, _):
        for i in range(G):
            spread(y2g[j * G + i], y2u, j * G + i)
        return _

    wait_all(counts + [blocks])
    lax.fori_loop(0, T, spread_y2, 0)

    zq, zi = s["zq"], s["zi"]
    count = jnp.sum(cg[...], axis=0)[:1]
    at_count = lanes((PK, LANE)) == 3 * CLS
    count = jnp.where(at_count, jnp.broadcast_to(count, (PK, LANE)), 0.0)

    arrivals = Group(net, zi)

    def z2_blocks(j, _):
        dz, p = j // T + 1, T * (j % T)
        zz = ring(z, dz)
        term = dot(a_v[zz, pl.ds(p, T)].reshape(PAIR, WIDE), y2u[...], 1, 0)
        for k in (0, 1):
            zq[zz, p + k] = pack(term[k * ROW : (k + 1) * ROW]) + count
            arrivals.send(zq.at[zz, p + k], zi.at[z, y], net.dev(z=zz, y=p + k, c=1 - c))
        return _

    lax.fori_loop(0, N, z2_blocks, 0)
    mask_row, label_row = row_of(s["msk_o"], F32), row_of(s["lab_o"], jnp.int32)
    mask_all = jnp.broadcast_to(mask_row, (LANE, ROW)).T
    classes = lax.broadcasted_iota(jnp.int32, (LANE, ROW), 0)
    one_hot = (jnp.broadcast_to(label_row, (LANE, ROW)) == classes).astype(F32).T
    arrivals.wait_recv()
    packed = jnp.sum(zi[...].reshape(G * G, PK, LANE), axis=0)

    total = jnp.sum(jnp.where(at_count, packed, 0.0), axis=1, keepdims=True)
    total = jnp.concatenate([total, total, total], axis=0)
    logits = jnp.concatenate(unpack(packed), axis=0)
    valid = lanes((ROW, LANE)) < CLS
    top = jnp.max(jnp.where(valid, logits, -jnp.inf), axis=1, keepdims=True)
    shifted = jnp.where(valid, logits - top, 0.0)
    norm = jnp.sum(jnp.where(valid, jnp.exp(shifted), 0.0), axis=1, keepdims=True)
    log_probs = shifted - jnp.log(norm)
    picked = jnp.where(valid, -(mask_all * (one_hot * log_probs)), 0.0)
    loss_part = jnp.sum(picked, axis=0, keepdims=True)
    g2 = jnp.where(valid, (jnp.exp(log_probs) - one_hot) * (mask_all / total), 0.0).astype(BF16).astype(F32)
    g2s, g2g, g2u = s["g2s"], s["g2g"], s["g2u"]
    g2s[...] = pack(g2).astype(BF16)

    arrivals = net.rep_each(g2s, g2g)
    masks.second()
    arrivals(lambda zz, yy: spread(g2g[zz, yy], g2u, zz * G + yy))

    d2, d2i, d2s, d2t = (s[k] for k in ("d2", "d2i", "d2s", "d2t"))

    def a_cols(k, size):
        return a_v[:, :, :, span(k * size, size)].reshape(TALL, size)

    def d2_block(k):
        part = dot(g2u[...], a_cols(k, T * PAIR), 0, 0)[:CLS]
        d2[T * k] = part[:, :PAIR]
        d2[T * k + 1] = part[:, PAIR:]

    arrivals = Group(net, d2i.at[pl.ds(0, 3)])

    def d2_send(t):
        arrivals.send(d2.at[t], d2i.at[x], net.dev(x=t, c=1 - c))

    d2_block(1 - x // T)
    d2_send(ring(x, T))
    d2_send(3 - x)
    d2_block(x // T)
    d2_send(x + 1 - T * (x % T))
    d2i[x] = d2[x]
    arrivals.wait_recv()
    d2s[c] = jnp.sum(d2i[...], axis=0)
    net.send(d2s.at[c], d2s.at[c], net.partner()).wait_recv()
    d2t[...] = jnp.concatenate([d2s[0] + d2s[1], jnp.zeros((LANE - CLS, PAIR), F32)], axis=0).T

    dys, dyg, g1g = s["dys"], s["dyg"], s["g1g"]
    dys[...] = pack(d2t[span((1 - c) * ROW, ROW)].astype(BF16).astype(F32)).astype(BF16)
    arrivals = net.rep_each(dys, dyg)

    w2s, w2o, wx, wr, wf = (s[k] for k in ("w2s", "w2o", "wx", "wr", "wf"))
    dy2 = d2t[span(c * ROW, ROW)].astype(BF16)
    dw2_t = dot(dy2, h1[...], 0, 0)[:CLS]
    loss_tile = jnp.concatenate([loss_part, jnp.zeros((N - 1, LANE), F32)], axis=0)
    for h in (0, 1):
        w2s[h, :CLS] = dw2_t[:, h * LANE : (h + 1) * LANE]
        w2s[h, CLS:] = loss_tile
    swap = net.send(w2s.at[1 - c], w2o, net.partner())
    masks.rest.wait_recv()
    swap.wait_recv()
    wx[x] = w2s[c] + w2o[...]
    swaps = exchange(net, "x", lambda t: wx.at[x], wx)
    net.flush()

    def g1_block(zz, yy):
        dy = jnp.concatenate(unpack(dyg[zz, yy].astype(F32)), axis=0).astype(BF16)
        dh1 = dot(dy, w2b, 1, 0)
        g1g[zz, yy] = jnp.where(mg[zz, yy].astype(F32) > 0.0, dh1, 0.0).astype(BF16)

    arrivals(g1_block)

    e1, e1o, e1s, e1far, e1near = (s[k] for k in ("e1", "e1o", "e1s", "e1far", "e1near"))
    half, size = HID // T, HID // N
    q = size // T

    def tree_of(n):
        part = lambda t, d: span(t * size + d * q, q)
        at = lambda t, d: e1s.at[n, part(t, d)]
        return Tree(net, "x", at, lambda d: e1far.at[n, d], lambda d, e: e1near.at[n, d, pl.ds(e * q, q)], e1near.at[n])

    trees = [tree_of(n) for n in range(3)]
    wide = WIDE // 3

    def e1_block(n):
        e1[n] = dot(g1g[...].reshape(TALL, HID), a_cols(n, wide), 0, 0)
        return net.send(e1.at[n, span((1 - c) * half, half)], e1o.at[n], net.partner())

    def e1_join(n, copy):
        copy.wait_recv()
        e1s[n] = e1[n, span(c * half, half)] + e1o[n]
        trees[n].start()

    def free(tree):
        tree.free(0)
        tree.free(1)

    ahead = e1_block(0)
    for n in (1, 2):
        later = e1_block(n)
        e1_join(n - 1, ahead)
        ahead = later
        if n == 1:
            free(trees[0])
    e1_join(2, ahead)
    free(trees[1])
    free(trees[2])
    swaps.wait_recv()
    wr_own = s["wr_own"]
    wr_own[...] = jnp.sum(wx[...], axis=0)
    w_arrivals = net.rep_send(lambda zz, yy: wr_own, wr)
    for tree in trees:
        tree.relay()
    dw1_t = []
    for n, tree in enumerate(trees):
        tree.end()
        dy1 = (e1s[n, span(x * size, size)] + e1near[n, 0] + e1near[n, 1]).astype(BF16)
        dw1_t.append(dot(dy1, xg[...].reshape(WIDE, LANE)[n * wide : (n + 1) * wide], 1, 0))

    ra, rai, rf = s["ra"], s["rai"], s["rf"]
    ra[...] = dw1_t[0] + dw1_t[1] + dw1_t[2]
    arrivals = net.rep_send(lambda zz, yy: ra, rai)
    w_arrivals.wait_recv()
    wf[1 - c] = jnp.sum(wr[...].reshape(G * G, CLS + N, LANE), axis=0)
    swap = net.send(wf.at[1 - c], wf.at[1 - c], net.partner())
    arrivals.wait_recv()
    place = (1 - c) * G + x
    rf[place] = jnp.sum(rai[...].reshape(G * G, size, LANE), axis=0)
    arrivals = gather_nodes(net, rf, place)
    swap.wait_recv()
    out_ref[:, span(LANE, CLS + N)] = wf[...]
    out_ref[0, span(LANE + CLS + N, N)] = jnp.broadcast_to(total[:1], (N, LANE))
    arrivals.wait_recv()
    out_ref[:, :LANE] = rf[...].reshape(T, LANE, LANE)
    net.flush()


def unpack_kernel(sums, loss_ref, dw1_ref, dw2_ref):
    for h in (0, 1):
        half = span(h * LANE, LANE)
        dw1_ref[:, half] = sums[h, :LANE].T
        dw2_ref[:, half] = sums[h, LANE : LANE + CLS]
    loss = jnp.sum(sums[0, LANE + CLS : LANE + CLS + N])
    loss_ref[0, 0] = loss / jnp.max(sums[0, LANE + CLS + N :])


def solution(mesh):
    vmem, smem = pl.BlockSpec(memory_space=pltpu.VMEM), pl.BlockSpec(memory_space=pltpu.SMEM)
    struct = lambda *shape: jax.ShapeDtypeStruct(shape, F32)

    def device_step(adj_blk, feat_blk, w_one, w_two, label_blk, mask_blk):
        sems = [pltpu.SemaphoreType.DMA((n,)) for n in (N_SEND, N_RECV, N + 1)]
        sums = pl.pallas_call(
            kernel,
            out_shape=struct(T, LANE + CLS + T * N, LANE),
            in_specs=[pl.BlockSpec(memory_space=pl.ANY)] * 6,
            out_specs=vmem,
            scratch_shapes=[pltpu.VMEM(shape, dtype) for shape, dtype in scratch_shapes().values()] + sems,
            compiler_params=pltpu.CompilerParams(collective_id=0, has_side_effects=True, vmem_limit_bytes=56 << 20),
        )(adj_blk.reshape(G, G, ROW, WIDE), feat_blk, w_one, w_two.T, label_blk, mask_blk)
        loss, dw1, dw2 = pl.pallas_call(
            unpack_kernel,
            out_shape=(struct(1, 1), struct(LANE, HID), struct(CLS, HID)),
            in_specs=[vmem],
            out_specs=(smem, vmem, vmem),
        )(sums)
        return loss.reshape(()), dw1, dw2.T

    row_spec = P(("rep", "nodes"))
    return jax.shard_map(
        device_step,
        mesh=mesh,
        in_specs=(P(None, "nodes", "rep"), row_spec, P(), P(), row_spec, row_spec),
        out_specs=(P(), P(), P()),
        check_vma=False,
    )
```
